32 devices in a mesh: gx: 8 (over y, x, core), gy: 4 (over z).
Axes of the slice: x: 2, y: 2, z: 4, core: 2. Of those that a mesh axis runs over, the one named last changes fastest.
Arguments:
- rhs_conc: float32 [16, 64, 2048], P('gx', 'gy'), may hold values from -60 to 60
- rhs_pots: float32 [16, 64, 33], P('gx', 'gy'), may hold values from -60 to 60
- diffusion: float32 [16, 64, 32], P('gx', 'gy'), may hold values from 0.05 to 5
- exchange: float32 [16, 64, 32], P('gx', 'gy'), may hold values from 0.2 to 4
- slope: float32 [16, 64, 32], P('gx', 'gy'), may hold values from 0.1 to 1
Outputs:
- sol_conc: float32 [16, 64, 2048], P('gx', 'gy')
- sol_pots: float32 [16, 64, 33], P('gx', 'gy')
The draws below stay inside these ranges and needn't reach their ends.
All inputs are finite; a program needn't handle non-finite values.
Results may differ from the reference program's by a relative error of at most 0.0003.
Values sent between devices are 32-bit elements; how exact they have to be, the bound alone decides.
No kernel may reach another device: no remote copies, remote signals or barrier semaphores. Data moves between devices by JAX's collectives and lax.ppermute only.
A program may use at most 64 MiB of HBM per device.

```python
import math
import jax
import jax.numpy as jnp
from jax import lax

NE = 32
NR = 64
ITERS = 10
NX = 16
NY = 64


def column_scale(key):
    scale_key = jax.random.fold_in(key, 7)
    row_place = jnp.arange(NX, dtype=jnp.float32)[:, None] / max(NX - 1, 1)
    spread_field = jnp.exp(jax.random.uniform(scale_key, (NX, NY), jnp.float32) * math.log(10.0))
    scale_field = spread_field * jnp.exp(row_place * math.log(3.0))
    return 0.25 * scale_field


def draw_values(key, width):
    values = jnp.clip(jax.random.normal(key, (NX, NY, width), jnp.float32), -5.0, 5.0)
    return values


def draw_rhs_conc(key, part):
    scale_field = column_scale(key)
    values = draw_values(jax.random.fold_in(key, 11), NE * NR)
    return scale_field[:, :, None] * values


def draw_rhs_pots(key, part):
    scale_field = column_scale(key)
    values = draw_values(jax.random.fold_in(key, 13), NE + 1)
    return scale_field[:, :, None] * values


def levels(stream_key, extent, cuts, low, high):
    def one(position, blocks):
        heights = jax.random.uniform(jax.random.fold_in(jax.random.fold_in(stream_key, 6), position), (blocks,), jnp.float32, low / len(cuts), high / len(cuts))
        return jnp.repeat(jnp.exp(heights), extent[position] // blocks).reshape((-1,) + (1,) * (len(extent) - position - 1))

    gain = one(*cuts[0])
    for cut in cuts[1:]:
        gain = gain * one(*cut)
    return gain


def setup_inputs(seed: int = 0) -> dict:
    seeds = jax.random.split(jax.random.key(seed), 6)
    rhs_conc = draw_rhs_conc(jax.random.fold_in(seeds[5], 71), 0)
    rhs_pots = draw_rhs_pots(jax.random.fold_in(seeds[5], 71), 0)
    diffusion = jnp.clip(jnp.exp(math.log(5.0) - 4.6051702 * jax.random.uniform(seeds[2], (NX, NY, NE), jnp.float32) ** levels(seeds[2], (NX, NY, NE), ((0, 8), (1, 4)), -0.2, 0.2)), 0.05, 5.0)
    exchange = jnp.clip(jnp.exp(math.log(4.0) - 2.9957323 * jax.random.uniform(seeds[3], (NX, NY, NE), jnp.float32) ** levels(seeds[3], (NX, NY, NE), ((0, 8), (1, 4)), -0.2, 0.2)), 0.2, 4.0)
    slope = jnp.clip(0.1 + 0.9 * jax.random.uniform(seeds[4], (NX, NY, NE), jnp.float32) ** levels(seeds[4], (NX, NY, NE), ((0, 8), (1, 4)), -0.2, 0.2), 0.1, 1.0)
    return dict(rhs_conc=rhs_conc, rhs_pots=rhs_pots, diffusion=diffusion, exchange=exchange, slope=slope)


node_cond = 1.0
plane_cond = 0.5
collector_cond = 2.0
epsilon = 1e-06

def mirror_laplace(values):
    inner = jnp.concatenate([values[..., :1], values[..., :-1]], axis=-1)
    outer = jnp.concatenate([values[..., 1:], values[..., -1:]], axis=-1)
    return 2.0 * values - inner - outer

def local_operator(conc, padded, diffusion, exchange, slope):
    nodes = exchange.shape[2]
    shell_count = conc.shape[2] // nodes
    shells = conc.reshape(conc.shape[0], conc.shape[1], nodes, shell_count)
    center = padded[1:-1, 1:-1]
    lateral = 4.0 * center - padded[2:, 1:-1] - padded[:-2, 1:-1] - padded[1:-1, 2:] - padded[1:-1, :-2]
    node_pot = center[..., :nodes]
    collector = center[..., nodes]
    current = exchange * (node_pot - collector[..., None])
    surface = shells[..., shell_count - 1]
    surface_flag = (lax.broadcasted_iota(jnp.int32, (shell_count,), 0) == shell_count - 1).astype(jnp.float32)
    new_shells = shells + diffusion[..., None] * mirror_laplace(shells) + current[..., None] * surface_flag
    new_nodes = node_cond * mirror_laplace(node_pot) + current - slope * surface + plane_cond * lateral[..., :nodes]
    new_collector = collector_cond * lateral[..., nodes] - lax.optimization_barrier(jnp.mean(current, axis=-1))
    return (new_shells.reshape(conc.shape), jnp.concatenate([new_nodes, new_collector[..., None]], axis=-1))

def least_squares(columns, start_norm):
    count = len(columns)
    target = [start_norm] + [jnp.zeros_like(start_norm) for step in range(count)]
    cosines = []
    sines = []
    upper_rows = []
    for step in range(count):
        entries = list(columns[step])
        for row in range(step):
            first = cosines[row] * entries[row] + sines[row] * entries[row + 1]
            second = cosines[row] * entries[row + 1] - sines[row] * entries[row]
            entries[row] = first
            entries[row + 1] = second
        radius = jnp.sqrt(entries[step] * entries[step] + entries[step + 1] * entries[step + 1])
        cosine = entries[step] / radius
        sine = entries[step + 1] / radius
        entries[step] = radius
        cosines.append(cosine)
        sines.append(sine)
        lead = target[step]
        target[step] = cosine * lead
        target[step + 1] = -sine * lead
        upper_rows.append(entries[:step + 1])
    weights = [None] * count
    for row in range(count - 1, -1, -1):
        total = target[row]
        for later in range(row + 1, count):
            total = total - upper_rows[later][row] * weights[later]
        weights[row] = total / upper_rows[row][row]
    return weights

def apply_operator(conc, pots, diffusion, exchange, slope):
    padded = jnp.pad(pots, ((1, 1), (1, 1), (0, 0)))
    return local_operator(conc, padded, diffusion, exchange, slope)

def reference(rhs_conc, rhs_pots, diffusion, exchange, slope):
    start_norm = jnp.sqrt(jnp.sum(rhs_conc * rhs_conc) + jnp.sum(rhs_pots * rhs_pots) + epsilon)
    basis = [(rhs_conc / start_norm, rhs_pots / start_norm)]
    columns = []
    for step in range(ITERS):
        image_conc, image_pots = apply_operator(basis[step][0], basis[step][1], diffusion, exchange, slope)
        coeffs = [jnp.sum(vector[0] * image_conc) + jnp.sum(vector[1] * image_pots) for vector in basis]
        rest_conc, rest_pots = (image_conc, image_pots)
        for row in range(step + 1):
            rest_conc = rest_conc - coeffs[row] * basis[row][0]
            rest_pots = rest_pots - coeffs[row] * basis[row][1]
        height = jnp.sqrt(jnp.sum(rest_conc * rest_conc) + jnp.sum(rest_pots * rest_pots) + epsilon)
        basis.append((rest_conc / height, rest_pots / height))
        columns.append(coeffs + [height])
    weights = least_squares(columns, start_norm)
    sol_conc = weights[0] * basis[0][0]
    sol_pots = weights[0] * basis[0][1]
    for step in range(1, ITERS):
        sol_conc = sol_conc + weights[step] * basis[step][0]
        sol_pots = sol_pots + weights[step] * basis[step][1]
    return (sol_conc, sol_pots)
```

```python
import functools

import jax
import jax.numpy as jnp
from jax import lax
from jax.experimental import pallas as pl
from jax.experimental.pallas import tpu as pltpu
from jax.sharding import PartitionSpec as P

ITERS = 10
NR = 64
LANES = 128

node_cond = 1.0
plane_cond = 0.5
collector_cond = 2.0
epsilon = 1e-06

CENTER = 10.45
HALF = 9.55
INVERSE_MAX = 5.0e3
NORM_MIN = 1.0

KV = ITERS + 1
PAIRS = KV * (KV + 1) // 2
SHELLS = ITERS - 1
FIELDS = 5 + SHELLS


def lanes_of(shape):
    return lax.broadcasted_iota(jnp.int32, shape, len(shape) - 1)


def pick(values, index):
    return jnp.take_along_axis(values, index, axis=1, mode="promise_in_bounds")


def pack_kernel(conc_ref, pots_ref, diff_ref, exch_ref, slope_ref, send_ref, deep_ref):
    rows, ys, nodes = exch_ref.shape
    half = rows * nodes
    lane = lanes_of((ys, LANES))

    def join(ref):
        return jnp.concatenate([ref[x][:, :nodes] for x in range(rows)], axis=1)

    collector = jnp.concatenate(
        [jnp.broadcast_to(pots_ref[x][:, nodes : nodes + 1], (ys, nodes)) for x in range(rows)],
        axis=1,
    )
    plain = [join(pots_ref), collector, join(diff_ref), join(exch_ref), join(slope_ref)]
    node = lane % half
    shells = [jnp.zeros((ys, LANES), jnp.float32) for k in range(SHELLS + 1)]
    for x in range(rows):
        for tile in range(nodes * NR // LANES):
            cells = conc_ref[x, :, tile * LANES : (tile + 1) * LANES]
            here = (node // 2) == (x * nodes // 2 + tile)
            for k in range(SHELLS + 1):
                found = pick(cells, (node % 2) * NR + (NR - 1 - k))
                shells[k] = jnp.where(here, found, shells[k])
    low = lane < half
    send_ref[0] = jnp.concatenate([plain[0], plain[1]], axis=1)
    send_ref[1] = jnp.concatenate([plain[2], plain[3]], axis=1)
    send_ref[2] = jnp.where(low, jnp.concatenate([plain[4], plain[4]], axis=1), shells[0])
    for k in range(1, SHELLS, 2):
        send_ref[2 + (k + 1) // 2] = jnp.where(low, shells[k], shells[k + 1])
    deep_ref[...] = shells[SHELLS]


def powers_kernel(
    spot_ref, conc_ref, diff_ref, own_ref, left_ref, right_ref, deep_ref,
    basis_ref, gram_ref,
    field_ref, current_ref, dexp_ref, acc_ref,
):
    rows, ys, nodes = diff_ref.shape
    blocks = own_ref.shape[0]
    half = rows * nodes
    reach = left_ref.shape[2]
    quads = blocks // 2
    window = field_ref.shape[2]
    spot = spot_ref[0]
    quad = spot // 2
    odd = (spot % 2) == 1
    lane2 = lanes_of((ys, LANES))

    field_ref[...] = jnp.zeros(field_ref.shape, jnp.float32)
    for source, start, count in ((own_ref, 0, ys), (right_ref, ys, reach), (left_ref, window - reach, reach)):
        low = lanes_of((count, LANES)) < half
        for field in range(FIELDS):
            for q in range(quads):
                a = source[2 * q, field // 2]
                b = source[2 * q + 1, field // 2]
                if field % 2 == 0:
                    value = jnp.where(low, a, pltpu.roll(b, half, 1))
                else:
                    value = jnp.where(low, pltpu.roll(a, half, 1), b)
                field_ref[field, q, start : start + count, :] = value
    field_ref[FIELDS, quad, 0:ys, :] = deep_ref[...]

    shape = (quads, window, LANES)
    flat = (quads * window, LANES)
    lane = lanes_of(shape)
    diff = field_ref[2]
    exch = field_ref[3]
    slope = field_ref[4]
    inside = exch > 0.0
    first = (lane % nodes) == 0
    last = (lane % nodes) == (nodes - 1)
    block = (lax.broadcasted_iota(jnp.int32, (LANES, LANES), 0) // nodes) == (
        lanes_of((LANES, LANES)) // nodes
    )
    mean_mat = jnp.where(block, 1.0 / nodes, 0.0)

    def lroll(value, shift):
        return pltpu.roll(value.reshape(flat), shift % LANES, 1).reshape(shape)

    def plane(value):
        up = lroll(value, -nodes)
        down = lroll(value, nodes)
        zero = jnp.zeros((1, window, LANES), jnp.float32)
        up_next = jnp.concatenate([up[1:], zero], axis=0)
        down_prev = jnp.concatenate([zero, down[:-1]], axis=0)
        xp = jnp.where(lane < LANES - nodes, up, up_next)
        xm = jnp.where(lane >= nodes, down, down_prev)
        yp = jnp.stack([pltpu.roll(value[q], window - 1, 0) for q in range(quads)])
        ym = jnp.stack([pltpu.roll(value[q], 1, 0) for q in range(quads)])
        return 4.0 * value - xp - xm - yp - ym

    def own_of(ref_value):
        return jnp.where(odd, pltpu.roll(ref_value, half, 1), ref_value)

    pots = field_ref[0]
    coll = field_ref[1]
    shells = [field_ref[5 + k] for k in range(SHELLS + 1)]
    old_pots, old_coll, old_shells = None, None, None
    low2 = lane2 < half
    head = (lane2 % nodes) == 0

    for step in range(KV):
        field_ref[0] = pots
        field_ref[1] = coll
        own_p = own_of(field_ref[0, quad, 0:ys, :])
        own_v = own_of(field_ref[1, quad, 0:ys, :])
        tile = jnp.where(low2, own_p, jnp.where(head, pltpu.roll(own_v, half, 1), 0.0))
        basis_ref[step, basis_ref.shape[1] - 1] = tile
        if step == ITERS:
            break
        flow = exch * (pots - coll)
        field_ref[2] = flow
        current_ref[step] = own_of(field_ref[2, quad, 0:ys, :])
        mean = jnp.dot(
            flow.reshape(flat), mean_mat, precision=lax.Precision.HIGHEST,
            preferred_element_type=jnp.float32,
        ).reshape(shape)
        inner = jnp.where(first, pots, lroll(pots, 1))
        outer = jnp.where(last, pots, lroll(pots, -1))
        image_p = (
            node_cond * (2.0 * pots - inner - outer)
            + flow
            - slope * shells[0]
            + plane_cond * plane(pots)
        )
        image_v = collector_cond * plane(coll) - mean
        keep = SHELLS - step
        image_s = []
        for k in range(keep):
            if k == 0:
                image_s.append(shells[0] + diff * (shells[0] - shells[1]) + flow)
            else:
                image_s.append(
                    shells[k] + diff * (2.0 * shells[k] - shells[k + 1] - shells[k - 1])
                )
        scale = (1.0 if step == 0 else 2.0) / HALF

        def recur(image, now, old):
            value = scale * (image - CENTER * now)
            return value if old is None else value - old

        new_pots = jnp.where(inside, recur(image_p, pots, old_pots), 0.0)
        new_coll = jnp.where(inside, recur(image_v, coll, old_coll), 0.0)
        new_shells = [
            recur(image_s[k], shells[k], None if old_shells is None else old_shells[k])
            for k in range(keep)
        ]
        old_pots, old_coll, old_shells = pots, coll, shells
        pots, coll, shells = new_pots, new_coll, new_shells

    tiles = nodes * NR // LANES
    upper = lane2 // NR
    surface = (lane2 % NR) == (NR - 1)
    bottom = (lane2 % NR) == 0
    for x in range(rows):
        packed = jnp.concatenate([diff_ref[x]] * (LANES // nodes), axis=1)
        for tile in range(tiles):
            dexp_ref[x * tiles + tile] = pick(packed, 2 * tile + upper)
            basis_ref[0, x * tiles + tile] = conc_ref[x, :, tile * LANES : (tile + 1) * LANES]

    def advance(step, carry):
        gain = jnp.where(step == 0, 1.0 / HALF, 2.0 / HALF)
        back = jnp.where(step == 0, 0.0, 1.0)
        before = jnp.maximum(step - 1, 0)
        flow = current_ref[step]
        for x in range(rows):
            for tile in range(tiles):
                at = x * tiles + tile
                now = basis_ref[step, at]
                old = basis_ref[before, at]
                inner = jnp.where(bottom, now, pltpu.roll(now, 1, 1))
                outer = jnp.where(surface, now, pltpu.roll(now, LANES - 1, 1))
                source = jnp.where(surface, pick(flow, x * nodes + 2 * tile + upper), 0.0)
                image = now + dexp_ref[at] * (2.0 * now - inner - outer) + source
                basis_ref[step + 1, at] = gain * (image - CENTER * now) - back * old
        return carry

    lax.fori_loop(0, ITERS, advance, 0)

    acc_ref[...] = jnp.zeros(acc_ref.shape, jnp.float32)
    count = basis_ref.shape[1]

    def gather_gram(at, carry):
        cells = [basis_ref[k, at] for k in range(KV)]
        pair = 0
        for i in range(KV):
            for j in range(i, KV):
                product = cells[i] * cells[j]
                acc_ref[pair] += product[:8] + product[8:]
                pair += 1
        return carry

    lax.fori_loop(0, count, gather_gram, 0)
    sums = jnp.sum(acc_ref[...], axis=1)
    gram_ref[...] = lax.dot_general(
        jnp.ones((gram_ref.shape[0], LANES), jnp.float32), sums, (((1,), (1,)), ((), ())),
        precision=lax.Precision.HIGHEST, preferred_element_type=jnp.float32,
    )


def solve_kernel(sums_ref, basis_ref, conc_ref, pots_ref, flag_ref):
    rows, ys, width = conc_ref.shape
    nodes = pots_ref.shape[2] - 1
    half = rows * nodes
    tiles = width // LANES
    side = 16
    total = jnp.sum(sums_ref[...], axis=0, keepdims=True)
    shape = (side, LANES)
    row = lax.broadcasted_iota(jnp.int32, shape, 0)
    col = lanes_of(shape)
    small = jnp.minimum(row, col)
    large = jnp.maximum(row, col)
    index = small * KV - (small * (small - 1)) // 2 + (large - small)
    valid = (row < KV) & (col < KV)
    index = jnp.where(valid, index, 0)
    gram = jnp.where(valid, pick(jnp.broadcast_to(total, shape), index), 0.0)
    eye = (row == col).astype(jnp.float32)

    def lane_sum(value):
        return jnp.sum(value, axis=1, keepdims=True)

    def sub_sum(value):
        return jnp.sum(value, axis=0, keepdims=True)

    column = (side, 1)
    crow = lax.broadcasted_iota(jnp.int32, column, 0)
    norm0 = gram[0:1, 0:1]
    beta = jnp.sqrt(norm0 + epsilon)
    coeffs = []
    images = []
    q = jnp.where(crow == 0, 1.0, 0.0) / beta
    gq = lane_sum(jnp.where(col == 0, gram, 0.0)) / beta
    table = jnp.where(col == 0, q, 0.0)
    gtable = jnp.where(col == 0, gq, 0.0)
    diag = lane_sum(gram * eye)
    columns = []
    coeffs.append(q)
    worst = jnp.zeros((1, 1), jnp.float32)
    for step in range(ITERS):
        down = pltpu.roll(jnp.broadcast_to(q, shape), 1, 0)
        up = jnp.where(
            row < side - 1, pltpu.roll(jnp.broadcast_to(q, shape), side - 1, 0), 0.0
        )
        q_full = jnp.broadcast_to(q, shape)
        first = jnp.broadcast_to(q[0:1], shape)
        w = CENTER * q_full + (0.5 * HALF) * (down + up) + jnp.where(
            row == 1, (0.5 * HALF) * first, 0.0
        )
        w_row = sub_sum(eye * w)
        g = lane_sum(gram * w_row)
        h_row = sub_sum(table * g)
        u = w[:, 0:1] - lane_sum(table * h_row)
        gu = g - lane_sum(gtable * h_row)
        square = sub_sum(u * gu)
        height = jnp.sqrt(square + epsilon)
        inverse = 1.0 / height
        q = u * inverse
        gq = gu * inverse
        columns.append(
            [lane_sum(jnp.where(lanes_of((1, LANES)) == i, h_row, 0.0)) for i in range(step + 1)]
            + [height]
        )
        coeffs.append(q)
        if step < ITERS - 1:
            table = jnp.where(col == step + 1, q, table)
            gtable = jnp.where(col == step + 1, gq, gtable)
        worst = jnp.maximum(worst, sub_sum(q * q * diag))
    good = (worst < INVERSE_MAX) & (norm0 > NORM_MIN)
    weights = least_squares(columns, beta)
    mix = weights[0] * coeffs[0]
    for step in range(1, ITERS):
        mix = mix + weights[step] * coeffs[step]
    bad = jnp.where(good & (jnp.abs(sub_sum(mix)) < 1e30), 0, 1)
    flag_ref[0] = jnp.max(bad)
    mix_full = jnp.broadcast_to(mix, shape)
    parts = [jnp.broadcast_to(mix_full[k : k + 1], (ys, LANES)) for k in range(ITERS)]

    def combine(at):
        value = parts[0] * basis_ref[0, at]
        for k in range(1, ITERS):
            value = value + parts[k] * basis_ref[k, at]
        return value

    for x in range(rows):
        for tile in range(tiles):
            conc_ref[x, :, tile * LANES : (tile + 1) * LANES] = combine(x * tiles + tile)
    last = combine(rows * tiles)
    for x in range(rows):
        pots_ref[x] = jnp.concatenate(
            [
                last[:, x * nodes : (x + 1) * nodes],
                last[:, half + x * nodes : half + x * nodes + 1],
            ],
            axis=1,
        )


def least_squares(columns, start_norm):
    count = len(columns)
    target = [start_norm] + [jnp.zeros_like(start_norm) for step in range(count)]
    cosines = []
    sines = []
    upper_rows = []
    for step in range(count):
        entries = list(columns[step])
        for row in range(step):
            first = cosines[row] * entries[row] + sines[row] * entries[row + 1]
            second = cosines[row] * entries[row + 1] - sines[row] * entries[row]
            entries[row] = first
            entries[row + 1] = second
        radius = jnp.sqrt(entries[step] * entries[step] + entries[step + 1] * entries[step + 1])
        cosine = entries[step] / radius
        sine = entries[step + 1] / radius
        entries[step] = radius
        cosines.append(cosine)
        sines.append(sine)
        lead = target[step]
        target[step] = cosine * lead
        target[step + 1] = -sine * lead
        upper_rows.append(entries[: step + 1])
    weights = [None] * count
    for row in range(count - 1, -1, -1):
        total = target[row]
        for later in range(row + 1, count):
            total = total - upper_rows[later][row] * weights[later]
        weights[row] = total / upper_rows[row][row]
    return weights


def shifted(cells, axis, dim):
    count = lax.axis_size(axis)
    size = cells.shape[dim]
    head = lax.slice_in_dim(cells, 0, 1, axis=dim)
    tail = lax.slice_in_dim(cells, size - 1, size, axis=dim)
    before = lax.ppermute(tail, axis, [(i, i + 1) for i in range(count - 1)])
    after = lax.ppermute(head, axis, [(i + 1, i) for i in range(count - 1)])
    padded = jnp.concatenate([before, cells, after], axis=dim)
    return lax.slice_in_dim(padded, 0, size, axis=dim), lax.slice_in_dim(padded, 2, size + 2, axis=dim)


def mirror_laplace(values):
    inner = jnp.concatenate([values[..., :1], values[..., :-1]], axis=-1)
    outer = jnp.concatenate([values[..., 1:], values[..., -1:]], axis=-1)
    return 2.0 * values - inner - outer


def local_operator(conc, pots, diffusion, exchange, slope):
    nodes = exchange.shape[2]
    shells = conc.reshape(conc.shape[0], conc.shape[1], nodes, NR)
    xm, xp = shifted(pots, "gx", 0)
    ym, yp = shifted(pots, "gy", 1)
    lateral = 4.0 * pots - xm - xp - ym - yp
    node_pot = pots[..., :nodes]
    current = exchange * (node_pot - pots[..., nodes:])
    flag = (lax.broadcasted_iota(jnp.int32, (NR,), 0) == NR - 1).astype(jnp.float32)
    new_shells = shells + diffusion[..., None] * mirror_laplace(shells) + current[..., None] * flag
    new_nodes = (
        node_cond * mirror_laplace(node_pot)
        + current
        - slope * shells[..., NR - 1]
        + plane_cond * lateral[..., :nodes]
    )
    new_collector = collector_cond * lateral[..., nodes:] - jnp.mean(current, axis=-1, keepdims=True)
    return new_shells.reshape(conc.shape), jnp.concatenate([new_nodes, new_collector], axis=-1)


def weights_kernel(hess_ref, out_ref):
    def entry(i, j):
        return hess_ref[j, i : i + 1, 0:1]

    columns = [[entry(i, j) for i in range(j + 2)] for j in range(ITERS)]
    start = hess_ref[ITERS, 0:1, 0:1]
    for k, weight in enumerate(least_squares(columns, start)):
        out_ref[k : k + 1, :] = jnp.broadcast_to(weight, (1, LANES))


def plain_cycle(rhs_conc, rhs_pots, diffusion, exchange, slope):
    axes = ("gx", "gy")
    square = jnp.sum(rhs_conc * rhs_conc) + jnp.sum(rhs_pots * rhs_pots)
    start = jnp.sqrt(lax.psum(square, axes) + epsilon)
    basis_c = jnp.zeros((KV,) + rhs_conc.shape, jnp.float32).at[0].set(rhs_conc / start)
    basis_p = jnp.zeros((KV,) + rhs_pots.shape, jnp.float32).at[0].set(rhs_pots / start)
    hess = jnp.zeros((KV, 16), jnp.float32).at[ITERS, 0].set(start)
    spot = jnp.arange(16)

    def body(step, carry):
        basis_c, basis_p, hess = carry
        conc = lax.dynamic_index_in_dim(basis_c, step, 0, False)
        pots = lax.dynamic_index_in_dim(basis_p, step, 0, False)
        image_c, image_p = local_operator(conc, pots, diffusion, exchange, slope)
        dots = jnp.sum(basis_c * image_c, axis=(1, 2, 3)) + jnp.sum(basis_p * image_p, axis=(1, 2, 3))
        dots = lax.psum(dots, axes)
        rest_c = image_c - jnp.sum(dots[:, None, None, None] * basis_c, axis=0)
        rest_p = image_p - jnp.sum(dots[:, None, None, None] * basis_p, axis=0)
        square = lax.psum(jnp.sum(rest_c * rest_c) + jnp.sum(rest_p * rest_p), axes)
        height = jnp.sqrt(square + epsilon)
        basis_c = lax.dynamic_update_index_in_dim(basis_c, rest_c / height, step + 1, 0)
        basis_p = lax.dynamic_update_index_in_dim(basis_p, rest_p / height, step + 1, 0)
        line = jnp.concatenate([dots, jnp.zeros((16 - KV,), jnp.float32)])
        line = jnp.where(spot == step + 1, height, line)
        hess = lax.dynamic_update_index_in_dim(hess, line, step, 0)
        return basis_c, basis_p, hess

    basis_c, basis_p, hess = lax.fori_loop(0, ITERS, body, (basis_c, basis_p, hess))
    wide = jnp.broadcast_to(hess[:, :, None], hess.shape + (LANES,))
    weights = pl.pallas_call(
        weights_kernel, out_shape=jax.ShapeDtypeStruct((16, LANES), jnp.float32)
    )(wide)[:KV, 0]
    weights = jnp.where(jnp.arange(KV) < ITERS, weights, 0.0)[:, None, None, None]
    return jnp.sum(weights * basis_c, axis=0), jnp.sum(weights * basis_p, axis=0)


def shards(rhs_conc, rhs_pots, diffusion, exchange, slope):
    rows, ys, nodes = exchange.shape
    gx, gy = lax.axis_size("gx"), lax.axis_size("gy")
    half = rows * nodes
    pairs = FIELDS // 2
    reach = ITERS
    assert half * 2 == LANES and nodes * NR == rhs_conc.shape[2]
    assert ys == 16 and reach <= ys and gx % 2 == 0
    window = 8 * ((ys + 2 * reach + 1 + 7) // 8)
    tiles = rows * nodes * NR // LANES + 1
    f32 = jnp.float32
    vmem = pl.BlockSpec(memory_space=pltpu.VMEM)
    smem = pl.BlockSpec(memory_space=pltpu.SMEM)

    send, deep = pl.pallas_call(
        pack_kernel,
        out_shape=(
            jax.ShapeDtypeStruct((pairs, ys, LANES), f32),
            jax.ShapeDtypeStruct((ys, LANES), f32),
        ),
    )(rhs_conc, rhs_pots, diffusion, exchange, slope)
    own = lax.all_gather(send, "gx", axis=0, tiled=False)
    left = lax.ppermute(own[:, :, ys - reach :], "gy", [(i, i + 1) for i in range(gy - 1)])
    right = lax.ppermute(own[:, :, :reach], "gy", [(i + 1, i) for i in range(gy - 1)])
    spot = lax.axis_index("gx").astype(jnp.int32).reshape(1)

    basis, gram = pl.pallas_call(
        powers_kernel,
        in_specs=[smem] + [vmem] * 6,
        out_specs=(vmem, vmem),
        out_shape=(
            jax.ShapeDtypeStruct((KV, tiles, ys, LANES), f32),
            jax.ShapeDtypeStruct((gx * gy, LANES), f32),
        ),
        scratch_shapes=[
            pltpu.VMEM((FIELDS + 1, gx // 2, window, LANES), f32),
            pltpu.VMEM((ITERS, ys, LANES), f32),
            pltpu.VMEM((tiles - 1, ys, LANES), f32),
            pltpu.VMEM((LANES, 8, LANES), f32),
        ],
    )(spot, rhs_conc, diffusion, own, left, right, deep)

    sums = lax.all_to_all(gram, ("gx", "gy"), 0, 0, tiled=True)

    conc, pots, flag = pl.pallas_call(
        solve_kernel,
        out_shape=(
            jax.ShapeDtypeStruct(rhs_conc.shape, f32),
            jax.ShapeDtypeStruct(rhs_pots.shape, f32),
            jax.ShapeDtypeStruct((1,), jnp.int32),
        ),
        out_specs=(vmem, vmem, smem),
    )(sums, basis)
    return lax.cond(
        flag[0] > 0,
        lambda: plain_cycle(rhs_conc, rhs_pots, diffusion, exchange, slope),
        lambda: (conc, pots),
    )


def solution(mesh):
    spec = P("gx", "gy", None)
    return jax.shard_map(
        shards, mesh=mesh, in_specs=(spec,) * 5, out_specs=(spec, spec), check_vma=False
    )
```

```python
import functools

import jax
import jax.numpy as jnp
from jax import lax
from jax.experimental import pallas as pl
from jax.experimental.pallas import tpu as pltpu
from jax.sharding import PartitionSpec as P

ITERS = 10
NR = 64
LANES = 128

node_cond = 1.0
plane_cond = 0.5
collector_cond = 2.0
epsilon = 1e-06

CENTER = 10.45
HALF = 9.55
INVERSE_MAX = 5.0e3
NORM_MIN = 1.0

KV = ITERS + 1
PAIRS = KV * (KV + 1) // 2
SHELLS = ITERS - 1
FIELDS = 5 + SHELLS
REACHES = [ITERS, SHELLS, SHELLS] + [SHELLS - k for k in range(1, SHELLS, 2)]
STARTS = [sum(REACHES[:pair]) for pair in range(len(REACHES))]
EDGE = sum(REACHES)


def lanes_of(shape):
    return lax.broadcasted_iota(jnp.int32, shape, len(shape) - 1)


def pick(values, index):
    return jnp.take_along_axis(values, index, axis=1, mode="promise_in_bounds")


def pack_kernel(conc_ref, pots_ref, diff_ref, exch_ref, slope_ref, send_ref, up_ref, down_ref, deep_ref):
    rows, ys, nodes = exch_ref.shape
    half = rows * nodes
    lane = lanes_of((ys, LANES))

    def join(ref):
        return jnp.concatenate([ref[x][:, :nodes] for x in range(rows)], axis=1)

    collector = jnp.concatenate(
        [jnp.broadcast_to(pots_ref[x][:, nodes : nodes + 1], (ys, nodes)) for x in range(rows)],
        axis=1,
    )
    plain = [join(pots_ref), collector, join(diff_ref), join(exch_ref), join(slope_ref)]
    node = lane % half
    shells = [jnp.zeros((ys, LANES), jnp.float32) for k in range(SHELLS + 1)]
    for x in range(rows):
        for tile in range(nodes * NR // LANES):
            cells = conc_ref[x, :, tile * LANES : (tile + 1) * LANES]
            here = (node // 2) == (x * nodes // 2 + tile)
            for k in range(SHELLS + 1):
                found = pick(cells, (node % 2) * NR + (NR - 1 - k))
                shells[k] = jnp.where(here, found, shells[k])
    low = lane < half
    packed = [
        jnp.concatenate([plain[0], plain[1]], axis=1),
        jnp.concatenate([plain[2], plain[3]], axis=1),
        jnp.where(low, jnp.concatenate([plain[4], plain[4]], axis=1), shells[0]),
    ]
    packed += [jnp.where(low, shells[k], shells[k + 1]) for k in range(1, SHELLS, 2)]
    for pair, (value, reach, start) in enumerate(zip(packed, REACHES, STARTS)):
        send_ref[pair * ys : (pair + 1) * ys, :] = value
        up_ref[start : start + reach, :] = value[ys - reach :]
        down_ref[start : start + reach, :] = value[:reach]
    deep_ref[...] = shells[SHELLS]


def powers_kernel(
    spot_ref, conc_ref, diff_ref, all_ref, deep_ref,
    basis_ref, gram_ref,
    field_ref, current_ref, dexp_ref, acc_ref,
):
    rows, ys, nodes = diff_ref.shape
    blocks = all_ref.shape[0]
    half = rows * nodes
    quads = blocks // 2
    window = field_ref.shape[2]
    spot = spot_ref[0]
    quad = spot // 2
    odd = (spot % 2) == 1
    lane2 = lanes_of((ys, LANES))

    field_ref[...] = jnp.zeros(field_ref.shape, jnp.float32)
    body = (FIELDS // 2) * ys
    for field in range(FIELDS):
        pair = field // 2
        reach, start = REACHES[pair], STARTS[pair]
        for place, origin, count in (
            (0, pair * ys, ys),
            (window - reach, body + start, reach),
            (ys, body + EDGE + start, reach),
        ):
            low = lanes_of((count, LANES)) < half
            for q in range(quads):
                a = all_ref[2 * q, origin : origin + count, :]
                b = all_ref[2 * q + 1, origin : origin + count, :]
                if field % 2 == 0:
                    value = jnp.where(low, a, pltpu.roll(b, half, 1))
                else:
                    value = jnp.where(low, pltpu.roll(a, half, 1), b)
                field_ref[field, q, place : place + count, :] = value
    field_ref[FIELDS, quad, 0:ys, :] = deep_ref[...]

    shape = (quads, window, LANES)
    flat = (quads * window, LANES)
    lane = lanes_of(shape)
    diff = field_ref[2]
    exch = field_ref[3]
    slope = field_ref[4]
    inside = exch > 0.0
    first = (lane % nodes) == 0
    last = (lane % nodes) == (nodes - 1)
    block = (lax.broadcasted_iota(jnp.int32, (LANES, LANES), 0) // nodes) == (
        lanes_of((LANES, LANES)) // nodes
    )
    mean_mat = jnp.where(block, 1.0 / nodes, 0.0)

    def lroll(value, shift):
        return pltpu.roll(value.reshape(flat), shift % LANES, 1).reshape(shape)

    def plane(value):
        up = lroll(value, -nodes)
        down = lroll(value, nodes)
        zero = jnp.zeros((1, window, LANES), jnp.float32)
        up_next = jnp.concatenate([up[1:], zero], axis=0)
        down_prev = jnp.concatenate([zero, down[:-1]], axis=0)
        xp = jnp.where(lane < LANES - nodes, up, up_next)
        xm = jnp.where(lane >= nodes, down, down_prev)
        yp = jnp.stack([pltpu.roll(value[q], window - 1, 0) for q in range(quads)])
        ym = jnp.stack([pltpu.roll(value[q], 1, 0) for q in range(quads)])
        return 4.0 * value - xp - xm - yp - ym

    def own_of(ref_value):
        return jnp.where(odd, pltpu.roll(ref_value, half, 1), ref_value)

    pots = field_ref[0]
    coll = field_ref[1]
    shells = [field_ref[5 + k] for k in range(SHELLS + 1)]
    old_pots, old_coll, old_shells = None, None, None
    low2 = lane2 < half
    head = (lane2 % nodes) == 0

    for step in range(KV):
        field_ref[0] = pots
        field_ref[1] = coll
        own_p = own_of(field_ref[0, quad, 0:ys, :])
        own_v = own_of(field_ref[1, quad, 0:ys, :])
        tile = jnp.where(low2, own_p, jnp.where(head, pltpu.roll(own_v, half, 1), 0.0))
        basis_ref[step, basis_ref.shape[1] - 1] = tile
        if step == ITERS:
            break
        flow = exch * (pots - coll)
        field_ref[2] = flow
        current_ref[step] = own_of(field_ref[2, quad, 0:ys, :])
        mean = jnp.dot(
            flow.reshape(flat), mean_mat, precision=lax.Precision.HIGHEST,
            preferred_element_type=jnp.float32,
        ).reshape(shape)
        inner = jnp.where(first, pots, lroll(pots, 1))
        outer = jnp.where(last, pots, lroll(pots, -1))
        image_p = (
            node_cond * (2.0 * pots - inner - outer)
            + flow
            - slope * shells[0]
            + plane_cond * plane(pots)
        )
        image_v = collector_cond * plane(coll) - mean
        keep = SHELLS - step
        image_s = []
        for k in range(keep):
            if k == 0:
                image_s.append(shells[0] + diff * (shells[0] - shells[1]) + flow)
            else:
                image_s.append(
                    shells[k] + diff * (2.0 * shells[k] - shells[k + 1] - shells[k - 1])
                )
        scale = (1.0 if step == 0 else 2.0) / HALF

        def recur(image, now, old):
            value = scale * (image - CENTER * now)
            return value if old is None else value - old

        new_pots = jnp.where(inside, recur(image_p, pots, old_pots), 0.0)
        new_coll = jnp.where(inside, recur(image_v, coll, old_coll), 0.0)
        new_shells = [
            recur(image_s[k], shells[k], None if old_shells is None else old_shells[k])
            for k in range(keep)
        ]
        old_pots, old_coll, old_shells = pots, coll, shells
        pots, coll, shells = new_pots, new_coll, new_shells

    tiles = nodes * NR // LANES
    upper = lane2 // NR
    surface = (lane2 % NR) == (NR - 1)
    bottom = (lane2 % NR) == 0
    for x in range(rows):
        packed = jnp.concatenate([diff_ref[x]] * (LANES // nodes), axis=1)
        for tile in range(tiles):
            dexp_ref[x * tiles + tile] = pick(packed, 2 * tile + upper)
            basis_ref[0, x * tiles + tile] = conc_ref[x, :, tile * LANES : (tile + 1) * LANES]

    def advance(step, carry):
        gain = jnp.where(step == 0, 1.0 / HALF, 2.0 / HALF)
        back = jnp.where(step == 0, 0.0, 1.0)
        before = jnp.maximum(step - 1, 0)
        flow = current_ref[step]
        for x in range(rows):
            for tile in range(tiles):
                at = x * tiles + tile
                now = basis_ref[step, at]
                old = basis_ref[before, at]
                inner = jnp.where(bottom, now, pltpu.roll(now, 1, 1))
                outer = jnp.where(surface, now, pltpu.roll(now, LANES - 1, 1))
                source = jnp.where(surface, pick(flow, x * nodes + 2 * tile + upper), 0.0)
                image = now + dexp_ref[at] * (2.0 * now - inner - outer) + source
                basis_ref[step + 1, at] = gain * (image - CENTER * now) - back * old
        return carry

    lax.fori_loop(0, ITERS, advance, 0)

    acc_ref[...] = jnp.zeros(acc_ref.shape, jnp.float32)
    count = basis_ref.shape[1]

    def gather_gram(at, carry):
        cells = [basis_ref[k, at] for k in range(KV)]
        pair = 0
        for i in range(KV):
            for j in range(i, KV):
                product = cells[i] * cells[j]
                acc_ref[pair] += product[:8] + product[8:]
                pair += 1
        return carry

    lax.fori_loop(0, count, gather_gram, 0)
    sums = jnp.sum(acc_ref[...], axis=1)
    gram_ref[...] = lax.dot_general(
        jnp.ones((gram_ref.shape[0], LANES), jnp.float32), sums, (((1,), (1,)), ((), ())),
        precision=lax.Precision.HIGHEST, preferred_element_type=jnp.float32,
    )


def solve_kernel(sums_ref, basis_ref, conc_ref, pots_ref, flag_ref):
    rows, ys, width = conc_ref.shape
    nodes = pots_ref.shape[2] - 1
    half = rows * nodes
    tiles = width // LANES
    side = 16
    total = jnp.sum(sums_ref[...], axis=0, keepdims=True)
    shape = (side, LANES)
    row = lax.broadcasted_iota(jnp.int32, shape, 0)
    col = lanes_of(shape)
    small = jnp.minimum(row, col)
    large = jnp.maximum(row, col)
    index = small * KV - (small * (small - 1)) // 2 + (large - small)
    valid = (row < KV) & (col < KV)
    index = jnp.where(valid, index, 0)
    gram = jnp.where(valid, pick(jnp.broadcast_to(total, shape), index), 0.0)
    eye = (row == col).astype(jnp.float32)

    def lane_sum(value):
        return jnp.sum(value, axis=1, keepdims=True)

    def sub_sum(value):
        return jnp.sum(value, axis=0, keepdims=True)

    column = (side, 1)
    crow = lax.broadcasted_iota(jnp.int32, column, 0)
    norm0 = gram[0:1, 0:1]
    beta = jnp.sqrt(norm0 + epsilon)
    coeffs = []
    images = []
    q = jnp.where(crow == 0, 1.0, 0.0) / beta
    gq = lane_sum(jnp.where(col == 0, gram, 0.0)) / beta
    table = jnp.where(col == 0, q, 0.0)
    gtable = jnp.where(col == 0, gq, 0.0)
    diag = lane_sum(gram * eye)
    columns = []
    coeffs.append(q)
    worst = jnp.zeros((1, 1), jnp.float32)
    for step in range(ITERS):
        down = pltpu.roll(jnp.broadcast_to(q, shape), 1, 0)
        up = jnp.where(
            row < side - 1, pltpu.roll(jnp.broadcast_to(q, shape), side - 1, 0), 0.0
        )
        q_full = jnp.broadcast_to(q, shape)
        first = jnp.broadcast_to(q[0:1], shape)
        w = CENTER * q_full + (0.5 * HALF) * (down + up) + jnp.where(
            row == 1, (0.5 * HALF) * first, 0.0
        )
        w_row = sub_sum(eye * w)
        g = lane_sum(gram * w_row)
        h_row = sub_sum(table * g)
        u = w[:, 0:1] - lane_sum(table * h_row)
        gu = g - lane_sum(gtable * h_row)
        square = sub_sum(u * gu)
        height = jnp.sqrt(square + epsilon)
        inverse = 1.0 / height
        q = u * inverse
        gq = gu * inverse
        columns.append(
            [lane_sum(jnp.where(lanes_of((1, LANES)) == i, h_row, 0.0)) for i in range(step + 1)]
            + [height]
        )
        coeffs.append(q)
        if step < ITERS - 1:
            table = jnp.where(col == step + 1, q, table)
            gtable = jnp.where(col == step + 1, gq, gtable)
        worst = jnp.maximum(worst, sub_sum(q * q * diag))
    good = (worst < INVERSE_MAX) & (norm0 > NORM_MIN)
    weights = least_squares(columns, beta)
    mix = weights[0] * coeffs[0]
    for step in range(1, ITERS):
        mix = mix + weights[step] * coeffs[step]
    bad = jnp.where(good & (jnp.abs(sub_sum(mix)) < 1e30), 0, 1)
    flag_ref[0] = jnp.max(bad)
    mix_full = jnp.broadcast_to(mix, shape)
    parts = [jnp.broadcast_to(mix_full[k : k + 1], (ys, LANES)) for k in range(ITERS)]

    def combine(at):
        value = parts[0] * basis_ref[0, at]
        for k in range(1, ITERS):
            value = value + parts[k] * basis_ref[k, at]
        return value

    for x in range(rows):
        for tile in range(tiles):
            conc_ref[x, :, tile * LANES : (tile + 1) * LANES] = combine(x * tiles + tile)
    last = combine(rows * tiles)
    for x in range(rows):
        pots_ref[x] = jnp.concatenate(
            [
                last[:, x * nodes : (x + 1) * nodes],
                last[:, half + x * nodes : half + x * nodes + 1],
            ],
            axis=1,
        )


def least_squares(columns, start_norm):
    count = len(columns)
    target = [start_norm] + [jnp.zeros_like(start_norm) for step in range(count)]
    cosines = []
    sines = []
    upper_rows = []
    for step in range(count):
        entries = list(columns[step])
        for row in range(step):
            first = cosines[row] * entries[row] + sines[row] * entries[row + 1]
            second = cosines[row] * entries[row + 1] - sines[row] * entries[row]
            entries[row] = first
            entries[row + 1] = second
        radius = jnp.sqrt(entries[step] * entries[step] + entries[step + 1] * entries[step + 1])
        cosine = entries[step] / radius
        sine = entries[step + 1] / radius
        entries[step] = radius
        cosines.append(cosine)
        sines.append(sine)
        lead = target[step]
        target[step] = cosine * lead
        target[step + 1] = -sine * lead
        upper_rows.append(entries[: step + 1])
    weights = [None] * count
    for row in range(count - 1, -1, -1):
        total = target[row]
        for later in range(row + 1, count):
            total = total - upper_rows[later][row] * weights[later]
        weights[row] = total / upper_rows[row][row]
    return weights


def shifted(cells, axis, dim):
    count = lax.axis_size(axis)
    size = cells.shape[dim]
    head = lax.slice_in_dim(cells, 0, 1, axis=dim)
    tail = lax.slice_in_dim(cells, size - 1, size, axis=dim)
    before = lax.ppermute(tail, axis, [(i, i + 1) for i in range(count - 1)])
    after = lax.ppermute(head, axis, [(i + 1, i) for i in range(count - 1)])
    padded = jnp.concatenate([before, cells, after], axis=dim)
    return lax.slice_in_dim(padded, 0, size, axis=dim), lax.slice_in_dim(padded, 2, size + 2, axis=dim)


def mirror_laplace(values):
    inner = jnp.concatenate([values[..., :1], values[..., :-1]], axis=-1)
    outer = jnp.concatenate([values[..., 1:], values[..., -1:]], axis=-1)
    return 2.0 * values - inner - outer


def local_operator(conc, pots, diffusion, exchange, slope):
    nodes = exchange.shape[2]
    shells = conc.reshape(conc.shape[0], conc.shape[1], nodes, NR)
    xm, xp = shifted(pots, "gx", 0)
    ym, yp = shifted(pots, "gy", 1)
    lateral = 4.0 * pots - xm - xp - ym - yp
    node_pot = pots[..., :nodes]
    current = exchange * (node_pot - pots[..., nodes:])
    flag = (lax.broadcasted_iota(jnp.int32, (NR,), 0) == NR - 1).astype(jnp.float32)
    new_shells = shells + diffusion[..., None] * mirror_laplace(shells) + current[..., None] * flag
    new_nodes = (
        node_cond * mirror_laplace(node_pot)
        + current
        - slope * shells[..., NR - 1]
        + plane_cond * lateral[..., :nodes]
    )
    new_collector = collector_cond * lateral[..., nodes:] - jnp.mean(current, axis=-1, keepdims=True)
    return new_shells.reshape(conc.shape), jnp.concatenate([new_nodes, new_collector], axis=-1)


def weights_kernel(hess_ref, out_ref):
    def entry(i, j):
        return hess_ref[j, i : i + 1, 0:1]

    columns = [[entry(i, j) for i in range(j + 2)] for j in range(ITERS)]
    start = hess_ref[ITERS, 0:1, 0:1]
    for k, weight in enumerate(least_squares(columns, start)):
        out_ref[k : k + 1, :] = jnp.broadcast_to(weight, (1, LANES))


def plain_cycle(rhs_conc, rhs_pots, diffusion, exchange, slope):
    axes = ("gx", "gy")
    square = jnp.sum(rhs_conc * rhs_conc) + jnp.sum(rhs_pots * rhs_pots)
    start = jnp.sqrt(lax.psum(square, axes) + epsilon)
    basis_c = jnp.zeros((KV,) + rhs_conc.shape, jnp.float32).at[0].set(rhs_conc / start)
    basis_p = jnp.zeros((KV,) + rhs_pots.shape, jnp.float32).at[0].set(rhs_pots / start)
    hess = jnp.zeros((KV, 16), jnp.float32).at[ITERS, 0].set(start)
    spot = jnp.arange(16)

    def body(step, carry):
        basis_c, basis_p, hess = carry
        conc = lax.dynamic_index_in_dim(basis_c, step, 0, False)
        pots = lax.dynamic_index_in_dim(basis_p, step, 0, False)
        image_c, image_p = local_operator(conc, pots, diffusion, exchange, slope)
        dots = jnp.sum(basis_c * image_c, axis=(1, 2, 3)) + jnp.sum(basis_p * image_p, axis=(1, 2, 3))
        dots = lax.psum(dots, axes)
        rest_c = image_c - jnp.sum(dots[:, None, None, None] * basis_c, axis=0)
        rest_p = image_p - jnp.sum(dots[:, None, None, None] * basis_p, axis=0)
        square = lax.psum(jnp.sum(rest_c * rest_c) + jnp.sum(rest_p * rest_p), axes)
        height = jnp.sqrt(square + epsilon)
        basis_c = lax.dynamic_update_index_in_dim(basis_c, rest_c / height, step + 1, 0)
        basis_p = lax.dynamic_update_index_in_dim(basis_p, rest_p / height, step + 1, 0)
        line = jnp.concatenate([dots, jnp.zeros((16 - KV,), jnp.float32)])
        line = jnp.where(spot == step + 1, height, line)
        hess = lax.dynamic_update_index_in_dim(hess, line, step, 0)
        return basis_c, basis_p, hess

    basis_c, basis_p, hess = lax.fori_loop(0, ITERS, body, (basis_c, basis_p, hess))
    wide = jnp.broadcast_to(hess[:, :, None], hess.shape + (LANES,))
    weights = pl.pallas_call(
        weights_kernel, out_shape=jax.ShapeDtypeStruct((16, LANES), jnp.float32)
    )(wide)[:KV, 0]
    weights = jnp.where(jnp.arange(KV) < ITERS, weights, 0.0)[:, None, None, None]
    return jnp.sum(weights * basis_c, axis=0), jnp.sum(weights * basis_p, axis=0)


def shards(rhs_conc, rhs_pots, diffusion, exchange, slope):
    rows, ys, nodes = exchange.shape
    gx, gy = lax.axis_size("gx"), lax.axis_size("gy")
    half = rows * nodes
    pairs = FIELDS // 2
    assert half * 2 == LANES and nodes * NR == rhs_conc.shape[2]
    assert ys == 16 and ITERS <= ys and gx % 2 == 0
    window = 8 * ((ys + 2 * ITERS + 1 + 7) // 8)
    tiles = rows * nodes * NR // LANES + 1
    f32 = jnp.float32
    vmem = pl.BlockSpec(memory_space=pltpu.VMEM)
    smem = pl.BlockSpec(memory_space=pltpu.SMEM)
    params = pltpu.CompilerParams(vmem_limit_bytes=24 << 20)

    send, up, down, deep = pl.pallas_call(
        pack_kernel,
        out_shape=(
            jax.ShapeDtypeStruct((pairs * ys, LANES), f32),
            jax.ShapeDtypeStruct((EDGE, LANES), f32),
            jax.ShapeDtypeStruct((EDGE, LANES), f32),
            jax.ShapeDtypeStruct((ys, LANES), f32),
        ),
        compiler_params=params,
    )(rhs_conc, rhs_pots, diffusion, exchange, slope)
    left = lax.ppermute(up, "gy", [(i, i + 1) for i in range(gy - 1)])
    right = lax.ppermute(down, "gy", [(i + 1, i) for i in range(gy - 1)])
    block = jnp.concatenate([send, left, right], axis=0)
    everything = lax.all_gather(block, "gx", axis=0, tiled=False)
    spot = lax.axis_index("gx").astype(jnp.int32).reshape(1)

    basis, gram = pl.pallas_call(
        powers_kernel,
        in_specs=[smem] + [vmem] * 4,
        out_specs=(vmem, vmem),
        compiler_params=params,
        out_shape=(
            jax.ShapeDtypeStruct((KV, tiles, ys, LANES), f32),
            jax.ShapeDtypeStruct((gx * gy, LANES), f32),
        ),
        scratch_shapes=[
            pltpu.VMEM((FIELDS + 1, gx // 2, window, LANES), f32),
            pltpu.VMEM((ITERS, ys, LANES), f32),
            pltpu.VMEM((tiles - 1, ys, LANES), f32),
            pltpu.VMEM((LANES, 8, LANES), f32),
        ],
    )(spot, rhs_conc, diffusion, everything, deep)

    sums = lax.all_to_all(gram, ("gx", "gy"), 0, 0, tiled=True)

    conc, pots, flag = pl.pallas_call(
        solve_kernel,
        out_shape=(
            jax.ShapeDtypeStruct(rhs_conc.shape, f32),
            jax.ShapeDtypeStruct(rhs_pots.shape, f32),
            jax.ShapeDtypeStruct((1,), jnp.int32),
        ),
        out_specs=(vmem, vmem, smem),
        compiler_params=params,
    )(sums, basis)
    return lax.cond(
        flag[0] > 0,
        lambda: plain_cycle(rhs_conc, rhs_pots, diffusion, exchange, slope),
        lambda: (conc, pots),
    )


def solution(mesh):
    spec = P("gx", "gy", None)
    return jax.shard_map(
        shards, mesh=mesh, in_specs=(spec,) * 5, out_specs=(spec, spec), check_vma=False
    )
```

```python
import functools

import jax
import jax.numpy as jnp
from jax import lax
from jax.experimental import pallas as pl
from jax.experimental.pallas import tpu as pltpu
from jax.sharding import PartitionSpec as P

ITERS = 10
NR = 64
LANES = 128

node_cond = 1.0
plane_cond = 0.5
collector_cond = 2.0
epsilon = 1e-06

CENTER = 10.45
HALF = 9.55
INVERSE_MAX = 2.0e3
NORM_MIN = 1.0

KV = ITERS + 1
PAIRS = KV * (KV + 1) // 2
SHELLS = ITERS - 1
FIELDS = 5 + SHELLS
REACHES = [ITERS, SHELLS, SHELLS] + [SHELLS - k for k in range(1, SHELLS, 2)]
STARTS = [sum(REACHES[:pair]) for pair in range(len(REACHES))]
EDGE = sum(REACHES)


def lanes_of(shape):
    return lax.broadcasted_iota(jnp.int32, shape, len(shape) - 1)


def pick(values, index):
    return jnp.take_along_axis(values, index, axis=1, mode="promise_in_bounds")


def pack_kernel(conc_ref, pots_ref, diff_ref, exch_ref, slope_ref, send_ref, up_ref, down_ref):
    rows, ys, nodes = exch_ref.shape
    half = rows * nodes
    lane = lanes_of((ys, LANES))
    low = lane < half

    def join(ref):
        return [ref[x][:, :nodes] for x in range(rows)]

    collector = [
        jnp.broadcast_to(pots_ref[x][:, nodes : nodes + 1], (ys, nodes)) for x in range(rows)
    ]
    slope = join(slope_ref)
    packed = [
        jnp.concatenate(join(pots_ref) + collector, axis=1),
        jnp.concatenate(join(diff_ref) + join(exch_ref), axis=1),
        jnp.where(low, jnp.concatenate(slope + slope, axis=1), outer_shells(conc_ref, nodes, 0, 0)),
    ]
    packed += [outer_shells(conc_ref, nodes, k, k + 1) for k in range(1, SHELLS, 2)]
    for pair, (value, reach, start) in enumerate(zip(packed, REACHES, STARTS)):
        send_ref[pair * ys : (pair + 1) * ys, :] = value
        up_ref[start : start + reach, :] = value[ys - reach :]
        down_ref[start : start + reach, :] = value[:reach]


def outer_shells(conc_ref, nodes, near, far):
    rows, ys, width = conc_ref.shape
    half = rows * nodes
    lane = lanes_of((ys, LANES))
    node = lane % half
    index = (node % 2) * NR + (NR - 1 - near) - jnp.where(lane < half, 0, far - near)
    found = jnp.zeros((ys, LANES), jnp.float32)
    for x in range(rows):
        for tile in range(width // LANES):
            cells = conc_ref[x, :, tile * LANES : (tile + 1) * LANES]
            here = (node // 2) == (x * nodes // 2 + tile)
            found = jnp.where(here, pick(cells, index), found)
    return found


GAIN = 2.0 / HALF
KEEP = GAIN * (1.0 - CENTER)


def add_gram(cells, lead_mask, acc_ref):
    pair = 0
    for i in range(KV):
        lead = cells[i] if lead_mask is None else cells[i] * lead_mask
        for j in range(i, KV):
            product = lead * cells[j]
            if product.shape[0] == 16:
                product = product[:8] + product[8:]
            acc_ref[pair] += product
            pair += 1


def lane_totals(acc_ref, count):
    sums = jnp.sum(acc_ref[...], axis=1)
    return lax.dot_general(
        jnp.ones((count, LANES), jnp.float32), sums, (((1,), (1,)), ((), ())),
        precision=lax.Precision.HIGHEST, preferred_element_type=jnp.float32,
    )


def turn_nodes(turned, at, rows, ys, nodes):
    lane = lanes_of((8, LANES))
    result = jnp.zeros((8, LANES), jnp.float32)
    for slot in range(nodes // 8):
        for x in range(rows):
            start = x * nodes + 8 * slot
            place = (slot * rows + x) * ys
            piece = pltpu.roll(turned[start : start + 8, :], (place - at) % LANES, 1)
            result = jnp.where((lane >= place) & (lane < place + ys), piece, result)
    return result


def free_kernel(conc_ref, diff_ref, basis_ref, coef_ref, deep_ref, gram_ref, last_ref, acc_ref):
    rows, ys, nodes = diff_ref.shape
    slots = nodes // 8
    deep_ref[...] = outer_shells(conc_ref, nodes, SHELLS, SHELLS)
    spread = jnp.concatenate([diff_ref[x] for x in range(rows)] * 2, axis=1)
    spread = jnp.concatenate([spread] * (LANES // ys), axis=0)
    gain = GAIN * turn_nodes(spread.T, 0, rows, ys, nodes)
    coef_ref[0] = gain
    coef_ref[1] = KEEP + 2.0 * gain
    for group in range(4):
        cells = jnp.concatenate(
            [
                conc_ref[x, :, (4 * slot + group) * LANES : (4 * slot + group + 1) * LANES]
                for slot in range(slots)
                for x in range(rows)
            ],
            axis=0,
        ).T
        for upper in range(LANES // NR):
            basis_ref[0, 2 * group + upper] = cells[upper * NR : (upper + 1) * NR]
    sub = lax.broadcasted_iota(jnp.int32, (8, LANES), 0)

    def image(step, row, base):
        now = basis_ref[step, row, base : base + 8, :]
        if base == 0:
            prev = jnp.where(sub == 0, now, pltpu.roll(now, 1, 0))
        else:
            prev = basis_ref[step, row, base - 1 : base + 7, :]
        if base == NR - 8:
            following = jnp.where(sub == 7, now, pltpu.roll(now, 7, 0))
        else:
            following = basis_ref[step, row, base + 1 : base + 9, :]
        gain = jnp.broadcast_to(coef_ref[0, row : row + 1, :], (8, LANES))
        keep = jnp.broadcast_to(coef_ref[1, row : row + 1, :], (8, LANES))
        return keep * now - gain * (prev + following)

    for row in range(8):
        for base in range(0, NR, 8):
            basis_ref[1, row, base : base + 8, :] = 0.5 * image(0, row, base)

    def advance(step, carry):
        for row in range(8):
            for base in range(0, NR, 8):
                basis_ref[step + 1, row, base : base + 8, :] = (
                    image(step, row, base) - basis_ref[step - 1, row, base : base + 8, :]
                )
        return carry

    lax.fori_loop(1, ITERS - 1, advance, 0)
    for row in range(8):
        for base in range(0, NR, 8):
            last_ref[row, base : base + 8, :] = (
                image(ITERS - 1, row, base) - basis_ref[ITERS - 2, row, base : base + 8, :]
            )

    def cells(row, start, stop):
        line = [basis_ref[k, row, start:stop, :] for k in range(ITERS)]
        return line + [last_ref[row, start:stop, :]]

    acc_ref[...] = jnp.zeros(acc_ref.shape, jnp.float32)
    inner = jnp.where(sub < 16 - ITERS, 1.0, 0.0)

    def gram_row(row, carry):
        for base in range(0, NR - 16, 16):
            add_gram(cells(row, base, base + 16), None, acc_ref)
        add_gram(cells(row, NR - 16, NR - 8), inner, acc_ref)
        return carry

    lax.fori_loop(0, 8, gram_row, 0)
    gram_ref[...] = lane_totals(acc_ref, 8)


def powers_kernel(
    spot_ref, all_ref, basis_ref, coeft_ref, deep_ref, inner_ref,
    outer_ref, gram_ref,
    pot_ref, col_ref, shell_ref, coef_ref, flow_ref, mean_ref, own_ref, tail_ref, acc_ref,
    *, rows, nodes,
):
    ys = deep_ref.shape[0]
    half = rows * nodes
    quads = all_ref.shape[0] // 2
    window = pot_ref.shape[2]
    spot = spot_ref[0]
    quad = spot // 2
    odd = (spot % 2) == 1
    lane2 = lanes_of((ys, LANES))
    low2 = lane2 < half
    head = (lane2 % nodes) == 0

    def room(field):
        if field < 2:
            return (pot_ref if field == 0 else col_ref).at[0]
        return coef_ref.at[field - 2] if field < 5 else shell_ref.at[0, field - 5]

    body = (FIELDS // 2) * ys
    for field in range(FIELDS):
        pair = field // 2
        reach, start = REACHES[pair], STARTS[pair]
        gap = (ys + reach, window - reach)
        scale = GAIN if field == 2 else 1.0
        for q in range(quads):
            room(field)[q, gap[0] : gap[1], :] = jnp.zeros((gap[1] - gap[0], LANES), jnp.float32)
            for place, origin, count in (
                (0, pair * ys, ys),
                (window - reach, body + start, reach),
                (ys, body + EDGE + start, reach),
            ):
                low = lanes_of((count, LANES)) < half
                a = all_ref[2 * q, origin : origin + count, :]
                b = all_ref[2 * q + 1, origin : origin + count, :]
                if field % 2 == 0:
                    value = jnp.where(low, a, pltpu.roll(b, half, 1))
                else:
                    value = jnp.where(low, pltpu.roll(a, half, 1), b)
                room(field)[q, place : place + count, :] = value * scale if field == 2 else value
    for q in range(quads):
        shell_ref[0, SHELLS, q] = jnp.zeros((window, LANES), jnp.float32)
    shell_ref[0, SHELLS, quad, 0:ys, :] = deep_ref[...]

    block = (lax.broadcasted_iota(jnp.int32, (LANES, LANES), 0) // nodes) == (
        lanes_of((LANES, LANES)) // nodes
    )
    mean_mat = jnp.where(block, 1.0 / nodes, 0.0).astype(jnp.bfloat16)
    def own_of(value):
        return jnp.where(odd, pltpu.roll(value, half, 1), value)

    def room_for(step):
        return outer_ref.at[step] if step < ITERS else tail_ref

    for step in range(KV):
        now, old = step % 2, (step + 1) % 2
        own_p = own_of(pot_ref[now, quad, 0:ys, :])
        own_v = own_of(col_ref[now, quad, 0:ys, :])
        room_for(step)[8] = jnp.where(
            low2, own_p, jnp.where(head, pltpu.roll(own_v, half, 1), 0.0)
        )
        if step == ITERS:
            break
        spans = [(0, window)] if step < 2 else [(0, ys + 8), (window - 8, window)]
        size = sum(stop - start for start, stop in spans)
        lane = lanes_of((size, LANES))

        def load(view):
            return jnp.concatenate([view[start:stop, :] for start, stop in spans], axis=0)

        def store(view, value):
            at = 0
            for start, stop in spans:
                view[start:stop, :] = value[at : at + stop - start]
                at += stop - start

        def around(ref, q):
            here = load(ref.at[now, q])
            following = load(ref.at[now, q + 1]) if q + 1 < quads else jnp.zeros_like(here)
            previous = load(ref.at[now, q - 1]) if q > 0 else jnp.zeros_like(here)
            xp = pltpu.roll(jnp.where(lane < nodes, following, here), LANES - nodes, 1)
            xm = pltpu.roll(jnp.where(lane >= LANES - nodes, previous, here), nodes, 1)
            return (xp + xm) + (pltpu.roll(here, size - 1, 0) + pltpu.roll(here, 1, 0))

        def finish(value, view):
            return 0.5 * value if step == 0 else value - load(view)

        for q in range(quads):
            flow = load(coef_ref.at[1, q]) * (load(pot_ref.at[now, q]) - load(col_ref.at[now, q]))
            store(flow_ref.at[q], flow)
            top = flow.astype(jnp.bfloat16)
            rest = flow - top.astype(jnp.float32)
            middle = rest.astype(jnp.bfloat16)
            rest = rest - middle.astype(jnp.float32)
            pieces = jnp.concatenate([top, middle, rest.astype(jnp.bfloat16)], axis=0)
            means = jnp.dot(pieces, mean_mat, preferred_element_type=jnp.float32)
            store(mean_ref.at[q], means[:size] + (means[size : 2 * size] + means[2 * size :]))
        wanted = SHELLS - step
        last = (lane % nodes) == (nodes - 1)
        for q in range(quads):
            flow = load(flow_ref.at[q])
            inside = load(coef_ref.at[1, q]) > 0.0
            diff = load(coef_ref.at[0, q])
            shell = load(shell_ref.at[now, 0, q])
            surface = shell
            fall_before = None
            for k in range(wanted):
                deeper = load(shell_ref.at[now, k + 1, q])
                fall = shell - deeper
                if k == 0:
                    value = KEEP * shell + (diff * fall + GAIN * flow)
                else:
                    value = KEEP * shell + diff * (fall - fall_before)
                view = shell_ref.at[old, k, q]
                store(view, finish(value, view))
                shell, fall_before = deeper, fall
            pots = load(pot_ref.at[now, q])
            drop = jnp.where(last, 0.0, pots - pltpu.roll(pots, LANES - 1, 1))
            value = (
                node_cond * (drop - pltpu.roll(drop, 1, 1))
                + (flow - load(coef_ref.at[2, q]) * surface)
                + (4.0 * plane_cond - CENTER) * pots
                - plane_cond * around(pot_ref, q)
            )
            view = pot_ref.at[old, q]
            store(view, jnp.where(inside, finish(GAIN * value, view), 0.0))
            coll = load(col_ref.at[now, q])
            value = (
                (4.0 * collector_cond - CENTER) * coll
                - collector_cond * around(col_ref, q)
                - load(mean_ref.at[q])
            )
            view = col_ref.at[old, q]
            store(view, jnp.where(inside, finish(GAIN * value, view), 0.0))
        own_ref[step * ys : (step + 1) * ys, :] = own_of(flow_ref[quad, 0:ys, :])

    own_ref[ITERS * ys :, :] = jnp.zeros((own_ref.shape[0] - ITERS * ys, LANES), jnp.float32)
    turned = [own_ref[at : at + LANES, :].T for at in range(0, own_ref.shape[0], LANES)]
    flows = [
        GAIN * turn_nodes(turned[step * ys // LANES], step * ys % LANES, rows, ys, nodes)
        for step in range(ITERS)
    ]
    sub = lax.broadcasted_iota(jnp.int32, (24, LANES), 0)
    for row in range(8):
        gain = jnp.broadcast_to(coeft_ref[0, row : row + 1, :], (24, LANES))
        keep = jnp.broadcast_to(coeft_ref[1, row : row + 1, :], (24, LANES))
        now, old = basis_ref[0, row, NR - 24 :, :], None
        outer_ref[0, row] = now[8:]
        for step in range(ITERS):
            prev = jnp.where(sub == 0, now, pltpu.roll(now, 1, 0))
            following = jnp.where(sub == 23, now, pltpu.roll(now, 23, 0))
            flow = jnp.broadcast_to(flows[step][row : row + 1, :], (24, LANES))
            value = keep * now - gain * (prev + following) + jnp.where(sub == 23, flow, 0.0)
            value = 0.5 * value if step == 0 else value - old
            now, old = value, now
            room_for(step + 1)[row] = now[8:]

    acc_ref[...] = jnp.zeros(acc_ref.shape, jnp.float32)
    inside = jnp.where(lax.broadcasted_iota(jnp.int32, (16, LANES), 0) >= 16 - ITERS, 1.0, 0.0)

    def gram_row(at, carry):
        mask = jnp.where(at < 8, inside, 1.0)
        add_gram([outer_ref[k, at] for k in range(ITERS)] + [tail_ref[at]], mask, acc_ref)
        return carry

    lax.fori_loop(0, 9, gram_row, 0)
    total = lane_totals(acc_ref, gram_ref.shape[0])
    gram_ref[...] = total + jnp.broadcast_to(inner_ref[0:1, :], total.shape)


def solve_kernel(
    sums_ref, basis_ref, outer_ref, conc_out, pots_out, flag_ref, conc_ref, pots_ref, sems
):
    rows, ys, width = conc_ref.shape
    nodes = pots_ref.shape[2] - 1
    half = rows * nodes
    side = 16
    total = jnp.sum(sums_ref[...], axis=0, keepdims=True)
    shape = (side, LANES)
    row = lax.broadcasted_iota(jnp.int32, shape, 0)
    col = lanes_of(shape)
    small = jnp.minimum(row, col)
    large = jnp.maximum(row, col)
    index = small * KV - (small * (small - 1)) // 2 + (large - small)
    valid = (row < KV) & (col < KV)
    index = jnp.where(valid, index, 0)
    gram = jnp.where(valid, pick(jnp.broadcast_to(total, shape), index), 0.0)
    eye = (row == col).astype(jnp.float32)

    def lane_sum(value):
        return jnp.sum(value, axis=1, keepdims=True)

    def sub_sum(value):
        return jnp.sum(value, axis=0, keepdims=True)

    column = (side, 1)
    crow = lax.broadcasted_iota(jnp.int32, column, 0)
    norm0 = gram[0:1, 0:1]
    beta = jnp.sqrt(norm0 + epsilon)
    coeffs = []
    images = []
    q = jnp.where(crow == 0, 1.0, 0.0) / beta
    gq = lane_sum(jnp.where(col == 0, gram, 0.0)) / beta
    table = jnp.where(col == 0, q, 0.0)
    gtable = jnp.where(col == 0, gq, 0.0)
    diag = lane_sum(gram * eye)
    columns = []
    coeffs.append(q)
    worst = jnp.zeros((1, 1), jnp.float32)
    for step in range(ITERS):
        down = pltpu.roll(jnp.broadcast_to(q, shape), 1, 0)
        up = jnp.where(
            row < side - 1, pltpu.roll(jnp.broadcast_to(q, shape), side - 1, 0), 0.0
        )
        q_full = jnp.broadcast_to(q, shape)
        first = jnp.broadcast_to(q[0:1], shape)
        w = CENTER * q_full + (0.5 * HALF) * (down + up) + jnp.where(
            row == 1, (0.5 * HALF) * first, 0.0
        )
        w_row = sub_sum(eye * w)
        g = lane_sum(gram * w_row)
        h_row = sub_sum(table * g)
        u = w[:, 0:1] - lane_sum(table * h_row)
        gu = g - lane_sum(gtable * h_row)
        square = sub_sum(u * gu)
        height = jnp.sqrt(square + epsilon)
        inverse = 1.0 / height
        q = u * inverse
        gq = gu * inverse
        columns.append(
            [lane_sum(jnp.where(lanes_of((1, LANES)) == i, h_row, 0.0)) for i in range(step + 1)]
            + [height]
        )
        coeffs.append(q)
        if step < ITERS - 1:
            table = jnp.where(col == step + 1, q, table)
            gtable = jnp.where(col == step + 1, gq, gtable)
        worst = jnp.maximum(worst, sub_sum(q * q * diag))
    good = (worst < INVERSE_MAX) & (norm0 > NORM_MIN)
    weights = least_squares(columns, beta)
    mix = weights[0] * coeffs[0]
    for step in range(1, ITERS):
        mix = mix + weights[step] * coeffs[step]
    bad = jnp.where(good & (jnp.abs(sub_sum(mix)) < 1e30), 0, 1)
    flag_ref[0] = jnp.max(bad)
    mix_full = jnp.broadcast_to(mix, shape)
    parts = [jnp.broadcast_to(mix_full[k : k + 1], (ys, LANES)) for k in range(ITERS)]

    def combine(ref, at):
        value = parts[0] * ref[(0, *at)]
        for k in range(1, ITERS):
            value = value + parts[k] * ref[(k, *at)]
        return value

    last = combine(outer_ref, (8,))
    for x in range(rows):
        pots_ref[x] = jnp.concatenate(
            [
                last[:, x * nodes : (x + 1) * nodes],
                last[:, half + x * nodes : half + x * nodes + 1],
            ],
            axis=1,
        )
    copies = [pltpu.make_async_copy(pots_ref, pots_out, sems.at[0])]
    copies[0].start()
    reached = lax.broadcasted_iota(jnp.int32, (16, LANES), 0) >= 16 - ITERS
    for group in range(4):
        pieces = []
        for at in (2 * group, 2 * group + 1):
            for base in range(0, NR - 16, 16):
                pieces.append(combine(basis_ref, (at, slice(base, base + 16))))
            pieces.append(
                jnp.where(
                    reached,
                    combine(outer_ref, (at,)),
                    combine(basis_ref, (at, slice(NR - 16, NR))),
                )
            )
        cells = jnp.concatenate(pieces, axis=0).T
        for slot in range(nodes // 8):
            tile = 4 * slot + group
            for x in range(rows):
                start = (slot * rows + x) * ys
                conc_ref[x, :, tile * LANES : (tile + 1) * LANES] = cells[start : start + ys]
    for x in range(rows):
        copy = pltpu.make_async_copy(conc_ref.at[x], conc_out.at[x], sems.at[1 + x])
        copy.start()
        copies.append(copy)
    for copy in copies:
        copy.wait()


def least_squares(columns, start_norm):
    count = len(columns)
    target = [start_norm] + [jnp.zeros_like(start_norm) for step in range(count)]
    cosines = []
    sines = []
    upper_rows = []
    for step in range(count):
        entries = list(columns[step])
        for row in range(step):
            first = cosines[row] * entries[row] + sines[row] * entries[row + 1]
            second = cosines[row] * entries[row + 1] - sines[row] * entries[row]
            entries[row] = first
            entries[row + 1] = second
        radius = jnp.sqrt(entries[step] * entries[step] + entries[step + 1] * entries[step + 1])
        cosine = entries[step] / radius
        sine = entries[step + 1] / radius
        entries[step] = radius
        cosines.append(cosine)
        sines.append(sine)
        lead = target[step]
        target[step] = cosine * lead
        target[step + 1] = -sine * lead
        upper_rows.append(entries[: step + 1])
    weights = [None] * count
    for row in range(count - 1, -1, -1):
        total = target[row]
        for later in range(row + 1, count):
            total = total - upper_rows[later][row] * weights[later]
        weights[row] = total / upper_rows[row][row]
    return weights


def shifted(cells, axis, dim):
    count = lax.axis_size(axis)
    size = cells.shape[dim]
    head = lax.slice_in_dim(cells, 0, 1, axis=dim)
    tail = lax.slice_in_dim(cells, size - 1, size, axis=dim)
    before = lax.ppermute(tail, axis, [(i, i + 1) for i in range(count - 1)])
    after = lax.ppermute(head, axis, [(i + 1, i) for i in range(count - 1)])
    padded = jnp.concatenate([before, cells, after], axis=dim)
    return lax.slice_in_dim(padded, 0, size, axis=dim), lax.slice_in_dim(padded, 2, size + 2, axis=dim)


def mirror_laplace(values):
    inner = jnp.concatenate([values[..., :1], values[..., :-1]], axis=-1)
    outer = jnp.concatenate([values[..., 1:], values[..., -1:]], axis=-1)
    return 2.0 * values - inner - outer


def local_operator(conc, pots, diffusion, exchange, slope):
    nodes = exchange.shape[2]
    shells = conc.reshape(conc.shape[0], conc.shape[1], nodes, NR)
    xm, xp = shifted(pots, "gx", 0)
    ym, yp = shifted(pots, "gy", 1)
    lateral = 4.0 * pots - xm - xp - ym - yp
    node_pot = pots[..., :nodes]
    current = exchange * (node_pot - pots[..., nodes:])
    flag = (lax.broadcasted_iota(jnp.int32, (NR,), 0) == NR - 1).astype(jnp.float32)
    new_shells = shells + diffusion[..., None] * mirror_laplace(shells) + current[..., None] * flag
    new_nodes = (
        node_cond * mirror_laplace(node_pot)
        + current
        - slope * shells[..., NR - 1]
        + plane_cond * lateral[..., :nodes]
    )
    new_collector = collector_cond * lateral[..., nodes:] - jnp.mean(current, axis=-1, keepdims=True)
    return new_shells.reshape(conc.shape), jnp.concatenate([new_nodes, new_collector], axis=-1)


def weights_kernel(hess_ref, out_ref):
    def entry(i, j):
        return hess_ref[j, i : i + 1, 0:1]

    columns = [[entry(i, j) for i in range(j + 2)] for j in range(ITERS)]
    start = hess_ref[ITERS, 0:1, 0:1]
    for k, weight in enumerate(least_squares(columns, start)):
        out_ref[k : k + 1, :] = jnp.broadcast_to(weight, (1, LANES))


def plain_cycle(rhs_conc, rhs_pots, diffusion, exchange, slope):
    axes = ("gx", "gy")
    square = jnp.sum(rhs_conc * rhs_conc) + jnp.sum(rhs_pots * rhs_pots)
    start = jnp.sqrt(lax.psum(square, axes) + epsilon)
    basis_c = jnp.zeros((KV,) + rhs_conc.shape, jnp.float32).at[0].set(rhs_conc / start)
    basis_p = jnp.zeros((KV,) + rhs_pots.shape, jnp.float32).at[0].set(rhs_pots / start)
    hess = jnp.zeros((KV, 16), jnp.float32).at[ITERS, 0].set(start)
    spot = jnp.arange(16)

    def body(step, carry):
        basis_c, basis_p, hess = carry
        conc = lax.dynamic_index_in_dim(basis_c, step, 0, False)
        pots = lax.dynamic_index_in_dim(basis_p, step, 0, False)
        image_c, image_p = local_operator(conc, pots, diffusion, exchange, slope)
        dots = jnp.sum(basis_c * image_c, axis=(1, 2, 3)) + jnp.sum(basis_p * image_p, axis=(1, 2, 3))
        dots = lax.psum(dots, axes)
        rest_c = image_c - jnp.sum(dots[:, None, None, None] * basis_c, axis=0)
        rest_p = image_p - jnp.sum(dots[:, None, None, None] * basis_p, axis=0)
        square = lax.psum(jnp.sum(rest_c * rest_c) + jnp.sum(rest_p * rest_p), axes)
        height = jnp.sqrt(square + epsilon)
        basis_c = lax.dynamic_update_index_in_dim(basis_c, rest_c / height, step + 1, 0)
        basis_p = lax.dynamic_update_index_in_dim(basis_p, rest_p / height, step + 1, 0)
        line = jnp.concatenate([dots, jnp.zeros((16 - KV,), jnp.float32)])
        line = jnp.where(spot == step + 1, height, line)
        hess = lax.dynamic_update_index_in_dim(hess, line, step, 0)
        return basis_c, basis_p, hess

    basis_c, basis_p, hess = lax.fori_loop(0, ITERS, body, (basis_c, basis_p, hess))
    wide = jnp.broadcast_to(hess[:, :, None], hess.shape + (LANES,))
    weights = pl.pallas_call(
        weights_kernel, out_shape=jax.ShapeDtypeStruct((16, LANES), jnp.float32)
    )(wide)[:KV, 0]
    weights = jnp.where(jnp.arange(KV) < ITERS, weights, 0.0)[:, None, None, None]
    return jnp.sum(weights * basis_c, axis=0), jnp.sum(weights * basis_p, axis=0)


def shards(rhs_conc, rhs_pots, diffusion, exchange, slope):
    rows, ys, nodes = exchange.shape
    gx, gy = lax.axis_size("gx"), lax.axis_size("gy")
    half = rows * nodes
    pairs = FIELDS // 2
    assert half * 2 == LANES and nodes * NR == rhs_conc.shape[2]
    assert ys == 16 and ITERS <= ys and gx % 2 == 0
    assert half * 2 == rows * nodes // 8 * ys and LANES == 2 * NR
    window = 8 * ((ys + 2 * ITERS + 1 + 7) // 8)
    f32 = jnp.float32
    vmem = pl.BlockSpec(memory_space=pltpu.VMEM)
    smem = pl.BlockSpec(memory_space=pltpu.SMEM)
    hbm = pl.BlockSpec(memory_space=pltpu.HBM)
    params = pltpu.CompilerParams(vmem_limit_bytes=24 << 20)

    send, up, down = pl.pallas_call(
        pack_kernel,
        out_shape=(
            jax.ShapeDtypeStruct((pairs * ys, LANES), f32),
            jax.ShapeDtypeStruct((EDGE, LANES), f32),
            jax.ShapeDtypeStruct((EDGE, LANES), f32),
        ),
        compiler_params=params,
    )(rhs_conc, rhs_pots, diffusion, exchange, slope)
    left = lax.ppermute(up, "gy", [(i, i + 1) for i in range(gy - 1)])
    right = lax.ppermute(down, "gy", [(i + 1, i) for i in range(gy - 1)])
    basis, coefs, deep, inner_gram = pl.pallas_call(
        free_kernel,
        out_shape=(
            jax.ShapeDtypeStruct((ITERS, 8, NR, LANES), f32),
            jax.ShapeDtypeStruct((2, 8, LANES), f32),
            jax.ShapeDtypeStruct((ys, LANES), f32),
            jax.ShapeDtypeStruct((8, LANES), f32),
        ),
        scratch_shapes=[
            pltpu.VMEM((8, NR, LANES), f32),
            pltpu.VMEM((LANES, 8, LANES), f32),
        ],
        compiler_params=params,
        cost_estimate=pl.CostEstimate(flops=20000000, transcendentals=0, bytes_accessed=3000000),
    )(rhs_conc, diffusion)
    left, right, inner_gram = lax.optimization_barrier((left, right, inner_gram))
    block = jnp.concatenate([send, left, right], axis=0)
    everything = lax.all_gather(block, "gx", axis=0, tiled=False)
    spot = lax.axis_index("gx").astype(jnp.int32).reshape(1)

    quads = gx // 2
    outer, gram = pl.pallas_call(
        functools.partial(powers_kernel, rows=rows, nodes=nodes),
        in_specs=[smem] + [vmem] * 5,
        out_specs=(vmem, vmem),
        out_shape=(
            jax.ShapeDtypeStruct((ITERS, 9, 16, LANES), f32),
            jax.ShapeDtypeStruct((gx * gy, LANES), f32),
        ),
        scratch_shapes=[
            pltpu.VMEM((2, quads, window, LANES), f32),
            pltpu.VMEM((2, quads, window, LANES), f32),
            pltpu.VMEM((2, SHELLS + 1, quads, window, LANES), f32),
            pltpu.VMEM((3, quads, window, LANES), f32),
            pltpu.VMEM((quads, window, LANES), f32),
            pltpu.VMEM((quads, window, LANES), f32),
            pltpu.VMEM((LANES * pl.cdiv(ITERS * ys, LANES), LANES), f32),
            pltpu.VMEM((9, 16, LANES), f32),
            pltpu.VMEM((LANES, 8, LANES), f32),
        ],
        compiler_params=params,
    )(spot, everything, basis, coefs, deep, inner_gram)

    sums = lax.all_to_all(gram, ("gx", "gy"), 0, 0, tiled=True)

    conc, pots, flag = pl.pallas_call(
        solve_kernel,
        out_shape=(
            jax.ShapeDtypeStruct(rhs_conc.shape, f32),
            jax.ShapeDtypeStruct(rhs_pots.shape, f32),
            jax.ShapeDtypeStruct((1,), jnp.int32),
        ),
        out_specs=(hbm, hbm, smem),
        scratch_shapes=[
            pltpu.VMEM(rhs_conc.shape, f32),
            pltpu.VMEM(rhs_pots.shape, f32),
            pltpu.SemaphoreType.DMA((rows + 1,)),
        ],
        compiler_params=params,
    )(sums, basis, outer)
    return lax.while_loop(
        lambda carry: carry[0] > 0,
        lambda carry: (0, *plain_cycle(rhs_conc, rhs_pots, diffusion, exchange, slope)),
        (flag[0], conc, pots),
    )[1:]


def solution(mesh):
    spec = P("gx", "gy", None)
    return jax.shard_map(
        shards, mesh=mesh, in_specs=(spec,) * 5, out_specs=(spec, spec), check_vma=False
    )
```

```python
import functools

import jax
import jax.numpy as jnp
from jax import lax
from jax.experimental import pallas as pl
from jax.experimental.pallas import tpu as pltpu
from jax.sharding import PartitionSpec as P

ITERS = 10
NR = 64
LANES = 128

node_cond = 1.0
plane_cond = 0.5
collector_cond = 2.0
epsilon = 1e-06

CENTER = 10.45
HALF = 9.55
INVERSE_MAX = 2.0e3
NORM_MIN = 1.0

KV = ITERS + 1
PAIRS = KV * (KV + 1) // 2
SHELLS = ITERS - 1
FIELDS = 5 + SHELLS
REACHES = [ITERS, SHELLS, SHELLS] + [SHELLS - k for k in range(1, SHELLS, 2)]
STARTS = [sum(REACHES[:pair]) for pair in range(len(REACHES))]
EDGE = sum(REACHES)


def lanes_of(shape):
    return lax.broadcasted_iota(jnp.int32, shape, len(shape) - 1)


def pick(values, index):
    return jnp.take_along_axis(values, index, axis=1, mode="promise_in_bounds")


def pack_kernel(conc_ref, pots_ref, diff_ref, exch_ref, slope_ref, send_ref, up_ref, down_ref):
    rows, ys, nodes = exch_ref.shape
    half = rows * nodes
    lane = lanes_of((ys, LANES))
    low = lane < half

    def join(ref):
        return [ref[x][:, :nodes] for x in range(rows)]

    collector = [
        jnp.broadcast_to(pots_ref[x][:, nodes : nodes + 1], (ys, nodes)) for x in range(rows)
    ]
    slope = join(slope_ref)
    packed = [
        jnp.concatenate(join(pots_ref) + collector, axis=1),
        jnp.concatenate(join(diff_ref) + join(exch_ref), axis=1),
        jnp.where(low, jnp.concatenate(slope + slope, axis=1), outer_shells(conc_ref, nodes, 0, 0)),
    ]
    packed += [outer_shells(conc_ref, nodes, k, k + 1) for k in range(1, SHELLS, 2)]
    for pair, (value, reach, start) in enumerate(zip(packed, REACHES, STARTS)):
        send_ref[pair * ys : (pair + 1) * ys, :] = value
        up_ref[start : start + reach, :] = value[ys - reach :]
        down_ref[start : start + reach, :] = value[:reach]


def outer_shells(conc_ref, nodes, near, far):
    rows, ys, width = conc_ref.shape
    half = rows * nodes
    lane = lanes_of((ys, LANES))
    node = lane % half
    index = (node % 2) * NR + (NR - 1 - near) - jnp.where(lane < half, 0, far - near)
    found = jnp.zeros((ys, LANES), jnp.float32)
    for x in range(rows):
        for tile in range(width // LANES):
            cells = conc_ref[x, :, tile * LANES : (tile + 1) * LANES]
            here = (node // 2) == (x * nodes // 2 + tile)
            found = jnp.where(here, pick(cells, index), found)
    return found


GAIN = 2.0 / HALF
KEEP = GAIN * (1.0 - CENTER)


def add_gram(cells, lead_mask, acc_ref):
    pair = 0
    for i in range(KV):
        lead = cells[i] if lead_mask is None else cells[i] * lead_mask
        for j in range(i, KV):
            product = lead * cells[j]
            if product.shape[0] == 16:
                product = product[:8] + product[8:]
            acc_ref[pair] += product
            pair += 1


def lane_totals(acc_ref, count):
    sums = jnp.sum(acc_ref[...], axis=1)
    return lax.dot_general(
        jnp.ones((count, LANES), jnp.float32), sums, (((1,), (1,)), ((), ())),
        precision=lax.Precision.HIGHEST, preferred_element_type=jnp.float32,
    )


def turn_nodes(turned, at, rows, ys, nodes):
    lane = lanes_of((8, LANES))
    result = jnp.zeros((8, LANES), jnp.float32)
    for slot in range(nodes // 8):
        for x in range(rows):
            start = x * nodes + 8 * slot
            place = (slot * rows + x) * ys
            piece = pltpu.roll(turned[start : start + 8, :], (place - at) % LANES, 1)
            result = jnp.where((lane >= place) & (lane < place + ys), piece, result)
    return result


def free_kernel(conc_ref, diff_ref, basis_ref, coef_ref, deep_ref, gram_ref, last_ref, acc_ref):
    rows, ys, nodes = diff_ref.shape
    slots = nodes // 8
    deep_ref[...] = outer_shells(conc_ref, nodes, SHELLS, SHELLS)
    spread = jnp.concatenate([diff_ref[x] for x in range(rows)] * 2, axis=1)
    spread = jnp.concatenate([spread] * (LANES // ys), axis=0)
    gain = GAIN * turn_nodes(spread.T, 0, rows, ys, nodes)
    coef_ref[0] = gain
    coef_ref[1] = KEEP + 2.0 * gain
    for group in range(4):
        cells = jnp.concatenate(
            [
                conc_ref[x, :, (4 * slot + group) * LANES : (4 * slot + group + 1) * LANES]
                for slot in range(slots)
                for x in range(rows)
            ],
            axis=0,
        ).T
        for upper in range(LANES // NR):
            basis_ref[0, 2 * group + upper] = cells[upper * NR : (upper + 1) * NR]
    sub = lax.broadcasted_iota(jnp.int32, (8, LANES), 0)

    def image(step, row, base):
        now = basis_ref[step, row, base : base + 8, :]
        if base == 0:
            prev = jnp.where(sub == 0, now, pltpu.roll(now, 1, 0))
        else:
            prev = basis_ref[step, row, base - 1 : base + 7, :]
        if base == NR - 8:
            following = jnp.where(sub == 7, now, pltpu.roll(now, 7, 0))
        else:
            following = basis_ref[step, row, base + 1 : base + 9, :]
        gain = jnp.broadcast_to(coef_ref[0, row : row + 1, :], (8, LANES))
        keep = jnp.broadcast_to(coef_ref[1, row : row + 1, :], (8, LANES))
        return keep * now - gain * (prev + following)

    for row in range(8):
        for base in range(0, NR, 8):
            basis_ref[1, row, base : base + 8, :] = 0.5 * image(0, row, base)

    def advance(step, carry):
        for row in range(8):
            for base in range(0, NR, 8):
                basis_ref[step + 1, row, base : base + 8, :] = (
                    image(step, row, base) - basis_ref[step - 1, row, base : base + 8, :]
                )
        return carry

    lax.fori_loop(1, ITERS - 1, advance, 0)
    for row in range(8):
        for base in range(0, NR, 8):
            last_ref[row, base : base + 8, :] = (
                image(ITERS - 1, row, base) - basis_ref[ITERS - 2, row, base : base + 8, :]
            )

    def cells(row, start, stop):
        line = [basis_ref[k, row, start:stop, :] for k in range(ITERS)]
        return line + [last_ref[row, start:stop, :]]

    acc_ref[...] = jnp.zeros(acc_ref.shape, jnp.float32)
    inner = jnp.where(sub < 16 - ITERS, 1.0, 0.0)

    def gram_row(row, carry):
        for base in range(0, NR - 16, 16):
            add_gram(cells(row, base, base + 16), None, acc_ref)
        add_gram(cells(row, NR - 16, NR - 8), inner, acc_ref)
        return carry

    lax.fori_loop(0, 8, gram_row, 0)
    gram_ref[...] = lane_totals(acc_ref, 8)


def powers_kernel(
    spot_ref, all_ref, basis_ref, coeft_ref, deep_ref, inner_ref,
    outer_ref, gram_ref,
    pot_ref, col_ref, shell_ref, coef_ref, flow_ref, mean_ref, own_ref, tail_ref, acc_ref,
    *, rows, nodes,
):
    ys = deep_ref.shape[0]
    half = rows * nodes
    quads = all_ref.shape[0] // 2
    window = pot_ref.shape[2]
    spot = spot_ref[0]
    quad = spot // 2
    odd = (spot % 2) == 1
    lane2 = lanes_of((ys, LANES))
    low2 = lane2 < half
    head = (lane2 % nodes) == 0

    def room(field):
        if field < 2:
            return (pot_ref if field == 0 else col_ref).at[0]
        return coef_ref.at[field - 2] if field < 5 else shell_ref.at[0, field - 5]

    body = (FIELDS // 2) * ys
    for field in range(FIELDS):
        pair = field // 2
        reach, start = REACHES[pair], STARTS[pair]
        gap = (ys + reach, window - reach)
        scale = GAIN if field == 2 else 1.0
        for q in range(quads):
            room(field)[q, gap[0] : gap[1], :] = jnp.zeros((gap[1] - gap[0], LANES), jnp.float32)
            for place, origin, count in (
                (0, pair * ys, ys),
                (window - reach, body + start, reach),
                (ys, body + EDGE + start, reach),
            ):
                low = lanes_of((count, LANES)) < half
                a = all_ref[2 * q, origin : origin + count, :]
                b = all_ref[2 * q + 1, origin : origin + count, :]
                if field % 2 == 0:
                    value = jnp.where(low, a, pltpu.roll(b, half, 1))
                else:
                    value = jnp.where(low, pltpu.roll(a, half, 1), b)
                room(field)[q, place : place + count, :] = value * scale if field == 2 else value
    for q in range(quads):
        shell_ref[0, SHELLS, q] = jnp.zeros((window, LANES), jnp.float32)
    shell_ref[0, SHELLS, quad, 0:ys, :] = deep_ref[...]

    block = (lax.broadcasted_iota(jnp.int32, (LANES, LANES), 0) // nodes) == (
        lanes_of((LANES, LANES)) // nodes
    )
    mean_mat = jnp.where(block, 1.0 / nodes, 0.0).astype(jnp.bfloat16)
    def own_of(value):
        return jnp.where(odd, pltpu.roll(value, half, 1), value)

    def room_for(step):
        return outer_ref.at[step] if step < ITERS else tail_ref

    for step in range(KV):
        now, old = step % 2, (step + 1) % 2
        own_p = own_of(pot_ref[now, quad, 0:ys, :])
        own_v = own_of(col_ref[now, quad, 0:ys, :])
        room_for(step)[8] = jnp.where(
            low2, own_p, jnp.where(head, pltpu.roll(own_v, half, 1), 0.0)
        )
        if step == ITERS:
            break
        spans = [(0, window)] if step < 2 else [(0, ys + 8), (window - 8, window)]
        size = sum(stop - start for start, stop in spans)
        lane = lanes_of((size, LANES))

        def load(view):
            return jnp.concatenate([view[start:stop, :] for start, stop in spans], axis=0)

        def store(view, value):
            at = 0
            for start, stop in spans:
                view[start:stop, :] = value[at : at + stop - start]
                at += stop - start

        def around(ref, q):
            here = load(ref.at[now, q])
            following = load(ref.at[now, q + 1]) if q + 1 < quads else jnp.zeros_like(here)
            previous = load(ref.at[now, q - 1]) if q > 0 else jnp.zeros_like(here)
            xp = pltpu.roll(jnp.where(lane < nodes, following, here), LANES - nodes, 1)
            xm = pltpu.roll(jnp.where(lane >= LANES - nodes, previous, here), nodes, 1)
            return (xp + xm) + (pltpu.roll(here, size - 1, 0) + pltpu.roll(here, 1, 0))

        def finish(value, view):
            return 0.5 * value if step == 0 else value - load(view)

        for q in range(quads):
            flow = load(coef_ref.at[1, q]) * (load(pot_ref.at[now, q]) - load(col_ref.at[now, q]))
            store(flow_ref.at[q], flow)
            top = flow.astype(jnp.bfloat16)
            rest = flow - top.astype(jnp.float32)
            middle = rest.astype(jnp.bfloat16)
            rest = rest - middle.astype(jnp.float32)
            pieces = jnp.concatenate([top, middle, rest.astype(jnp.bfloat16)], axis=0)
            means = jnp.dot(pieces, mean_mat, preferred_element_type=jnp.float32)
            store(mean_ref.at[q], means[:size] + (means[size : 2 * size] + means[2 * size :]))
        wanted = SHELLS - step
        last = (lane % nodes) == (nodes - 1)
        for q in range(quads):
            flow = load(flow_ref.at[q])
            inside = load(coef_ref.at[1, q]) > 0.0
            diff = load(coef_ref.at[0, q])
            shell = load(shell_ref.at[now, 0, q])
            surface = shell
            fall_before = None
            for k in range(wanted):
                deeper = load(shell_ref.at[now, k + 1, q])
                fall = shell - deeper
                if k == 0:
                    value = KEEP * shell + (diff * fall + GAIN * flow)
                else:
                    value = KEEP * shell + diff * (fall - fall_before)
                view = shell_ref.at[old, k, q]
                store(view, finish(value, view))
                shell, fall_before = deeper, fall
            pots = load(pot_ref.at[now, q])
            drop = jnp.where(last, 0.0, pots - pltpu.roll(pots, LANES - 1, 1))
            value = (
                node_cond * (drop - pltpu.roll(drop, 1, 1))
                + (flow - load(coef_ref.at[2, q]) * surface)
                + (4.0 * plane_cond - CENTER) * pots
                - plane_cond * around(pot_ref, q)
            )
            view = pot_ref.at[old, q]
            store(view, jnp.where(inside, finish(GAIN * value, view), 0.0))
            coll = load(col_ref.at[now, q])
            value = (
                (4.0 * collector_cond - CENTER) * coll
                - collector_cond * around(col_ref, q)
                - load(mean_ref.at[q])
            )
            view = col_ref.at[old, q]
            store(view, jnp.where(inside, finish(GAIN * value, view), 0.0))
        own_ref[step * ys : (step + 1) * ys, :] = own_of(flow_ref[quad, 0:ys, :])

    own_ref[ITERS * ys :, :] = jnp.zeros((own_ref.shape[0] - ITERS * ys, LANES), jnp.float32)
    turned = [own_ref[at : at + LANES, :].T for at in range(0, own_ref.shape[0], LANES)]
    flows = [
        GAIN * turn_nodes(turned[step * ys // LANES], step * ys % LANES, rows, ys, nodes)
        for step in range(ITERS)
    ]
    sub = lax.broadcasted_iota(jnp.int32, (24, LANES), 0)
    for row in range(8):
        gain = jnp.broadcast_to(coeft_ref[0, row : row + 1, :], (24, LANES))
        keep = jnp.broadcast_to(coeft_ref[1, row : row + 1, :], (24, LANES))
        now, old = basis_ref[0, row, NR - 24 :, :], None
        outer_ref[0, row] = now[8:]
        for step in range(ITERS):
            prev = jnp.where(sub == 0, now, pltpu.roll(now, 1, 0))
            following = jnp.where(sub == 23, now, pltpu.roll(now, 23, 0))
            flow = jnp.broadcast_to(flows[step][row : row + 1, :], (24, LANES))
            value = keep * now - gain * (prev + following) + jnp.where(sub == 23, flow, 0.0)
            value = 0.5 * value if step == 0 else value - old
            now, old = value, now
            room_for(step + 1)[row] = now[8:]

    acc_ref[...] = jnp.zeros(acc_ref.shape, jnp.float32)
    inside = jnp.where(lax.broadcasted_iota(jnp.int32, (16, LANES), 0) >= 16 - ITERS, 1.0, 0.0)

    def gram_row(at, carry):
        mask = jnp.where(at < 8, inside, 1.0)
        add_gram([outer_ref[k, at] for k in range(ITERS)] + [tail_ref[at]], mask, acc_ref)
        return carry

    lax.fori_loop(0, 9, gram_row, 0)
    total = lane_totals(acc_ref, gram_ref.shape[0])
    gram_ref[...] = total + jnp.broadcast_to(inner_ref[0:1, :], total.shape)


def solve_kernel(
    sums_ref, basis_ref, outer_ref, conc_out, pots_out, flag_ref, conc_ref, pots_ref, sems
):
    rows, ys, width = conc_ref.shape
    nodes = pots_ref.shape[2] - 1
    half = rows * nodes
    side = 16
    total = jnp.sum(sums_ref[...], axis=0, keepdims=True)
    shape = (side, LANES)
    row = lax.broadcasted_iota(jnp.int32, shape, 0)
    col = lanes_of(shape)
    small = jnp.minimum(row, col)
    large = jnp.maximum(row, col)
    index = small * KV - (small * (small - 1)) // 2 + (large - small)
    valid = (row < KV) & (col < KV)
    index = jnp.where(valid, index, 0)
    gram = jnp.where(valid, pick(jnp.broadcast_to(total, shape), index), 0.0)

    def sub_sum(value):
        return jnp.sum(value, axis=0, keepdims=True)

    def full(value):
        return jnp.broadcast_to(value, shape)

    grams = [full(gram[:, k : k + 1]) for k in range(KV)]
    diag = jnp.zeros(shape, jnp.float32)
    for k in range(KV):
        diag = jnp.where(row == k, grams[k], diag)
    shifted_grams = [CENTER * grams[0] + HALF * grams[1]]
    for k in range(1, ITERS):
        shifted_grams.append(CENTER * grams[k] + (0.5 * HALF) * (grams[k - 1] + grams[k + 1]))
    norm0 = gram[0:1, 0:1]
    start = full(norm0) + epsilon
    inverse = lax.rsqrt(start)
    beta = (start * inverse)[0:1]
    coeffs = [jnp.where(row == 0, inverse, 0.0)]
    images = [grams[0] * inverse]
    columns = []
    worst = jnp.zeros((1, LANES), jnp.float32)
    for step in range(ITERS):
        q = coeffs[step]
        entries = [full(q[k : k + 1]) for k in range(step + 1)]
        down = pltpu.roll(q, 1, 0)
        up = jnp.where(row < side - 1, pltpu.roll(q, side - 1, 0), 0.0)
        w = CENTER * q + (0.5 * HALF) * (down + up)
        w = w + jnp.where(row == 1, (0.5 * HALF) * entries[0], 0.0)
        g = tree_sum([shifted_grams[k] * entries[k] for k in range(step + 1)])
        heads = [sub_sum(coeffs[i] * g) for i in range(step + 1)]
        wide = [full(value) for value in heads]
        u = w - tree_sum([wide[i] * coeffs[i] for i in range(step + 1)])
        gu = g - tree_sum([wide[i] * images[i] for i in range(step + 1)])
        square = sub_sum(u * gu) + epsilon
        inverse = lax.rsqrt(square)
        columns.append(heads + [square * inverse])
        inverse = full(inverse)
        coeffs.append(u * inverse)
        images.append(gu * inverse)
        worst = jnp.maximum(worst, sub_sum(coeffs[-1] * coeffs[-1] * diag))
    good = (worst < INVERSE_MAX) & (norm0 > NORM_MIN)
    weights = least_squares(columns, beta)
    mix = tree_sum([full(weights[step]) * coeffs[step] for step in range(ITERS)])
    bad = jnp.where(good & (jnp.abs(sub_sum(mix)) < 1e30), 0, 1)
    flag_ref[0] = jnp.max(bad)
    parts = [jnp.broadcast_to(mix[k : k + 1], (ys, LANES)) for k in range(ITERS)]

    def combine(ref, at):
        value = parts[0] * ref[(0, *at)]
        for k in range(1, ITERS):
            value = value + parts[k] * ref[(k, *at)]
        return value

    last = combine(outer_ref, (8,))
    for x in range(rows):
        pots_ref[x] = jnp.concatenate(
            [
                last[:, x * nodes : (x + 1) * nodes],
                last[:, half + x * nodes : half + x * nodes + 1],
            ],
            axis=1,
        )
    copies = [pltpu.make_async_copy(pots_ref, pots_out, sems.at[0])]
    copies[0].start()
    reached = lax.broadcasted_iota(jnp.int32, (16, LANES), 0) >= 16 - ITERS
    for group in range(4):
        pieces = []
        for at in (2 * group, 2 * group + 1):
            for base in range(0, NR - 16, 16):
                pieces.append(combine(basis_ref, (at, slice(base, base + 16))))
            pieces.append(
                jnp.where(
                    reached,
                    combine(outer_ref, (at,)),
                    combine(basis_ref, (at, slice(NR - 16, NR))),
                )
            )
        cells = jnp.concatenate(pieces, axis=0).T
        for slot in range(nodes // 8):
            tile = 4 * slot + group
            for x in range(rows):
                start = (slot * rows + x) * ys
                conc_ref[x, :, tile * LANES : (tile + 1) * LANES] = cells[start : start + ys]
            view = (slice(None), slice(None), slice(tile * LANES, (tile + 1) * LANES))
            copy = pltpu.make_async_copy(conc_ref.at[view], conc_out.at[view], sems.at[1 + tile])
            copy.start()
            copies.append(copy)
    for copy in copies:
        copy.wait()


def tree_sum(values):
    while len(values) > 1:
        values = [
            values[i] + values[i + 1] if i + 1 < len(values) else values[i]
            for i in range(0, len(values), 2)
        ]
    return values[0]


def least_squares(columns, start_norm):
    count = len(columns)
    target = [start_norm] + [jnp.zeros_like(start_norm) for step in range(count)]
    cosines = []
    sines = []
    upper_rows = []
    inverses = []
    for step in range(count):
        entries = list(columns[step])
        for row in range(step):
            first = cosines[row] * entries[row] + sines[row] * entries[row + 1]
            second = cosines[row] * entries[row + 1] - sines[row] * entries[row]
            entries[row] = first
            entries[row + 1] = second
        inverse = lax.rsqrt(entries[step] * entries[step] + entries[step + 1] * entries[step + 1])
        cosine = entries[step] * inverse
        sine = entries[step + 1] * inverse
        inverses.append(inverse)
        cosines.append(cosine)
        sines.append(sine)
        lead = target[step]
        target[step] = cosine * lead
        target[step + 1] = -sine * lead
        upper_rows.append(entries[:step])
    weights = [None] * count
    for row in range(count - 1, -1, -1):
        total = target[row]
        for later in range(count - 1, row, -1):
            total = total - upper_rows[later][row] * weights[later]
        weights[row] = total * inverses[row]
    return weights


def shifted(cells, axis, dim):
    count = lax.axis_size(axis)
    size = cells.shape[dim]
    head = lax.slice_in_dim(cells, 0, 1, axis=dim)
    tail = lax.slice_in_dim(cells, size - 1, size, axis=dim)
    before = lax.ppermute(tail, axis, [(i, i + 1) for i in range(count - 1)])
    after = lax.ppermute(head, axis, [(i + 1, i) for i in range(count - 1)])
    padded = jnp.concatenate([before, cells, after], axis=dim)
    return lax.slice_in_dim(padded, 0, size, axis=dim), lax.slice_in_dim(padded, 2, size + 2, axis=dim)


def mirror_laplace(values):
    inner = jnp.concatenate([values[..., :1], values[..., :-1]], axis=-1)
    outer = jnp.concatenate([values[..., 1:], values[..., -1:]], axis=-1)
    return 2.0 * values - inner - outer


def local_operator(conc, pots, diffusion, exchange, slope):
    nodes = exchange.shape[2]
    shells = conc.reshape(conc.shape[0], conc.shape[1], nodes, NR)
    xm, xp = shifted(pots, "gx", 0)
    ym, yp = shifted(pots, "gy", 1)
    lateral = 4.0 * pots - xm - xp - ym - yp
    node_pot = pots[..., :nodes]
    current = exchange * (node_pot - pots[..., nodes:])
    flag = (lax.broadcasted_iota(jnp.int32, (NR,), 0) == NR - 1).astype(jnp.float32)
    new_shells = shells + diffusion[..., None] * mirror_laplace(shells) + current[..., None] * flag
    new_nodes = (
        node_cond * mirror_laplace(node_pot)
        + current
        - slope * shells[..., NR - 1]
        + plane_cond * lateral[..., :nodes]
    )
    new_collector = collector_cond * lateral[..., nodes:] - jnp.mean(current, axis=-1, keepdims=True)
    return new_shells.reshape(conc.shape), jnp.concatenate([new_nodes, new_collector], axis=-1)


def weights_kernel(hess_ref, out_ref):
    def entry(i, j):
        return hess_ref[j, i : i + 1, 0:1]

    columns = [[entry(i, j) for i in range(j + 2)] for j in range(ITERS)]
    start = hess_ref[ITERS, 0:1, 0:1]
    for k, weight in enumerate(least_squares(columns, start)):
        out_ref[k : k + 1, :] = jnp.broadcast_to(weight, (1, LANES))


def plain_cycle(rhs_conc, rhs_pots, diffusion, exchange, slope):
    axes = ("gx", "gy")
    square = jnp.sum(rhs_conc * rhs_conc) + jnp.sum(rhs_pots * rhs_pots)
    start = jnp.sqrt(lax.psum(square, axes) + epsilon)
    basis_c = jnp.zeros((KV,) + rhs_conc.shape, jnp.float32).at[0].set(rhs_conc / start)
    basis_p = jnp.zeros((KV,) + rhs_pots.shape, jnp.float32).at[0].set(rhs_pots / start)
    hess = jnp.zeros((KV, 16), jnp.float32).at[ITERS, 0].set(start)
    spot = jnp.arange(16)

    def body(step, carry):
        basis_c, basis_p, hess = carry
        conc = lax.dynamic_index_in_dim(basis_c, step, 0, False)
        pots = lax.dynamic_index_in_dim(basis_p, step, 0, False)
        image_c, image_p = local_operator(conc, pots, diffusion, exchange, slope)
        dots = jnp.sum(basis_c * image_c, axis=(1, 2, 3)) + jnp.sum(basis_p * image_p, axis=(1, 2, 3))
        dots = lax.psum(dots, axes)
        rest_c = image_c - jnp.sum(dots[:, None, None, None] * basis_c, axis=0)
        rest_p = image_p - jnp.sum(dots[:, None, None, None] * basis_p, axis=0)
        square = lax.psum(jnp.sum(rest_c * rest_c) + jnp.sum(rest_p * rest_p), axes)
        height = jnp.sqrt(square + epsilon)
        basis_c = lax.dynamic_update_index_in_dim(basis_c, rest_c / height, step + 1, 0)
        basis_p = lax.dynamic_update_index_in_dim(basis_p, rest_p / height, step + 1, 0)
        line = jnp.concatenate([dots, jnp.zeros((16 - KV,), jnp.float32)])
        line = jnp.where(spot == step + 1, height, line)
        hess = lax.dynamic_update_index_in_dim(hess, line, step, 0)
        return basis_c, basis_p, hess

    basis_c, basis_p, hess = lax.fori_loop(0, ITERS, body, (basis_c, basis_p, hess))
    wide = jnp.broadcast_to(hess[:, :, None], hess.shape + (LANES,))
    weights = pl.pallas_call(
        weights_kernel, out_shape=jax.ShapeDtypeStruct((16, LANES), jnp.float32)
    )(wide)[:KV, 0]
    weights = jnp.where(jnp.arange(KV) < ITERS, weights, 0.0)[:, None, None, None]
    return jnp.sum(weights * basis_c, axis=0), jnp.sum(weights * basis_p, axis=0)


def shards(rhs_conc, rhs_pots, diffusion, exchange, slope):
    rows, ys, nodes = exchange.shape
    gx, gy = lax.axis_size("gx"), lax.axis_size("gy")
    half = rows * nodes
    pairs = FIELDS // 2
    assert half * 2 == LANES and nodes * NR == rhs_conc.shape[2]
    assert ys == 16 and ITERS <= ys and gx % 2 == 0
    assert half * 2 == rows * nodes // 8 * ys and LANES == 2 * NR
    window = 8 * ((ys + 2 * ITERS + 1 + 7) // 8)
    f32 = jnp.float32
    vmem = pl.BlockSpec(memory_space=pltpu.VMEM)
    smem = pl.BlockSpec(memory_space=pltpu.SMEM)
    hbm = pl.BlockSpec(memory_space=pltpu.HBM)
    params = pltpu.CompilerParams(vmem_limit_bytes=24 << 20)

    send, up, down = pl.pallas_call(
        pack_kernel,
        out_shape=(
            jax.ShapeDtypeStruct((pairs * ys, LANES), f32),
            jax.ShapeDtypeStruct((EDGE, LANES), f32),
            jax.ShapeDtypeStruct((EDGE, LANES), f32),
        ),
        compiler_params=params,
    )(rhs_conc, rhs_pots, diffusion, exchange, slope)
    left = lax.ppermute(up, "gy", [(i, i + 1) for i in range(gy - 1)])
    right = lax.ppermute(down, "gy", [(i + 1, i) for i in range(gy - 1)])
    basis, coefs, deep, inner_gram = pl.pallas_call(
        free_kernel,
        out_shape=(
            jax.ShapeDtypeStruct((ITERS, 8, NR, LANES), f32),
            jax.ShapeDtypeStruct((2, 8, LANES), f32),
            jax.ShapeDtypeStruct((ys, LANES), f32),
            jax.ShapeDtypeStruct((8, LANES), f32),
        ),
        scratch_shapes=[
            pltpu.VMEM((8, NR, LANES), f32),
            pltpu.VMEM((LANES, 8, LANES), f32),
        ],
        compiler_params=params,
        cost_estimate=pl.CostEstimate(flops=20000000, transcendentals=0, bytes_accessed=3000000),
    )(rhs_conc, diffusion)
    left, right, inner_gram = lax.optimization_barrier((left, right, inner_gram))
    block = jnp.concatenate([send, left, right], axis=0)
    everything = lax.all_gather(block, "gx", axis=0, tiled=False)
    spot = lax.axis_index("gx").astype(jnp.int32).reshape(1)

    quads = gx // 2
    outer, gram = pl.pallas_call(
        functools.partial(powers_kernel, rows=rows, nodes=nodes),
        in_specs=[smem] + [vmem] * 5,
        out_specs=(vmem, vmem),
        out_shape=(
            jax.ShapeDtypeStruct((ITERS, 9, 16, LANES), f32),
            jax.ShapeDtypeStruct((gx * gy, LANES), f32),
        ),
        scratch_shapes=[
            pltpu.VMEM((2, quads, window, LANES), f32),
            pltpu.VMEM((2, quads, window, LANES), f32),
            pltpu.VMEM((2, SHELLS + 1, quads, window, LANES), f32),
            pltpu.VMEM((3, quads, window, LANES), f32),
            pltpu.VMEM((quads, window, LANES), f32),
            pltpu.VMEM((quads, window, LANES), f32),
            pltpu.VMEM((LANES * pl.cdiv(ITERS * ys, LANES), LANES), f32),
            pltpu.VMEM((9, 16, LANES), f32),
            pltpu.VMEM((LANES, 8, LANES), f32),
        ],
        compiler_params=params,
    )(spot, everything, basis, coefs, deep, inner_gram)

    sums = lax.all_to_all(gram, ("gx", "gy"), 0, 0, tiled=True)

    conc, pots, flag = pl.pallas_call(
        solve_kernel,
        out_shape=(
            jax.ShapeDtypeStruct(rhs_conc.shape, f32),
            jax.ShapeDtypeStruct(rhs_pots.shape, f32),
            jax.ShapeDtypeStruct((1,), jnp.int32),
        ),
        out_specs=(hbm, hbm, smem),
        scratch_shapes=[
            pltpu.VMEM(rhs_conc.shape, f32),
            pltpu.VMEM(rhs_pots.shape, f32),
            pltpu.SemaphoreType.DMA((1 + nodes * NR // LANES,)),
        ],
        compiler_params=params,
    )(sums, basis, outer)
    return lax.while_loop(
        lambda carry: carry[0] > 0,
        lambda carry: (0, *plain_cycle(rhs_conc, rhs_pots, diffusion, exchange, slope)),
        (flag[0], conc, pots),
    )[1:]


def solution(mesh):
    spec = P("gx", "gy", None)
    return jax.shard_map(
        shards, mesh=mesh, in_specs=(spec,) * 5, out_specs=(spec, spec), check_vma=False
    )
```

```python
import functools

import jax
import jax.numpy as jnp
from jax import lax
from jax.experimental import pallas as pl
from jax.experimental.pallas import tpu as pltpu
from jax.sharding import PartitionSpec as P

ITERS = 10
NR = 64
LANES = 128

node_cond = 1.0
plane_cond = 0.5
collector_cond = 2.0
epsilon = 1e-06

CENTER = 10.45
HALF = 9.55
INVERSE_MAX = 2.0e3
NORM_MIN = 1.0

KV = ITERS + 1
PAIRS = KV * (KV + 1) // 2
SHELLS = ITERS - 1
FIELDS = 5 + SHELLS
REACHES = [ITERS, SHELLS, SHELLS] + [SHELLS - k for k in range(1, SHELLS, 2)]
STARTS = [sum(REACHES[:pair]) for pair in range(len(REACHES))]
EDGE = sum(REACHES)


def lanes_of(shape):
    return lax.broadcasted_iota(jnp.int32, shape, len(shape) - 1)


def pick(values, index):
    return jnp.take_along_axis(values, index, axis=1, mode="promise_in_bounds")


def pack_kernel(
    conc_ref, pots_ref, diff_ref, exch_ref, slope_ref, send_ref, up_ref, down_ref, copy_ref, spread_ref
):
    rows, ys, nodes = exch_ref.shape
    half = rows * nodes
    lane = lanes_of((ys, LANES))
    low = lane < half
    copy_ref[...] = conc_ref[...]
    for x in range(rows):
        spread_ref[x] = diff_ref[x]

    def join(ref):
        return [ref[x][:, :nodes] for x in range(rows)]

    collector = [
        jnp.broadcast_to(pots_ref[x][:, nodes : nodes + 1], (ys, nodes)) for x in range(rows)
    ]
    slope = join(slope_ref)
    packed = [
        jnp.concatenate(join(pots_ref) + collector, axis=1),
        jnp.concatenate(join(diff_ref) + join(exch_ref), axis=1),
        jnp.where(low, jnp.concatenate(slope + slope, axis=1), outer_shells(conc_ref, nodes, 0, 0)),
    ]
    packed += [outer_shells(conc_ref, nodes, k, k + 1) for k in range(1, SHELLS, 2)]
    for pair, (value, reach, start) in enumerate(zip(packed, REACHES, STARTS)):
        send_ref[pair * ys : (pair + 1) * ys, :] = value
        up_ref[start : start + reach, :] = value[ys - reach :]
        down_ref[start : start + reach, :] = value[:reach]


def outer_shells(conc_ref, nodes, near, far):
    rows, ys, width = conc_ref.shape
    half = rows * nodes
    lane = lanes_of((ys, LANES))
    node = lane % half
    index = (node % 2) * NR + (NR - 1 - near) - jnp.where(lane < half, 0, far - near)
    found = jnp.zeros((ys, LANES), jnp.float32)
    for x in range(rows):
        for tile in range(width // LANES):
            cells = conc_ref[x, :, tile * LANES : (tile + 1) * LANES]
            here = (node // 2) == (x * nodes // 2 + tile)
            found = jnp.where(here, pick(cells, index), found)
    return found


GAIN = 2.0 / HALF
KEEP = GAIN * (1.0 - CENTER)


def add_gram(cells, lead_mask, acc_ref):
    pair = 0
    for i in range(KV):
        lead = cells[i] if lead_mask is None else cells[i] * lead_mask
        for j in range(i, KV):
            product = lead * cells[j]
            if product.shape[0] == 16:
                product = product[:8] + product[8:]
            acc_ref[pair] += product
            pair += 1


def lane_totals(acc_ref, count):
    sums = jnp.sum(acc_ref[...], axis=1)
    return lax.dot_general(
        jnp.ones((count, LANES), jnp.float32), sums, (((1,), (1,)), ((), ())),
        precision=lax.Precision.HIGHEST, preferred_element_type=jnp.float32,
    )


def turn_nodes(turned, at, rows, ys, nodes):
    lane = lanes_of((8, LANES))
    result = jnp.zeros((8, LANES), jnp.float32)
    for slot in range(nodes // 8):
        for x in range(rows):
            start = x * nodes + 8 * slot
            place = (slot * rows + x) * ys
            piece = pltpu.roll(turned[start : start + 8, :], (place - at) % LANES, 1)
            result = jnp.where((lane >= place) & (lane < place + ys), piece, result)
    return result


def free_kernel(conc_ref, diff_ref, basis_ref, coef_ref, deep_ref, gram_ref, last_ref, acc_ref):
    rows, ys, nodes = diff_ref.shape
    slots = nodes // 8
    deep_ref[...] = outer_shells(conc_ref, nodes, SHELLS, SHELLS)
    spread = jnp.concatenate([diff_ref[x] for x in range(rows)] * 2, axis=1)
    spread = jnp.concatenate([spread] * (LANES // ys), axis=0)
    gain = GAIN * turn_nodes(spread.T, 0, rows, ys, nodes)
    coef_ref[0] = gain
    coef_ref[1] = KEEP + 2.0 * gain
    for group in range(4):
        cells = jnp.concatenate(
            [
                conc_ref[x, :, (4 * slot + group) * LANES : (4 * slot + group + 1) * LANES]
                for slot in range(slots)
                for x in range(rows)
            ],
            axis=0,
        ).T
        for upper in range(LANES // NR):
            basis_ref[0, 2 * group + upper] = cells[upper * NR : (upper + 1) * NR]
    sub = lax.broadcasted_iota(jnp.int32, (8, LANES), 0)

    def image(step, row, base):
        now = basis_ref[step, row, base : base + 8, :]
        if base == 0:
            prev = jnp.where(sub == 0, now, pltpu.roll(now, 1, 0))
        else:
            prev = basis_ref[step, row, base - 1 : base + 7, :]
        if base == NR - 8:
            following = jnp.where(sub == 7, now, pltpu.roll(now, 7, 0))
        else:
            following = basis_ref[step, row, base + 1 : base + 9, :]
        gain = jnp.broadcast_to(coef_ref[0, row : row + 1, :], (8, LANES))
        keep = jnp.broadcast_to(coef_ref[1, row : row + 1, :], (8, LANES))
        return keep * now - gain * (prev + following)

    for row in range(8):
        for base in range(0, NR, 8):
            basis_ref[1, row, base : base + 8, :] = 0.5 * image(0, row, base)

    for step in range(1, ITERS - 1):
        for row in range(8):
            for base in range(0, NR, 8):
                basis_ref[step + 1, row, base : base + 8, :] = (
                    image(step, row, base) - basis_ref[step - 1, row, base : base + 8, :]
                )
    for row in range(8):
        for base in range(0, NR, 8):
            last_ref[row, base : base + 8, :] = (
                image(ITERS - 1, row, base) - basis_ref[ITERS - 2, row, base : base + 8, :]
            )

    def cells(row, start, stop):
        line = [basis_ref[k, row, start:stop, :] for k in range(ITERS)]
        return line + [last_ref[row, start:stop, :]]

    acc_ref[...] = jnp.zeros(acc_ref.shape, jnp.float32)
    inner = jnp.where(sub < 16 - ITERS, 1.0, 0.0)

    def gram_row(row, carry):
        for base in range(0, NR - 16, 16):
            add_gram(cells(row, base, base + 16), None, acc_ref)
        add_gram(cells(row, NR - 16, NR - 8), inner, acc_ref)
        return carry

    lax.fori_loop(0, 8, gram_row, 0)
    gram_ref[...] = lane_totals(acc_ref, 8)


def powers_kernel(
    spot_ref, all_ref, basis_ref, coeft_ref, deep_ref, inner_ref,
    outer_ref, gram_ref,
    pot_ref, col_ref, shell_ref, coef_ref, flow_ref, mean_ref, own_ref, tail_ref, acc_ref,
    *, rows, nodes,
):
    ys = deep_ref.shape[0]
    half = rows * nodes
    quads = all_ref.shape[0] // 2
    window = pot_ref.shape[2]
    spot = spot_ref[0]
    quad = spot // 2
    odd = (spot % 2) == 1
    lane2 = lanes_of((ys, LANES))
    low2 = lane2 < half
    head = (lane2 % nodes) == 0

    def room(field):
        if field < 2:
            return (pot_ref if field == 0 else col_ref).at[0]
        return coef_ref.at[field - 2] if field < 5 else shell_ref.at[0, field - 5]

    body = (FIELDS // 2) * ys
    for field in range(FIELDS):
        pair = field // 2
        reach, start = REACHES[pair], STARTS[pair]
        gap = (ys + reach, window - reach)
        scale = GAIN if field == 2 else 1.0
        for q in range(quads):
            room(field)[q, gap[0] : gap[1], :] = jnp.zeros((gap[1] - gap[0], LANES), jnp.float32)
            for place, origin, count in (
                (0, pair * ys, ys),
                (window - reach, body + start, reach),
                (ys, body + EDGE + start, reach),
            ):
                low = lanes_of((count, LANES)) < half
                a = all_ref[2 * q, origin : origin + count, :]
                b = all_ref[2 * q + 1, origin : origin + count, :]
                if field % 2 == 0:
                    value = jnp.where(low, a, pltpu.roll(b, half, 1))
                else:
                    value = jnp.where(low, pltpu.roll(a, half, 1), b)
                room(field)[q, place : place + count, :] = value * scale if field == 2 else value
    for q in range(quads):
        shell_ref[0, SHELLS, q] = jnp.zeros((window, LANES), jnp.float32)
    shell_ref[0, SHELLS, quad, 0:ys, :] = deep_ref[...]

    block = (lax.broadcasted_iota(jnp.int32, (LANES, LANES), 0) // nodes) == (
        lanes_of((LANES, LANES)) // nodes
    )
    mean_mat = jnp.where(block, 1.0 / nodes, 0.0).astype(jnp.bfloat16)
    def own_of(value):
        return jnp.where(odd, pltpu.roll(value, half, 1), value)

    def room_for(step):
        return outer_ref.at[step] if step < ITERS else tail_ref

    for step in range(KV):
        now, old = step % 2, (step + 1) % 2
        own_p = own_of(pot_ref[now, quad, 0:ys, :])
        own_v = own_of(col_ref[now, quad, 0:ys, :])
        room_for(step)[8] = jnp.where(
            low2, own_p, jnp.where(head, pltpu.roll(own_v, half, 1), 0.0)
        )
        if step == ITERS:
            break
        spans = [(0, window)] if step < 2 else [(0, ys + 8), (window - 8, window)]
        size = sum(stop - start for start, stop in spans)
        lane = lanes_of((size, LANES))

        def load(view):
            return jnp.concatenate([view[start:stop, :] for start, stop in spans], axis=0)

        def store(view, value):
            at = 0
            for start, stop in spans:
                view[start:stop, :] = value[at : at + stop - start]
                at += stop - start

        def around(ref, q):
            here = load(ref.at[now, q])
            following = load(ref.at[now, q + 1]) if q + 1 < quads else jnp.zeros_like(here)
            previous = load(ref.at[now, q - 1]) if q > 0 else jnp.zeros_like(here)
            xp = pltpu.roll(jnp.where(lane < nodes, following, here), LANES - nodes, 1)
            xm = pltpu.roll(jnp.where(lane >= LANES - nodes, previous, here), nodes, 1)
            return (xp + xm) + (pltpu.roll(here, size - 1, 0) + pltpu.roll(here, 1, 0))

        def finish(value, view):
            return 0.5 * value if step == 0 else value - load(view)

        for q in range(quads):
            flow = load(coef_ref.at[1, q]) * (load(pot_ref.at[now, q]) - load(col_ref.at[now, q]))
            store(flow_ref.at[q], flow)
            top = flow.astype(jnp.bfloat16)
            rest = flow - top.astype(jnp.float32)
            middle = rest.astype(jnp.bfloat16)
            rest = rest - middle.astype(jnp.float32)
            pieces = jnp.concatenate([top, middle, rest.astype(jnp.bfloat16)], axis=0)
            means = jnp.dot(pieces, mean_mat, preferred_element_type=jnp.float32)
            store(mean_ref.at[q], means[:size] + (means[size : 2 * size] + means[2 * size :]))
        wanted = SHELLS - step
        last = (lane % nodes) == (nodes - 1)
        for q in range(quads):
            flow = load(flow_ref.at[q])
            inside = load(coef_ref.at[1, q]) > 0.0
            diff = load(coef_ref.at[0, q])
            shell = load(shell_ref.at[now, 0, q])
            surface = shell
            fall_before = None
            for k in range(wanted):
                deeper = load(shell_ref.at[now, k + 1, q])
                fall = shell - deeper
                if k == 0:
                    value = KEEP * shell + (diff * fall + GAIN * flow)
                else:
                    value = KEEP * shell + diff * (fall - fall_before)
                view = shell_ref.at[old, k, q]
                store(view, finish(value, view))
                shell, fall_before = deeper, fall
            pots = load(pot_ref.at[now, q])
            drop = jnp.where(last, 0.0, pots - pltpu.roll(pots, LANES - 1, 1))
            value = (
                node_cond * (drop - pltpu.roll(drop, 1, 1))
                + (flow - load(coef_ref.at[2, q]) * surface)
                + (4.0 * plane_cond - CENTER) * pots
                - plane_cond * around(pot_ref, q)
            )
            view = pot_ref.at[old, q]
            store(view, jnp.where(inside, finish(GAIN * value, view), 0.0))
            coll = load(col_ref.at[now, q])
            value = (
                (4.0 * collector_cond - CENTER) * coll
                - collector_cond * around(col_ref, q)
                - load(mean_ref.at[q])
            )
            view = col_ref.at[old, q]
            store(view, jnp.where(inside, finish(GAIN * value, view), 0.0))
        own_ref[step * ys : (step + 1) * ys, :] = own_of(flow_ref[quad, 0:ys, :])

    own_ref[ITERS * ys :, :] = jnp.zeros((own_ref.shape[0] - ITERS * ys, LANES), jnp.float32)
    turned = [own_ref[at : at + LANES, :].T for at in range(0, own_ref.shape[0], LANES)]
    flows = [
        GAIN * turn_nodes(turned[step * ys // LANES], step * ys % LANES, rows, ys, nodes)
        for step in range(ITERS)
    ]
    sub = lax.broadcasted_iota(jnp.int32, (24, LANES), 0)
    for row in range(8):
        gain = jnp.broadcast_to(coeft_ref[0, row : row + 1, :], (24, LANES))
        keep = jnp.broadcast_to(coeft_ref[1, row : row + 1, :], (24, LANES))
        now, old = basis_ref[0, row, NR - 24 :, :], None
        outer_ref[0, row] = now[8:]
        for step in range(ITERS):
            prev = jnp.where(sub == 0, now, pltpu.roll(now, 1, 0))
            following = jnp.where(sub == 23, now, pltpu.roll(now, 23, 0))
            flow = jnp.broadcast_to(flows[step][row : row + 1, :], (24, LANES))
            value = keep * now - gain * (prev + following) + jnp.where(sub == 23, flow, 0.0)
            value = 0.5 * value if step == 0 else value - old
            now, old = value, now
            room_for(step + 1)[row] = now[8:]

    acc_ref[...] = jnp.zeros(acc_ref.shape, jnp.float32)
    inside = jnp.where(lax.broadcasted_iota(jnp.int32, (16, LANES), 0) >= 16 - ITERS, 1.0, 0.0)

    def gram_row(at, carry):
        mask = jnp.where(at < 8, inside, 1.0)
        add_gram([outer_ref[k, at] for k in range(ITERS)] + [tail_ref[at]], mask, acc_ref)
        return carry

    lax.fori_loop(0, 9, gram_row, 0)
    total = lane_totals(acc_ref, gram_ref.shape[0])
    gram_ref[...] = total + jnp.broadcast_to(inner_ref[0:1, :], total.shape)


def solve_kernel(
    sums_ref, basis_ref, outer_ref, conc_out, pots_out, flag_ref, conc_ref, pots_ref, sems
):
    rows, ys, width = conc_ref.shape
    nodes = pots_ref.shape[2] - 1
    half = rows * nodes
    side = 16
    total = jnp.sum(sums_ref[...], axis=0, keepdims=True)
    shape = (side, LANES)
    row = lax.broadcasted_iota(jnp.int32, shape, 0)
    col = lanes_of(shape)
    small = jnp.minimum(row, col)
    large = jnp.maximum(row, col)
    index = small * KV - (small * (small - 1)) // 2 + (large - small)
    valid = (row < KV) & (col < KV)
    index = jnp.where(valid, index, 0)
    gram = jnp.where(valid, pick(jnp.broadcast_to(total, shape), index), 0.0)

    def sub_sum(value):
        return jnp.sum(value, axis=0, keepdims=True)

    def full(value):
        return jnp.broadcast_to(value, shape)

    grams = [full(gram[:, k : k + 1]) for k in range(KV)]
    diag = jnp.zeros(shape, jnp.float32)
    for k in range(KV):
        diag = jnp.where(row == k, grams[k], diag)
    shifted_grams = [CENTER * grams[0] + HALF * grams[1]]
    for k in range(1, ITERS):
        shifted_grams.append(CENTER * grams[k] + (0.5 * HALF) * (grams[k - 1] + grams[k + 1]))
    norm0 = gram[0:1, 0:1]
    start = full(norm0) + epsilon
    inverse = lax.rsqrt(start)
    beta = (start * inverse)[0:1]
    coeffs = [jnp.where(row == 0, inverse, 0.0)]
    images = [grams[0] * inverse]
    columns = []
    worst = jnp.zeros((1, LANES), jnp.float32)
    for step in range(ITERS):
        q = coeffs[step]
        entries = [full(q[k : k + 1]) for k in range(step + 1)]
        down = pltpu.roll(q, 1, 0)
        up = jnp.where(row < side - 1, pltpu.roll(q, side - 1, 0), 0.0)
        w = CENTER * q + (0.5 * HALF) * (down + up)
        w = w + jnp.where(row == 1, (0.5 * HALF) * entries[0], 0.0)
        g = tree_sum([shifted_grams[k] * entries[k] for k in range(step + 1)])
        heads = [sub_sum(coeffs[i] * g) for i in range(step + 1)]
        wide = [full(value) for value in heads]
        u = w - tree_sum([wide[i] * coeffs[i] for i in range(step + 1)])
        gu = g - tree_sum([wide[i] * images[i] for i in range(step + 1)])
        square = sub_sum(u * gu) + epsilon
        inverse = lax.rsqrt(square)
        columns.append(heads + [square * inverse])
        inverse = full(inverse)
        coeffs.append(u * inverse)
        images.append(gu * inverse)
        worst = jnp.maximum(worst, sub_sum(coeffs[-1] * coeffs[-1] * diag))
    good = (worst < INVERSE_MAX) & (norm0 > NORM_MIN)
    weights = least_squares(columns, beta)
    mix = tree_sum([full(weights[step]) * coeffs[step] for step in range(ITERS)])
    bad = jnp.where(good & (jnp.abs(sub_sum(mix)) < 1e30), 0, 1)
    flag_ref[0] = jnp.max(bad)
    parts = [jnp.broadcast_to(mix[k : k + 1], (ys, LANES)) for k in range(ITERS)]

    def combine(ref, at):
        value = parts[0] * ref[(0, *at)]
        for k in range(1, ITERS):
            value = value + parts[k] * ref[(k, *at)]
        return value

    last = combine(outer_ref, (8,))
    for x in range(rows):
        pots_ref[x] = jnp.concatenate(
            [
                last[:, x * nodes : (x + 1) * nodes],
                last[:, half + x * nodes : half + x * nodes + 1],
            ],
            axis=1,
        )
    copies = [pltpu.make_async_copy(pots_ref, pots_out, sems.at[0])]
    copies[0].start()
    reached = lax.broadcasted_iota(jnp.int32, (16, LANES), 0) >= 16 - ITERS
    for group in range(4):
        pieces = []
        for at in (2 * group, 2 * group + 1):
            for base in range(0, NR - 16, 16):
                pieces.append(combine(basis_ref, (at, slice(base, base + 16))))
            pieces.append(
                jnp.where(
                    reached,
                    combine(outer_ref, (at,)),
                    combine(basis_ref, (at, slice(NR - 16, NR))),
                )
            )
        cells = jnp.concatenate(pieces, axis=0).T
        for slot in range(nodes // 8):
            tile = 4 * slot + group
            for x in range(rows):
                start = (slot * rows + x) * ys
                conc_ref[x, :, tile * LANES : (tile + 1) * LANES] = cells[start : start + ys]
            view = (slice(None), slice(None), slice(tile * LANES, (tile + 1) * LANES))
            copy = pltpu.make_async_copy(conc_ref.at[view], conc_out.at[view], sems.at[1 + tile])
            copy.start()
            copies.append(copy)
    for copy in copies:
        copy.wait()


def tree_sum(values):
    while len(values) > 1:
        values = [
            values[i] + values[i + 1] if i + 1 < len(values) else values[i]
            for i in range(0, len(values), 2)
        ]
    return values[0]


def least_squares(columns, start_norm):
    count = len(columns)
    target = [start_norm] + [jnp.zeros_like(start_norm) for step in range(count)]
    cosines = []
    sines = []
    upper_rows = []
    inverses = []
    for step in range(count):
        entries = list(columns[step])
        for row in range(step):
            first = cosines[row] * entries[row] + sines[row] * entries[row + 1]
            second = cosines[row] * entries[row + 1] - sines[row] * entries[row]
            entries[row] = first
            entries[row + 1] = second
        inverse = lax.rsqrt(entries[step] * entries[step] + entries[step + 1] * entries[step + 1])
        cosine = entries[step] * inverse
        sine = entries[step + 1] * inverse
        inverses.append(inverse)
        cosines.append(cosine)
        sines.append(sine)
        lead = target[step]
        target[step] = cosine * lead
        target[step + 1] = -sine * lead
        upper_rows.append(entries[:step])
    weights = [None] * count
    for row in range(count - 1, -1, -1):
        total = target[row]
        for later in range(count - 1, row, -1):
            total = total - upper_rows[later][row] * weights[later]
        weights[row] = total * inverses[row]
    return weights


def shifted(cells, axis, dim):
    count = lax.axis_size(axis)
    size = cells.shape[dim]
    head = lax.slice_in_dim(cells, 0, 1, axis=dim)
    tail = lax.slice_in_dim(cells, size - 1, size, axis=dim)
    before = lax.ppermute(tail, axis, [(i, i + 1) for i in range(count - 1)])
    after = lax.ppermute(head, axis, [(i + 1, i) for i in range(count - 1)])
    padded = jnp.concatenate([before, cells, after], axis=dim)
    return lax.slice_in_dim(padded, 0, size, axis=dim), lax.slice_in_dim(padded, 2, size + 2, axis=dim)


def mirror_laplace(values):
    inner = jnp.concatenate([values[..., :1], values[..., :-1]], axis=-1)
    outer = jnp.concatenate([values[..., 1:], values[..., -1:]], axis=-1)
    return 2.0 * values - inner - outer


def local_operator(conc, pots, diffusion, exchange, slope):
    nodes = exchange.shape[2]
    shells = conc.reshape(conc.shape[0], conc.shape[1], nodes, NR)
    xm, xp = shifted(pots, "gx", 0)
    ym, yp = shifted(pots, "gy", 1)
    lateral = 4.0 * pots - xm - xp - ym - yp
    node_pot = pots[..., :nodes]
    current = exchange * (node_pot - pots[..., nodes:])
    flag = (lax.broadcasted_iota(jnp.int32, (NR,), 0) == NR - 1).astype(jnp.float32)
    new_shells = shells + diffusion[..., None] * mirror_laplace(shells) + current[..., None] * flag
    new_nodes = (
        node_cond * mirror_laplace(node_pot)
        + current
        - slope * shells[..., NR - 1]
        + plane_cond * lateral[..., :nodes]
    )
    new_collector = collector_cond * lateral[..., nodes:] - jnp.mean(current, axis=-1, keepdims=True)
    return new_shells.reshape(conc.shape), jnp.concatenate([new_nodes, new_collector], axis=-1)


def weights_kernel(hess_ref, out_ref):
    def entry(i, j):
        return hess_ref[j, i : i + 1, 0:1]

    columns = [[entry(i, j) for i in range(j + 2)] for j in range(ITERS)]
    start = hess_ref[ITERS, 0:1, 0:1]
    for k, weight in enumerate(least_squares(columns, start)):
        out_ref[k : k + 1, :] = jnp.broadcast_to(weight, (1, LANES))


def plain_cycle(rhs_conc, rhs_pots, diffusion, exchange, slope):
    axes = ("gx", "gy")
    square = jnp.sum(rhs_conc * rhs_conc) + jnp.sum(rhs_pots * rhs_pots)
    start = jnp.sqrt(lax.psum(square, axes) + epsilon)
    basis_c = jnp.zeros((KV,) + rhs_conc.shape, jnp.float32).at[0].set(rhs_conc / start)
    basis_p = jnp.zeros((KV,) + rhs_pots.shape, jnp.float32).at[0].set(rhs_pots / start)
    hess = jnp.zeros((KV, 16), jnp.float32).at[ITERS, 0].set(start)
    spot = jnp.arange(16)

    def body(step, carry):
        basis_c, basis_p, hess = carry
        conc = lax.dynamic_index_in_dim(basis_c, step, 0, False)
        pots = lax.dynamic_index_in_dim(basis_p, step, 0, False)
        image_c, image_p = local_operator(conc, pots, diffusion, exchange, slope)
        dots = jnp.sum(basis_c * image_c, axis=(1, 2, 3)) + jnp.sum(basis_p * image_p, axis=(1, 2, 3))
        dots = lax.psum(dots, axes)
        rest_c = image_c - jnp.sum(dots[:, None, None, None] * basis_c, axis=0)
        rest_p = image_p - jnp.sum(dots[:, None, None, None] * basis_p, axis=0)
        square = lax.psum(jnp.sum(rest_c * rest_c) + jnp.sum(rest_p * rest_p), axes)
        height = jnp.sqrt(square + epsilon)
        basis_c = lax.dynamic_update_index_in_dim(basis_c, rest_c / height, step + 1, 0)
        basis_p = lax.dynamic_update_index_in_dim(basis_p, rest_p / height, step + 1, 0)
        line = jnp.concatenate([dots, jnp.zeros((16 - KV,), jnp.float32)])
        line = jnp.where(spot == step + 1, height, line)
        hess = lax.dynamic_update_index_in_dim(hess, line, step, 0)
        return basis_c, basis_p, hess

    basis_c, basis_p, hess = lax.fori_loop(0, ITERS, body, (basis_c, basis_p, hess))
    wide = jnp.broadcast_to(hess[:, :, None], hess.shape + (LANES,))
    weights = pl.pallas_call(
        weights_kernel, out_shape=jax.ShapeDtypeStruct((16, LANES), jnp.float32)
    )(wide)[:KV, 0]
    weights = jnp.where(jnp.arange(KV) < ITERS, weights, 0.0)[:, None, None, None]
    return jnp.sum(weights * basis_c, axis=0), jnp.sum(weights * basis_p, axis=0)


def shards(rhs_conc, rhs_pots, diffusion, exchange, slope):
    rows, ys, nodes = exchange.shape
    gx, gy = lax.axis_size("gx"), lax.axis_size("gy")
    half = rows * nodes
    pairs = FIELDS // 2
    assert half * 2 == LANES and nodes * NR == rhs_conc.shape[2]
    assert ys == 16 and ITERS <= ys and gx % 2 == 0
    assert half * 2 == rows * nodes // 8 * ys and LANES == 2 * NR
    window = 8 * ((ys + 2 * ITERS + 1 + 7) // 8)
    f32 = jnp.float32
    vmem = pl.BlockSpec(memory_space=pltpu.VMEM)
    smem = pl.BlockSpec(memory_space=pltpu.SMEM)
    hbm = pl.BlockSpec(memory_space=pltpu.HBM)
    params = pltpu.CompilerParams(vmem_limit_bytes=24 << 20)

    send, up, down, conc_copy, diff_copy = pl.pallas_call(
        pack_kernel,
        out_shape=(
            jax.ShapeDtypeStruct((pairs * ys, LANES), f32),
            jax.ShapeDtypeStruct((EDGE, LANES), f32),
            jax.ShapeDtypeStruct((EDGE, LANES), f32),
            jax.ShapeDtypeStruct(rhs_conc.shape, f32),
            jax.ShapeDtypeStruct(diffusion.shape, f32),
        ),
        compiler_params=params,
    )(rhs_conc, rhs_pots, diffusion, exchange, slope)
    even = lax.axis_index("gy") % 2 == 0
    swaps = [
        [pair for i in range(first, gy - 1, 2) for pair in ((i, i + 1), (i + 1, i))]
        for first in (0, 1)
    ]
    one = lax.ppermute(jnp.where(even, up, down), "gy", swaps[0])
    two = lax.ppermute(jnp.where(even, down, up), "gy", swaps[1])
    basis, coefs, deep, inner_gram = pl.pallas_call(
        free_kernel,
        out_shape=(
            jax.ShapeDtypeStruct((ITERS, 8, NR, LANES), f32),
            jax.ShapeDtypeStruct((2, 8, LANES), f32),
            jax.ShapeDtypeStruct((ys, LANES), f32),
            jax.ShapeDtypeStruct((8, LANES), f32),
        ),
        scratch_shapes=[
            pltpu.VMEM((8, NR, LANES), f32),
            pltpu.VMEM((LANES, 8, LANES), f32),
        ],
        compiler_params=params,
        cost_estimate=pl.CostEstimate(flops=20000000, transcendentals=0, bytes_accessed=3000000),
    )(conc_copy, diff_copy)
    one, two, inner_gram = lax.optimization_barrier((one, two, inner_gram))
    left, right = jnp.where(even, two, one), jnp.where(even, one, two)
    block = jnp.concatenate([send, left, right], axis=0)
    everything = lax.all_gather(block, "gx", axis=0, tiled=False)
    spot = lax.axis_index("gx").astype(jnp.int32).reshape(1)

    quads = gx // 2
    outer, gram = pl.pallas_call(
        functools.partial(powers_kernel, rows=rows, nodes=nodes),
        in_specs=[smem] + [vmem] * 5,
        out_specs=(vmem, vmem),
        out_shape=(
            jax.ShapeDtypeStruct((ITERS, 9, 16, LANES), f32),
            jax.ShapeDtypeStruct((gx * gy, LANES), f32),
        ),
        scratch_shapes=[
            pltpu.VMEM((2, quads, window, LANES), f32),
            pltpu.VMEM((2, quads, window, LANES), f32),
            pltpu.VMEM((2, SHELLS + 1, quads, window, LANES), f32),
            pltpu.VMEM((3, quads, window, LANES), f32),
            pltpu.VMEM((quads, window, LANES), f32),
            pltpu.VMEM((quads, window, LANES), f32),
            pltpu.VMEM((LANES * pl.cdiv(ITERS * ys, LANES), LANES), f32),
            pltpu.VMEM((9, 16, LANES), f32),
            pltpu.VMEM((LANES, 8, LANES), f32),
        ],
        compiler_params=params,
    )(spot, everything, basis, coefs, deep, inner_gram)

    sums = lax.all_to_all(gram, ("gx", "gy"), 0, 0, tiled=True)

    conc, pots, flag = pl.pallas_call(
        solve_kernel,
        out_shape=(
            jax.ShapeDtypeStruct(rhs_conc.shape, f32),
            jax.ShapeDtypeStruct(rhs_pots.shape, f32),
            jax.ShapeDtypeStruct((1,), jnp.int32),
        ),
        out_specs=(hbm, hbm, smem),
        scratch_shapes=[
            pltpu.VMEM(rhs_conc.shape, f32),
            pltpu.VMEM(rhs_pots.shape, f32),
            pltpu.SemaphoreType.DMA((1 + nodes * NR // LANES,)),
        ],
        compiler_params=params,
    )(sums, basis, outer)
    return lax.while_loop(
        lambda carry: carry[0] > 0,
        lambda carry: (0, *plain_cycle(rhs_conc, rhs_pots, diffusion, exchange, slope)),
        (flag[0], conc, pots),
    )[1:]


def solution(mesh):
    spec = P("gx", "gy", None)
    return jax.shard_map(
        shards, mesh=mesh, in_specs=(spec,) * 5, out_specs=(spec, spec), check_vma=False
    )
```

```python
import functools

import jax
import jax.numpy as jnp
from jax import lax
from jax.experimental import pallas as pl
from jax.experimental.pallas import tpu as pltpu
from jax.sharding import PartitionSpec as P

ITERS = 10
NR = 64
LANES = 128

node_cond = 1.0
plane_cond = 0.5
collector_cond = 2.0
epsilon = 1e-06

CENTER = 10.45
HALF = 9.55
INVERSE_MAX = 2.0e3
NORM_MIN = 1.0

KV = ITERS + 1
PAIRS = KV * (KV + 1) // 2
SHELLS = ITERS - 1
FIELDS = 5 + SHELLS
REACHES = [ITERS, SHELLS, SHELLS] + [SHELLS - k for k in range(1, SHELLS, 2)]
STARTS = [sum(REACHES[:pair]) for pair in range(len(REACHES))]
EDGE = sum(REACHES)


def lanes_of(shape):
    return lax.broadcasted_iota(jnp.int32, shape, len(shape) - 1)


def pick(values, index):
    return jnp.take_along_axis(values, index, axis=1, mode="promise_in_bounds")


def pack_kernel(
    conc_ref, pots_ref, diff_ref, exch_ref, slope_ref, send_ref, up_ref, down_ref, copy_ref, spread_ref
):
    rows, ys, nodes = exch_ref.shape
    half = rows * nodes
    lane = lanes_of((ys, LANES))
    low = lane < half
    copy_ref[...] = conc_ref[...]
    for x in range(rows):
        spread_ref[x] = diff_ref[x]

    def join(ref):
        return [ref[x][:, :nodes] for x in range(rows)]

    collector = [
        jnp.broadcast_to(pots_ref[x][:, nodes : nodes + 1], (ys, nodes)) for x in range(rows)
    ]
    slope = join(slope_ref)
    packed = [
        jnp.concatenate(join(pots_ref) + collector, axis=1),
        jnp.concatenate(join(diff_ref) + join(exch_ref), axis=1),
        jnp.where(low, jnp.concatenate(slope + slope, axis=1), outer_shells(conc_ref, nodes, 0, 0)),
    ]
    packed += [outer_shells(conc_ref, nodes, k, k + 1) for k in range(1, SHELLS, 2)]
    for pair, (value, reach, start) in enumerate(zip(packed, REACHES, STARTS)):
        send_ref[pair * ys : (pair + 1) * ys, :] = value
        up_ref[start : start + reach, :] = value[ys - reach :]
        down_ref[start : start + reach, :] = value[:reach]


def outer_shells(conc_ref, nodes, near, far):
    rows, ys, width = conc_ref.shape
    half = rows * nodes
    lane = lanes_of((ys, LANES))
    node = lane % half
    index = (node % 2) * NR + (NR - 1 - near) - jnp.where(lane < half, 0, far - near)
    found = jnp.zeros((ys, LANES), jnp.float32)
    for x in range(rows):
        for tile in range(width // LANES):
            cells = conc_ref[x, :, tile * LANES : (tile + 1) * LANES]
            here = (node // 2) == (x * nodes // 2 + tile)
            found = jnp.where(here, pick(cells, index), found)
    return found


GAIN = 2.0 / HALF
KEEP = GAIN * (1.0 - CENTER)


def add_gram(cells, lead_mask, acc_ref):
    pair = 0
    for i in range(KV):
        lead = cells[i] if lead_mask is None else cells[i] * lead_mask
        for j in range(i, KV):
            product = lead * cells[j]
            if product.shape[0] == 16:
                product = product[:8] + product[8:]
            acc_ref[pair] += product
            pair += 1


def lane_totals(acc_ref, count):
    sums = jnp.sum(acc_ref[...], axis=1)
    return lax.dot_general(
        jnp.ones((count, LANES), jnp.float32), sums, (((1,), (1,)), ((), ())),
        precision=lax.Precision.HIGHEST, preferred_element_type=jnp.float32,
    )


def turn_nodes(turned, at, rows, ys, nodes):
    lane = lanes_of((8, LANES))
    result = jnp.zeros((8, LANES), jnp.float32)
    for slot in range(nodes // 8):
        for x in range(rows):
            start = x * nodes + 8 * slot
            place = (slot * rows + x) * ys
            piece = pltpu.roll(turned[start : start + 8, :], (place - at) % LANES, 1)
            result = jnp.where((lane >= place) & (lane < place + ys), piece, result)
    return result


def free_kernel(conc_ref, diff_ref, basis_ref, coef_ref, deep_ref, gram_ref, last_ref, acc_ref):
    rows, ys, nodes = diff_ref.shape
    slots = nodes // 8
    deep_ref[...] = outer_shells(conc_ref, nodes, SHELLS, SHELLS)
    spread = jnp.concatenate([diff_ref[x] for x in range(rows)] * 2, axis=1)
    spread = jnp.concatenate([spread] * (LANES // ys), axis=0)
    gain = GAIN * turn_nodes(spread.T, 0, rows, ys, nodes)
    coef_ref[0] = gain
    coef_ref[1] = KEEP + 2.0 * gain
    for group in range(4):
        cells = jnp.concatenate(
            [
                conc_ref[x, :, (4 * slot + group) * LANES : (4 * slot + group + 1) * LANES]
                for slot in range(slots)
                for x in range(rows)
            ],
            axis=0,
        ).T
        for upper in range(LANES // NR):
            basis_ref[0, 2 * group + upper] = cells[upper * NR : (upper + 1) * NR]
    sub = lax.broadcasted_iota(jnp.int32, (8, LANES), 0)

    def image(step, row, base):
        now = basis_ref[step, row, base : base + 8, :]
        if base == 0:
            prev = jnp.where(sub == 0, now, pltpu.roll(now, 1, 0))
        else:
            prev = basis_ref[step, row, base - 1 : base + 7, :]
        if base == NR - 8:
            following = jnp.where(sub == 7, now, pltpu.roll(now, 7, 0))
        else:
            following = basis_ref[step, row, base + 1 : base + 9, :]
        gain = jnp.broadcast_to(coef_ref[0, row : row + 1, :], (8, LANES))
        keep = jnp.broadcast_to(coef_ref[1, row : row + 1, :], (8, LANES))
        return keep * now - gain * (prev + following)

    for row in range(8):
        for base in range(0, NR, 8):
            basis_ref[1, row, base : base + 8, :] = 0.5 * image(0, row, base)

    for step in range(1, ITERS - 1):
        for row in range(8):
            for base in range(0, NR, 8):
                basis_ref[step + 1, row, base : base + 8, :] = (
                    image(step, row, base) - basis_ref[step - 1, row, base : base + 8, :]
                )
    for row in range(8):
        for base in range(0, NR, 8):
            last_ref[row, base : base + 8, :] = (
                image(ITERS - 1, row, base) - basis_ref[ITERS - 2, row, base : base + 8, :]
            )

    def cells(row, start, stop):
        line = [basis_ref[k, row, start:stop, :] for k in range(ITERS)]
        return line + [last_ref[row, start:stop, :]]

    acc_ref[...] = jnp.zeros(acc_ref.shape, jnp.float32)
    inner = jnp.where(sub < 16 - ITERS, 1.0, 0.0)

    def gram_row(row, carry):
        for base in range(0, NR - 16, 16):
            add_gram(cells(row, base, base + 16), None, acc_ref)
        add_gram(cells(row, NR - 16, NR - 8), inner, acc_ref)
        return carry

    lax.fori_loop(0, 8, gram_row, 0)
    gram_ref[...] = lane_totals(acc_ref, 8)


def powers_kernel(
    spot_ref, all_ref, basis_ref, coeft_ref, deep_ref, inner_ref,
    outer_ref, gram_ref,
    pot_ref, col_ref, shell_ref, coef_ref, flow_ref, mean_ref, own_ref, tail_ref, acc_ref,
    *, rows, nodes,
):
    ys = deep_ref.shape[0]
    half = rows * nodes
    quads = all_ref.shape[0] // 2
    window = pot_ref.shape[2]
    spot = spot_ref[0]
    quad = spot // 2
    odd = (spot % 2) == 1
    lane2 = lanes_of((ys, LANES))
    low2 = lane2 < half
    head = (lane2 % nodes) == 0

    def room(field):
        if field < 2:
            return (pot_ref if field == 0 else col_ref).at[0]
        return coef_ref.at[field - 2] if field < 5 else shell_ref.at[0, field - 5]

    body = (FIELDS // 2) * ys
    for field in range(FIELDS):
        pair = field // 2
        reach, start = REACHES[pair], STARTS[pair]
        gap = (ys + reach, window - reach)
        scale = GAIN if field == 2 else 1.0
        for q in range(quads):
            room(field)[q, gap[0] : gap[1], :] = jnp.zeros((gap[1] - gap[0], LANES), jnp.float32)
            for place, origin, count in (
                (0, pair * ys, ys),
                (window - reach, body + start, reach),
                (ys, body + EDGE + start, reach),
            ):
                low = lanes_of((count, LANES)) < half
                a = all_ref[2 * q, origin : origin + count, :]
                b = all_ref[2 * q + 1, origin : origin + count, :]
                if field % 2 == 0:
                    value = jnp.where(low, a, pltpu.roll(b, half, 1))
                else:
                    value = jnp.where(low, pltpu.roll(a, half, 1), b)
                room(field)[q, place : place + count, :] = value * scale if field == 2 else value
    for q in range(quads):
        shell_ref[0, SHELLS, q] = jnp.zeros((window, LANES), jnp.float32)
    shell_ref[0, SHELLS, quad, 0:ys, :] = deep_ref[...]

    block = (lax.broadcasted_iota(jnp.int32, (LANES, LANES), 0) // nodes) == (
        lanes_of((LANES, LANES)) // nodes
    )
    mean_mat = jnp.where(block, 1.0 / nodes, 0.0).astype(jnp.bfloat16)
    def own_of(value):
        return jnp.where(odd, pltpu.roll(value, half, 1), value)

    def room_for(step):
        return outer_ref.at[step] if step < ITERS else tail_ref

    for step in range(KV):
        now, old = step % 2, (step + 1) % 2
        own_p = own_of(pot_ref[now, quad, 0:ys, :])
        own_v = own_of(col_ref[now, quad, 0:ys, :])
        room_for(step)[8] = jnp.where(
            low2, own_p, jnp.where(head, pltpu.roll(own_v, half, 1), 0.0)
        )
        if step == ITERS:
            break
        spans = [(0, window)] if step < 2 else [(0, ys + 8), (window - 8, window)]
        size = sum(stop - start for start, stop in spans)
        lane = lanes_of((size, LANES))

        def load(view):
            return jnp.concatenate([view[start:stop, :] for start, stop in spans], axis=0)

        def store(view, value):
            at = 0
            for start, stop in spans:
                view[start:stop, :] = value[at : at + stop - start]
                at += stop - start

        def around(ref, q):
            here = load(ref.at[now, q])
            following = load(ref.at[now, q + 1]) if q + 1 < quads else jnp.zeros_like(here)
            previous = load(ref.at[now, q - 1]) if q > 0 else jnp.zeros_like(here)
            xp = pltpu.roll(jnp.where(lane < nodes, following, here), LANES - nodes, 1)
            xm = pltpu.roll(jnp.where(lane >= LANES - nodes, previous, here), nodes, 1)
            return (xp + xm) + (pltpu.roll(here, size - 1, 0) + pltpu.roll(here, 1, 0))

        def finish(value, view):
            return 0.5 * value if step == 0 else value - load(view)

        for q in range(quads):
            flow = load(coef_ref.at[1, q]) * (load(pot_ref.at[now, q]) - load(col_ref.at[now, q]))
            store(flow_ref.at[q], flow)
            top = flow.astype(jnp.bfloat16)
            rest = flow - top.astype(jnp.float32)
            middle = rest.astype(jnp.bfloat16)
            rest = rest - middle.astype(jnp.float32)
            pieces = jnp.concatenate([top, middle, rest.astype(jnp.bfloat16)], axis=0)
            means = jnp.dot(pieces, mean_mat, preferred_element_type=jnp.float32)
            store(mean_ref.at[q], means[:size] + (means[size : 2 * size] + means[2 * size :]))
        wanted = SHELLS - step
        last = (lane % nodes) == (nodes - 1)
        for q in range(quads):
            flow = load(flow_ref.at[q])
            inside = load(coef_ref.at[1, q]) > 0.0
            diff = load(coef_ref.at[0, q])
            shell = load(shell_ref.at[now, 0, q])
            surface = shell
            fall_before = None
            for k in range(wanted):
                deeper = load(shell_ref.at[now, k + 1, q])
                fall = shell - deeper
                if k == 0:
                    value = KEEP * shell + (diff * fall + GAIN * flow)
                else:
                    value = KEEP * shell + diff * (fall - fall_before)
                view = shell_ref.at[old, k, q]
                store(view, finish(value, view))
                shell, fall_before = deeper, fall
            pots = load(pot_ref.at[now, q])
            drop = jnp.where(last, 0.0, pots - pltpu.roll(pots, LANES - 1, 1))
            value = (
                node_cond * (drop - pltpu.roll(drop, 1, 1))
                + (flow - load(coef_ref.at[2, q]) * surface)
                + (4.0 * plane_cond - CENTER) * pots
                - plane_cond * around(pot_ref, q)
            )
            view = pot_ref.at[old, q]
            store(view, jnp.where(inside, finish(GAIN * value, view), 0.0))
            coll = load(col_ref.at[now, q])
            value = (
                (4.0 * collector_cond - CENTER) * coll
                - collector_cond * around(col_ref, q)
                - load(mean_ref.at[q])
            )
            view = col_ref.at[old, q]
            store(view, jnp.where(inside, finish(GAIN * value, view), 0.0))
        own_ref[step * ys : (step + 1) * ys, :] = own_of(flow_ref[quad, 0:ys, :])

    own_ref[ITERS * ys :, :] = jnp.zeros((own_ref.shape[0] - ITERS * ys, LANES), jnp.float32)
    turned = [own_ref[at : at + LANES, :].T for at in range(0, own_ref.shape[0], LANES)]
    flows = [
        GAIN * turn_nodes(turned[step * ys // LANES], step * ys % LANES, rows, ys, nodes)
        for step in range(ITERS)
    ]
    tall = (16, LANES)
    sub = lax.broadcasted_iota(jnp.int32, tall, 0)
    for row in range(8):
        gain = jnp.broadcast_to(coeft_ref[0, row : row + 1, :], tall)
        keep = jnp.broadcast_to(coeft_ref[1, row : row + 1, :], tall)
        now, old = basis_ref[0, row, NR - 16 :, :], None
        outer_ref[0, row] = now
        for step in range(ITERS):
            above = jnp.broadcast_to(basis_ref[step, row, NR - 17 : NR - 16, :], tall)
            prev = jnp.where(sub == 0, above, pltpu.roll(now, 1, 0))
            following = jnp.where(sub == 15, now, pltpu.roll(now, 15, 0))
            flow = jnp.broadcast_to(flows[step][row : row + 1, :], tall)
            value = keep * now - gain * (prev + following) + jnp.where(sub == 15, flow, 0.0)
            value = 0.5 * value if step == 0 else value - old
            now, old = value, now
            room_for(step + 1)[row] = now

    acc_ref[...] = jnp.zeros(acc_ref.shape, jnp.float32)
    inside = jnp.where(lax.broadcasted_iota(jnp.int32, (16, LANES), 0) >= 16 - ITERS, 1.0, 0.0)

    def gram_row(at, carry):
        mask = jnp.where(at < 8, inside, 1.0)
        add_gram([outer_ref[k, at] for k in range(ITERS)] + [tail_ref[at]], mask, acc_ref)
        return carry

    lax.fori_loop(0, 9, gram_row, 0)
    total = lane_totals(acc_ref, gram_ref.shape[0])
    gram_ref[...] = total + jnp.broadcast_to(inner_ref[0:1, :], total.shape)


def solve_kernel(
    sums_ref, basis_ref, outer_ref, conc_out, pots_out, flag_ref, conc_ref, pots_ref, sems
):
    rows, ys, width = conc_ref.shape
    nodes = pots_ref.shape[2] - 1
    half = rows * nodes
    side = 16
    total = jnp.sum(sums_ref[...], axis=0, keepdims=True)
    shape = (side, LANES)
    row = lax.broadcasted_iota(jnp.int32, shape, 0)
    col = lanes_of(shape)
    small = jnp.minimum(row, col)
    large = jnp.maximum(row, col)
    index = small * KV - (small * (small - 1)) // 2 + (large - small)
    valid = (row < KV) & (col < KV)
    index = jnp.where(valid, index, 0)
    gram = jnp.where(valid, pick(jnp.broadcast_to(total, shape), index), 0.0)

    def sub_sum(value):
        return jnp.sum(value, axis=0, keepdims=True)

    def full(value):
        return jnp.broadcast_to(value, shape)

    grams = [full(gram[:, k : k + 1]) for k in range(KV)]
    diag = jnp.zeros(shape, jnp.float32)
    for k in range(KV):
        diag = jnp.where(row == k, grams[k], diag)
    shifted_grams = [CENTER * grams[0] + HALF * grams[1]]
    for k in range(1, ITERS):
        shifted_grams.append(CENTER * grams[k] + (0.5 * HALF) * (grams[k - 1] + grams[k + 1]))
    norm0 = gram[0:1, 0:1]
    start = full(norm0) + epsilon
    inverse = lax.rsqrt(start)
    beta = (start * inverse)[0:1]
    coeffs = [jnp.where(row == 0, inverse, 0.0)]
    images = [grams[0] * inverse]
    columns = []
    worst = jnp.zeros((1, LANES), jnp.float32)
    for step in range(ITERS):
        q = coeffs[step]
        entries = [full(q[k : k + 1]) for k in range(step + 1)]
        down = pltpu.roll(q, 1, 0)
        up = jnp.where(row < side - 1, pltpu.roll(q, side - 1, 0), 0.0)
        w = CENTER * q + (0.5 * HALF) * (down + up)
        w = w + jnp.where(row == 1, (0.5 * HALF) * entries[0], 0.0)
        g = tree_sum([shifted_grams[k] * entries[k] for k in range(step + 1)])
        heads = [sub_sum(coeffs[i] * g) for i in range(step + 1)]
        wide = [full(value) for value in heads]
        u = w - tree_sum([wide[i] * coeffs[i] for i in range(step + 1)])
        gu = g - tree_sum([wide[i] * images[i] for i in range(step + 1)])
        square = sub_sum(u * gu) + epsilon
        inverse = lax.rsqrt(square)
        columns.append(heads + [square * inverse])
        inverse = full(inverse)
        coeffs.append(u * inverse)
        images.append(gu * inverse)
        worst = jnp.maximum(worst, sub_sum(coeffs[-1] * coeffs[-1] * diag))
    good = (worst < INVERSE_MAX) & (norm0 > NORM_MIN)
    weights = least_squares(columns, beta)
    mix = tree_sum([full(weights[step]) * coeffs[step] for step in range(ITERS)])
    bad = jnp.where(good & (jnp.abs(sub_sum(mix)) < 1e30), 0, 1)
    flag_ref[0] = jnp.max(bad)
    parts = [jnp.broadcast_to(mix[k : k + 1], (ys, LANES)) for k in range(ITERS)]

    def combine(ref, at):
        value = parts[0] * ref[(0, *at)]
        for k in range(1, ITERS):
            value = value + parts[k] * ref[(k, *at)]
        return value

    last = combine(outer_ref, (8,))
    for x in range(rows):
        pots_ref[x] = jnp.concatenate(
            [
                last[:, x * nodes : (x + 1) * nodes],
                last[:, half + x * nodes : half + x * nodes + 1],
            ],
            axis=1,
        )
    copies = [pltpu.make_async_copy(pots_ref, pots_out, sems.at[0])]
    copies[0].start()
    reached = lax.broadcasted_iota(jnp.int32, (16, LANES), 0) >= 16 - ITERS
    for group in range(4):
        pieces = []
        for at in (2 * group, 2 * group + 1):
            for base in range(0, NR - 16, 16):
                pieces.append(combine(basis_ref, (at, slice(base, base + 16))))
            pieces.append(
                jnp.where(
                    reached,
                    combine(outer_ref, (at,)),
                    combine(basis_ref, (at, slice(NR - 16, NR))),
                )
            )
        cells = jnp.concatenate(pieces, axis=0).T
        for slot in range(nodes // 8):
            tile = 4 * slot + group
            for x in range(rows):
                start = (slot * rows + x) * ys
                conc_ref[x, :, tile * LANES : (tile + 1) * LANES] = cells[start : start + ys]
            view = (slice(None), slice(None), slice(tile * LANES, (tile + 1) * LANES))
            copy = pltpu.make_async_copy(conc_ref.at[view], conc_out.at[view], sems.at[1 + tile])
            copy.start()
            copies.append(copy)
    for copy in copies:
        copy.wait()


def tree_sum(values):
    while len(values) > 1:
        values = [
            values[i] + values[i + 1] if i + 1 < len(values) else values[i]
            for i in range(0, len(values), 2)
        ]
    return values[0]


def least_squares(columns, start_norm):
    count = len(columns)
    target = [start_norm] + [jnp.zeros_like(start_norm) for step in range(count)]
    cosines = []
    sines = []
    upper_rows = []
    inverses = []
    for step in range(count):
        entries = list(columns[step])
        for row in range(step):
            first = cosines[row] * entries[row] + sines[row] * entries[row + 1]
            second = cosines[row] * entries[row + 1] - sines[row] * entries[row]
            entries[row] = first
            entries[row + 1] = second
        inverse = lax.rsqrt(entries[step] * entries[step] + entries[step + 1] * entries[step + 1])
        cosine = entries[step] * inverse
        sine = entries[step + 1] * inverse
        inverses.append(inverse)
        cosines.append(cosine)
        sines.append(sine)
        lead = target[step]
        target[step] = cosine * lead
        target[step + 1] = -sine * lead
        upper_rows.append(entries[:step])
    weights = [None] * count
    for row in range(count - 1, -1, -1):
        total = target[row]
        for later in range(count - 1, row, -1):
            total = total - upper_rows[later][row] * weights[later]
        weights[row] = total * inverses[row]
    return weights


def shifted(cells, axis, dim):
    count = lax.axis_size(axis)
    size = cells.shape[dim]
    head = lax.slice_in_dim(cells, 0, 1, axis=dim)
    tail = lax.slice_in_dim(cells, size - 1, size, axis=dim)
    before = lax.ppermute(tail, axis, [(i, i + 1) for i in range(count - 1)])
    after = lax.ppermute(head, axis, [(i + 1, i) for i in range(count - 1)])
    padded = jnp.concatenate([before, cells, after], axis=dim)
    return lax.slice_in_dim(padded, 0, size, axis=dim), lax.slice_in_dim(padded, 2, size + 2, axis=dim)


def mirror_laplace(values):
    inner = jnp.concatenate([values[..., :1], values[..., :-1]], axis=-1)
    outer = jnp.concatenate([values[..., 1:], values[..., -1:]], axis=-1)
    return 2.0 * values - inner - outer


def local_operator(conc, pots, diffusion, exchange, slope):
    nodes = exchange.shape[2]
    shells = conc.reshape(conc.shape[0], conc.shape[1], nodes, NR)
    xm, xp = shifted(pots, "gx", 0)
    ym, yp = shifted(pots, "gy", 1)
    lateral = 4.0 * pots - xm - xp - ym - yp
    node_pot = pots[..., :nodes]
    current = exchange * (node_pot - pots[..., nodes:])
    flag = (lax.broadcasted_iota(jnp.int32, (NR,), 0) == NR - 1).astype(jnp.float32)
    new_shells = shells + diffusion[..., None] * mirror_laplace(shells) + current[..., None] * flag
    new_nodes = (
        node_cond * mirror_laplace(node_pot)
        + current
        - slope * shells[..., NR - 1]
        + plane_cond * lateral[..., :nodes]
    )
    new_collector = collector_cond * lateral[..., nodes:] - jnp.mean(current, axis=-1, keepdims=True)
    return new_shells.reshape(conc.shape), jnp.concatenate([new_nodes, new_collector], axis=-1)


def weights_kernel(hess_ref, out_ref):
    def entry(i, j):
        return hess_ref[j, i : i + 1, 0:1]

    columns = [[entry(i, j) for i in range(j + 2)] for j in range(ITERS)]
    start = hess_ref[ITERS, 0:1, 0:1]
    for k, weight in enumerate(least_squares(columns, start)):
        out_ref[k : k + 1, :] = jnp.broadcast_to(weight, (1, LANES))


def plain_cycle(rhs_conc, rhs_pots, diffusion, exchange, slope):
    axes = ("gx", "gy")
    square = jnp.sum(rhs_conc * rhs_conc) + jnp.sum(rhs_pots * rhs_pots)
    start = jnp.sqrt(lax.psum(square, axes) + epsilon)
    basis_c = jnp.zeros((KV,) + rhs_conc.shape, jnp.float32).at[0].set(rhs_conc / start)
    basis_p = jnp.zeros((KV,) + rhs_pots.shape, jnp.float32).at[0].set(rhs_pots / start)
    hess = jnp.zeros((KV, 16), jnp.float32).at[ITERS, 0].set(start)
    spot = jnp.arange(16)

    def body(step, carry):
        basis_c, basis_p, hess = carry
        conc = lax.dynamic_index_in_dim(basis_c, step, 0, False)
        pots = lax.dynamic_index_in_dim(basis_p, step, 0, False)
        image_c, image_p = local_operator(conc, pots, diffusion, exchange, slope)
        dots = jnp.sum(basis_c * image_c, axis=(1, 2, 3)) + jnp.sum(basis_p * image_p, axis=(1, 2, 3))
        dots = lax.psum(dots, axes)
        rest_c = image_c - jnp.sum(dots[:, None, None, None] * basis_c, axis=0)
        rest_p = image_p - jnp.sum(dots[:, None, None, None] * basis_p, axis=0)
        square = lax.psum(jnp.sum(rest_c * rest_c) + jnp.sum(rest_p * rest_p), axes)
        height = jnp.sqrt(square + epsilon)
        basis_c = lax.dynamic_update_index_in_dim(basis_c, rest_c / height, step + 1, 0)
        basis_p = lax.dynamic_update_index_in_dim(basis_p, rest_p / height, step + 1, 0)
        line = jnp.concatenate([dots, jnp.zeros((16 - KV,), jnp.float32)])
        line = jnp.where(spot == step + 1, height, line)
        hess = lax.dynamic_update_index_in_dim(hess, line, step, 0)
        return basis_c, basis_p, hess

    basis_c, basis_p, hess = lax.fori_loop(0, ITERS, body, (basis_c, basis_p, hess))
    wide = jnp.broadcast_to(hess[:, :, None], hess.shape + (LANES,))
    weights = pl.pallas_call(
        weights_kernel, out_shape=jax.ShapeDtypeStruct((16, LANES), jnp.float32)
    )(wide)[:KV, 0]
    weights = jnp.where(jnp.arange(KV) < ITERS, weights, 0.0)[:, None, None, None]
    return jnp.sum(weights * basis_c, axis=0), jnp.sum(weights * basis_p, axis=0)


def shards(rhs_conc, rhs_pots, diffusion, exchange, slope):
    rows, ys, nodes = exchange.shape
    gx, gy = lax.axis_size("gx"), lax.axis_size("gy")
    half = rows * nodes
    pairs = FIELDS // 2
    assert half * 2 == LANES and nodes * NR == rhs_conc.shape[2]
    assert ys == 16 and ITERS <= ys and gx % 2 == 0
    assert half * 2 == rows * nodes // 8 * ys and LANES == 2 * NR
    window = 8 * ((ys + 2 * ITERS + 1 + 7) // 8)
    f32 = jnp.float32
    vmem = pl.BlockSpec(memory_space=pltpu.VMEM)
    smem = pl.BlockSpec(memory_space=pltpu.SMEM)
    hbm = pl.BlockSpec(memory_space=pltpu.HBM)
    params = pltpu.CompilerParams(vmem_limit_bytes=24 << 20)

    send, up, down, conc_copy, diff_copy = pl.pallas_call(
        pack_kernel,
        out_shape=(
            jax.ShapeDtypeStruct((pairs * ys, LANES), f32),
            jax.ShapeDtypeStruct((EDGE, LANES), f32),
            jax.ShapeDtypeStruct((EDGE, LANES), f32),
            jax.ShapeDtypeStruct(rhs_conc.shape, f32),
            jax.ShapeDtypeStruct(diffusion.shape, f32),
        ),
        compiler_params=params,
    )(rhs_conc, rhs_pots, diffusion, exchange, slope)
    even = lax.axis_index("gy") % 2 == 0
    swaps = [
        [pair for i in range(first, gy - 1, 2) for pair in ((i, i + 1), (i + 1, i))]
        for first in (0, 1)
    ]
    one = lax.ppermute(jnp.where(even, up, down), "gy", swaps[0])
    two = lax.ppermute(jnp.where(even, down, up), "gy", swaps[1])
    basis, coefs, deep, inner_gram = pl.pallas_call(
        free_kernel,
        out_shape=(
            jax.ShapeDtypeStruct((ITERS, 8, NR, LANES), f32),
            jax.ShapeDtypeStruct((2, 8, LANES), f32),
            jax.ShapeDtypeStruct((ys, LANES), f32),
            jax.ShapeDtypeStruct((8, LANES), f32),
        ),
        scratch_shapes=[
            pltpu.VMEM((8, NR, LANES), f32),
            pltpu.VMEM((LANES, 8, LANES), f32),
        ],
        compiler_params=params,
        cost_estimate=pl.CostEstimate(flops=20000000, transcendentals=0, bytes_accessed=3000000),
    )(conc_copy, diff_copy)
    one, two, inner_gram = lax.optimization_barrier((one, two, inner_gram))
    left, right = jnp.where(even, two, one), jnp.where(even, one, two)
    block = jnp.concatenate([send, left, right], axis=0)
    everything = lax.all_gather(block, "gx", axis=0, tiled=False)
    spot = lax.axis_index("gx").astype(jnp.int32).reshape(1)

    quads = gx // 2
    outer, gram = pl.pallas_call(
        functools.partial(powers_kernel, rows=rows, nodes=nodes),
        in_specs=[smem] + [vmem] * 5,
        out_specs=(vmem, vmem),
        out_shape=(
            jax.ShapeDtypeStruct((ITERS, 9, 16, LANES), f32),
            jax.ShapeDtypeStruct((gx * gy, LANES), f32),
        ),
        scratch_shapes=[
            pltpu.VMEM((2, quads, window, LANES), f32),
            pltpu.VMEM((2, quads, window, LANES), f32),
            pltpu.VMEM((2, SHELLS + 1, quads, window, LANES), f32),
            pltpu.VMEM((3, quads, window, LANES), f32),
            pltpu.VMEM((quads, window, LANES), f32),
            pltpu.VMEM((quads, window, LANES), f32),
            pltpu.VMEM((LANES * pl.cdiv(ITERS * ys, LANES), LANES), f32),
            pltpu.VMEM((9, 16, LANES), f32),
            pltpu.VMEM((LANES, 8, LANES), f32),
        ],
        compiler_params=params,
    )(spot, everything, basis, coefs, deep, inner_gram)

    sums = lax.all_to_all(gram, ("gx", "gy"), 0, 0, tiled=True)

    conc, pots, flag = pl.pallas_call(
        solve_kernel,
        out_shape=(
            jax.ShapeDtypeStruct(rhs_conc.shape, f32),
            jax.ShapeDtypeStruct(rhs_pots.shape, f32),
            jax.ShapeDtypeStruct((1,), jnp.int32),
        ),
        out_specs=(hbm, hbm, smem),
        scratch_shapes=[
            pltpu.VMEM(rhs_conc.shape, f32),
            pltpu.VMEM(rhs_pots.shape, f32),
            pltpu.SemaphoreType.DMA((1 + nodes * NR // LANES,)),
        ],
        compiler_params=params,
    )(sums, basis, outer)
    return lax.while_loop(
        lambda carry: carry[0] > 0,
        lambda carry: (0, *plain_cycle(rhs_conc, rhs_pots, diffusion, exchange, slope)),
        (flag[0], conc, pots),
    )[1:]


def solution(mesh):
    spec = P("gx", "gy", None)
    return jax.shard_map(
        shards, mesh=mesh, in_specs=(spec,) * 5, out_specs=(spec, spec), check_vma=False
    )
```

```python
import functools

import jax
import jax.numpy as jnp
from jax import lax
from jax.experimental import pallas as pl
from jax.experimental.pallas import tpu as pltpu
from jax.sharding import PartitionSpec as P

ITERS = 10
NR = 64
LANES = 128

node_cond = 1.0
plane_cond = 0.5
collector_cond = 2.0
epsilon = 1e-06

CENTER = 10.45
HALF = 9.55
INVERSE_MAX = 2.0e3
NORM_MIN = 1.0

KV = ITERS + 1
PAIRS = KV * (KV + 1) // 2
SHELLS = ITERS - 1
FIELDS = 5 + SHELLS
REACHES = [ITERS, SHELLS, SHELLS] + [SHELLS - k for k in range(1, SHELLS, 2)]
STARTS = [sum(REACHES[:pair]) for pair in range(len(REACHES))]
EDGE = sum(REACHES)


def lanes_of(shape):
    return lax.broadcasted_iota(jnp.int32, shape, len(shape) - 1)


def pick(values, index):
    return jnp.take_along_axis(values, index, axis=1, mode="promise_in_bounds")


def pack_kernel(
    conc_ref, pots_ref, diff_ref, exch_ref, slope_ref, send_ref, up_ref, down_ref, copy_ref, spread_ref
):
    rows, ys, nodes = exch_ref.shape
    half = rows * nodes
    lane = lanes_of((ys, LANES))
    low = lane < half
    copy_ref[...] = conc_ref[...]
    for x in range(rows):
        spread_ref[x] = diff_ref[x]

    def join(ref):
        return [ref[x][:, :nodes] for x in range(rows)]

    collector = [
        jnp.broadcast_to(pots_ref[x][:, nodes : nodes + 1], (ys, nodes)) for x in range(rows)
    ]
    slope = join(slope_ref)
    packed = [
        jnp.concatenate(join(pots_ref) + collector, axis=1),
        jnp.concatenate(join(diff_ref) + join(exch_ref), axis=1),
        jnp.where(low, jnp.concatenate(slope + slope, axis=1), outer_shells(conc_ref, nodes, 0, 0)),
    ]
    packed += [outer_shells(conc_ref, nodes, k, k + 1) for k in range(1, SHELLS, 2)]
    for pair, (value, reach, start) in enumerate(zip(packed, REACHES, STARTS)):
        send_ref[pair * ys : (pair + 1) * ys, :] = value
        up_ref[start : start + reach, :] = value[ys - reach :]
        down_ref[start : start + reach, :] = value[:reach]


def outer_shells(conc_ref, nodes, near, far):
    rows, ys, width = conc_ref.shape
    half = rows * nodes
    lane = lanes_of((ys, LANES))
    node = lane % half
    index = (node % 2) * NR + (NR - 1 - near) - jnp.where(lane < half, 0, far - near)
    found = jnp.zeros((ys, LANES), jnp.float32)
    for x in range(rows):
        for tile in range(width // LANES):
            cells = conc_ref[x, :, tile * LANES : (tile + 1) * LANES]
            here = (node // 2) == (x * nodes // 2 + tile)
            found = jnp.where(here, pick(cells, index), found)
    return found


GAIN = 2.0 / HALF
KEEP = GAIN * (1.0 - CENTER)


def add_gram(cells, lead_mask, acc_ref):
    pair = 0
    for i in range(KV):
        lead = cells[i] if lead_mask is None else cells[i] * lead_mask
        for j in range(i, KV):
            product = lead * cells[j]
            if product.shape[0] == 16:
                product = product[:8] + product[8:]
            acc_ref[pair] += product
            pair += 1


def lane_totals(acc_ref, count):
    sums = jnp.sum(acc_ref[...], axis=1)
    return lax.dot_general(
        jnp.ones((count, LANES), jnp.float32), sums, (((1,), (1,)), ((), ())),
        precision=lax.Precision.HIGHEST, preferred_element_type=jnp.float32,
    )


def turn_nodes(turned, at, rows, ys, nodes):
    lane = lanes_of((8, LANES))
    result = jnp.zeros((8, LANES), jnp.float32)
    for slot in range(nodes // 8):
        for x in range(rows):
            start = x * nodes + 8 * slot
            place = (slot * rows + x) * ys
            piece = pltpu.roll(turned[start : start + 8, :], (place - at) % LANES, 1)
            result = jnp.where((lane >= place) & (lane < place + ys), piece, result)
    return result


def free_kernel(conc_ref, diff_ref, basis_ref, coef_ref, deep_ref, gram_ref, last_ref, acc_ref):
    rows, ys, nodes = diff_ref.shape
    slots = nodes // 8
    deep_ref[...] = outer_shells(conc_ref, nodes, SHELLS, SHELLS)
    spread = jnp.concatenate([diff_ref[x] for x in range(rows)] * 2, axis=1)
    spread = jnp.concatenate([spread] * (LANES // ys), axis=0)
    gain = GAIN * turn_nodes(spread.T, 0, rows, ys, nodes)
    coef_ref[0] = gain
    coef_ref[1] = KEEP + 2.0 * gain
    for group in range(4):
        cells = jnp.concatenate(
            [
                conc_ref[x, :, (4 * slot + group) * LANES : (4 * slot + group + 1) * LANES]
                for slot in range(slots)
                for x in range(rows)
            ],
            axis=0,
        ).T
        for upper in range(LANES // NR):
            basis_ref[0, 2 * group + upper] = cells[upper * NR : (upper + 1) * NR]
    sub = lax.broadcasted_iota(jnp.int32, (8, LANES), 0)

    def image(step, row, base):
        now = basis_ref[step, row, base : base + 8, :]
        if base == 0:
            prev = jnp.where(sub == 0, now, pltpu.roll(now, 1, 0))
        else:
            prev = basis_ref[step, row, base - 1 : base + 7, :]
        if base == NR - 8:
            following = jnp.where(sub == 7, now, pltpu.roll(now, 7, 0))
        else:
            following = basis_ref[step, row, base + 1 : base + 9, :]
        gain = jnp.broadcast_to(coef_ref[0, row : row + 1, :], (8, LANES))
        keep = jnp.broadcast_to(coef_ref[1, row : row + 1, :], (8, LANES))
        return keep * now - gain * (prev + following)

    for row in range(8):
        for base in range(0, NR, 8):
            basis_ref[1, row, base : base + 8, :] = 0.5 * image(0, row, base)

    for step in range(1, ITERS - 1):
        for row in range(8):
            for base in range(0, NR, 8):
                basis_ref[step + 1, row, base : base + 8, :] = (
                    image(step, row, base) - basis_ref[step - 1, row, base : base + 8, :]
                )
    for row in range(8):
        for base in range(0, NR, 8):
            last_ref[row, base : base + 8, :] = (
                image(ITERS - 1, row, base) - basis_ref[ITERS - 2, row, base : base + 8, :]
            )

    def cells(row, start, stop):
        line = [basis_ref[k, row, start:stop, :] for k in range(ITERS)]
        return line + [last_ref[row, start:stop, :]]

    acc_ref[...] = jnp.zeros(acc_ref.shape, jnp.float32)
    inner = jnp.where(sub < 16 - ITERS, 1.0, 0.0)

    def gram_row(row, carry):
        for base in range(0, NR - 16, 16):
            add_gram(cells(row, base, base + 16), None, acc_ref)
        add_gram(cells(row, NR - 16, NR - 8), inner, acc_ref)
        return carry

    lax.fori_loop(0, 8, gram_row, 0)
    gram_ref[...] = lane_totals(acc_ref, 8)


def powers_kernel(
    spot_ref, all_ref, basis_ref, coeft_ref, deep_ref, inner_ref,
    outer_ref, gram_ref,
    pot_ref, col_ref, shell_ref, coef_ref, flow_ref, mean_ref, own_ref, tail_ref, acc_ref,
    *, rows, nodes,
):
    ys = deep_ref.shape[0]
    half = rows * nodes
    quads = all_ref.shape[0] // 2
    window = pot_ref.shape[2]
    spot = spot_ref[0]
    quad = spot // 2
    odd = (spot % 2) == 1
    lane2 = lanes_of((ys, LANES))
    low2 = lane2 < half
    head = (lane2 % nodes) == 0

    def room(field):
        if field < 2:
            return (pot_ref if field == 0 else col_ref).at[0]
        return coef_ref.at[field - 2] if field < 5 else shell_ref.at[0, field - 5]

    body = (FIELDS // 2) * ys
    for field in range(FIELDS):
        pair = field // 2
        reach, start = REACHES[pair], STARTS[pair]
        gap = (ys + reach, window - reach)
        scale = GAIN if field == 2 else 1.0
        for q in range(quads):
            room(field)[q, gap[0] : gap[1], :] = jnp.zeros((gap[1] - gap[0], LANES), jnp.float32)
            for place, origin, count in (
                (0, pair * ys, ys),
                (window - reach, body + start, reach),
                (ys, body + EDGE + start, reach),
            ):
                low = lanes_of((count, LANES)) < half
                a = all_ref[2 * q, origin : origin + count, :]
                b = all_ref[2 * q + 1, origin : origin + count, :]
                if field % 2 == 0:
                    value = jnp.where(low, a, pltpu.roll(b, half, 1))
                else:
                    value = jnp.where(low, pltpu.roll(a, half, 1), b)
                room(field)[q, place : place + count, :] = value * scale if field == 2 else value
    for q in range(quads):
        shell_ref[0, SHELLS, q] = jnp.zeros((window, LANES), jnp.float32)
    shell_ref[0, SHELLS, quad, 0:ys, :] = deep_ref[...]

    block = (lax.broadcasted_iota(jnp.int32, (LANES, LANES), 0) // nodes) == (
        lanes_of((LANES, LANES)) // nodes
    )
    mean_mat = jnp.where(block, 1.0 / nodes, 0.0).astype(jnp.bfloat16)
    def own_of(value):
        return jnp.where(odd, pltpu.roll(value, half, 1), value)

    def room_for(step):
        return outer_ref.at[step] if step < ITERS else tail_ref

    for step in range(KV):
        now, old = step % 2, (step + 1) % 2
        own_p = own_of(pot_ref[now, quad, 0:ys, :])
        own_v = own_of(col_ref[now, quad, 0:ys, :])
        room_for(step)[8] = jnp.where(
            low2, own_p, jnp.where(head, pltpu.roll(own_v, half, 1), 0.0)
        )
        if step == ITERS:
            break
        spans = [(0, window)] if step < 2 else [(0, ys + 8), (window - 8, window)]
        size = sum(stop - start for start, stop in spans)
        lane = lanes_of((size, LANES))

        def load(view):
            return jnp.concatenate([view[start:stop, :] for start, stop in spans], axis=0)

        def store(view, value):
            at = 0
            for start, stop in spans:
                view[start:stop, :] = value[at : at + stop - start]
                at += stop - start

        def around(ref, q):
            here = load(ref.at[now, q])
            following = load(ref.at[now, q + 1]) if q + 1 < quads else jnp.zeros_like(here)
            previous = load(ref.at[now, q - 1]) if q > 0 else jnp.zeros_like(here)
            xp = pltpu.roll(jnp.where(lane < nodes, following, here), LANES - nodes, 1)
            xm = pltpu.roll(jnp.where(lane >= LANES - nodes, previous, here), nodes, 1)
            return (xp + xm) + (pltpu.roll(here, size - 1, 0) + pltpu.roll(here, 1, 0))

        def finish(value, view):
            return 0.5 * value if step == 0 else value - load(view)

        for q in range(quads):
            flow = load(coef_ref.at[1, q]) * (load(pot_ref.at[now, q]) - load(col_ref.at[now, q]))
            store(flow_ref.at[q], flow)
            top = flow.astype(jnp.bfloat16)
            rest = flow - top.astype(jnp.float32)
            middle = rest.astype(jnp.bfloat16)
            rest = rest - middle.astype(jnp.float32)
            pieces = jnp.concatenate([top, middle, rest.astype(jnp.bfloat16)], axis=0)
            means = jnp.dot(pieces, mean_mat, preferred_element_type=jnp.float32)
            store(mean_ref.at[q], means[:size] + (means[size : 2 * size] + means[2 * size :]))
        wanted = SHELLS - step
        last = (lane % nodes) == (nodes - 1)
        for q in range(quads):
            flow = load(flow_ref.at[q])
            inside = load(coef_ref.at[1, q]) > 0.0
            diff = load(coef_ref.at[0, q])
            shell = load(shell_ref.at[now, 0, q])
            surface = shell
            fall_before = None
            for k in range(wanted):
                deeper = load(shell_ref.at[now, k + 1, q])
                fall = shell - deeper
                if k == 0:
                    value = KEEP * shell + (diff * fall + GAIN * flow)
                else:
                    value = KEEP * shell + diff * (fall - fall_before)
                view = shell_ref.at[old, k, q]
                store(view, finish(value, view))
                shell, fall_before = deeper, fall
            pots = load(pot_ref.at[now, q])
            drop = jnp.where(last, 0.0, pots - pltpu.roll(pots, LANES - 1, 1))
            value = (
                node_cond * (drop - pltpu.roll(drop, 1, 1))
                + (flow - load(coef_ref.at[2, q]) * surface)
                + (4.0 * plane_cond - CENTER) * pots
                - plane_cond * around(pot_ref, q)
            )
            view = pot_ref.at[old, q]
            store(view, jnp.where(inside, finish(GAIN * value, view), 0.0))
            coll = load(col_ref.at[now, q])
            value = (
                (4.0 * collector_cond - CENTER) * coll
                - collector_cond * around(col_ref, q)
                - load(mean_ref.at[q])
            )
            view = col_ref.at[old, q]
            store(view, jnp.where(inside, finish(GAIN * value, view), 0.0))
        own_ref[step * ys : (step + 1) * ys, :] = own_of(flow_ref[quad, 0:ys, :])

    own_ref[ITERS * ys :, :] = jnp.zeros((own_ref.shape[0] - ITERS * ys, LANES), jnp.float32)
    turned = [own_ref[at : at + LANES, :].T for at in range(0, own_ref.shape[0], LANES)]
    flows = [
        GAIN * turn_nodes(turned[step * ys // LANES], step * ys % LANES, rows, ys, nodes)
        for step in range(ITERS)
    ]
    tall = (16, LANES)
    sub = lax.broadcasted_iota(jnp.int32, tall, 0)
    for row in range(8):
        gain = jnp.broadcast_to(coeft_ref[0, row : row + 1, :], tall)
        keep = jnp.broadcast_to(coeft_ref[1, row : row + 1, :], tall)
        now, old = basis_ref[0, row, NR - 16 :, :], None
        outer_ref[0, row] = now
        for step in range(ITERS):
            above = jnp.broadcast_to(basis_ref[step, row, NR - 17 : NR - 16, :], tall)
            prev = jnp.where(sub == 0, above, pltpu.roll(now, 1, 0))
            following = jnp.where(sub == 15, now, pltpu.roll(now, 15, 0))
            flow = jnp.broadcast_to(flows[step][row : row + 1, :], tall)
            value = keep * now - gain * (prev + following) + jnp.where(sub == 15, flow, 0.0)
            value = 0.5 * value if step == 0 else value - old
            now, old = value, now
            room_for(step + 1)[row] = now

    acc_ref[...] = jnp.zeros(acc_ref.shape, jnp.float32)
    inside = jnp.where(lax.broadcasted_iota(jnp.int32, (16, LANES), 0) >= 16 - ITERS, 1.0, 0.0)

    def gram_row(at, carry):
        mask = jnp.where(at < 8, inside, 1.0)
        add_gram([outer_ref[k, at] for k in range(ITERS)] + [tail_ref[at]], mask, acc_ref)
        return carry

    lax.fori_loop(0, 9, gram_row, 0)
    total = lane_totals(acc_ref, gram_ref.shape[0])
    gram_ref[...] = total + jnp.broadcast_to(inner_ref[0:1, :], total.shape)


def solve_kernel(
    sums_ref, basis_ref, outer_ref, conc_out, pots_out, flag_ref, conc_ref, pots_ref, sems
):
    rows, ys, width = conc_ref.shape
    nodes = pots_ref.shape[2] - 1
    half = rows * nodes
    side = 16
    total = jnp.sum(sums_ref[...], axis=0, keepdims=True)
    shape = (side, LANES)
    row = lax.broadcasted_iota(jnp.int32, shape, 0)
    col = lanes_of(shape)
    small = jnp.minimum(row, col)
    large = jnp.maximum(row, col)
    index = small * KV - (small * (small - 1)) // 2 + (large - small)
    valid = (row < KV) & (col < KV)
    index = jnp.where(valid, index, 0)
    gram = jnp.where(valid, pick(jnp.broadcast_to(total, shape), index), 0.0)

    def sub_sum(value):
        return jnp.sum(value, axis=0, keepdims=True)

    def full(value):
        return jnp.broadcast_to(value, shape)

    grams = [full(gram[:, k : k + 1]) for k in range(KV)]
    diag = jnp.zeros(shape, jnp.float32)
    for k in range(KV):
        diag = jnp.where(row == k, grams[k], diag)
    shifted_grams = [CENTER * grams[0] + HALF * grams[1]]
    for k in range(1, ITERS):
        shifted_grams.append(CENTER * grams[k] + (0.5 * HALF) * (grams[k - 1] + grams[k + 1]))
    norm0 = gram[0:1, 0:1]
    start = full(norm0) + epsilon
    inverse = lax.rsqrt(start)
    beta = (start * inverse)[0:1]
    coeffs = [jnp.where(row == 0, inverse, 0.0)]
    images = [grams[0] * inverse]
    columns = []
    worst = jnp.zeros((1, LANES), jnp.float32)
    for step in range(ITERS):
        q = coeffs[step]
        entries = [full(q[k : k + 1]) for k in range(step + 1)]
        down = pltpu.roll(q, 1, 0)
        up = jnp.where(row < side - 1, pltpu.roll(q, side - 1, 0), 0.0)
        w = CENTER * q + (0.5 * HALF) * (down + up)
        w = w + jnp.where(row == 1, (0.5 * HALF) * entries[0], 0.0)
        g = tree_sum([shifted_grams[k] * entries[k] for k in range(step + 1)])
        heads = [sub_sum(coeffs[i] * g) for i in range(step + 1)]
        wide = [full(value) for value in heads]
        u = w - tree_sum([wide[i] * coeffs[i] for i in range(step + 1)])
        gu = g - tree_sum([wide[i] * images[i] for i in range(step + 1)])
        square = sub_sum(u * gu) + epsilon
        inverse = lax.rsqrt(square)
        columns.append(heads + [square * inverse])
        inverse = full(inverse)
        coeffs.append(u * inverse)
        images.append(gu * inverse)
        worst = jnp.maximum(worst, sub_sum(coeffs[-1] * coeffs[-1] * diag))
    good = (worst < INVERSE_MAX) & (norm0 > NORM_MIN)
    weights = least_squares(columns, beta)
    mix = tree_sum([full(weights[step]) * coeffs[step] for step in range(ITERS)])
    bad = jnp.where(good & (jnp.abs(sub_sum(mix)) < 1e30), 0, 1)
    flag_ref[0] = jnp.max(bad)
    parts = [jnp.broadcast_to(mix[k : k + 1], (ys, LANES)) for k in range(ITERS)]

    def combine(ref, at):
        value = parts[0] * ref[(0, *at)]
        for k in range(1, ITERS):
            value = value + parts[k] * ref[(k, *at)]
        return value

    last = combine(outer_ref, (8,))
    for x in range(rows):
        pots_ref[x] = jnp.concatenate(
            [
                last[:, x * nodes : (x + 1) * nodes],
                last[:, half + x * nodes : half + x * nodes + 1],
            ],
            axis=1,
        )
    copies = [pltpu.make_async_copy(pots_ref, pots_out, sems.at[0])]
    copies[0].start()
    reached = lax.broadcasted_iota(jnp.int32, (16, LANES), 0) >= 16 - ITERS
    for group in range(4):
        pieces = []
        for at in (2 * group, 2 * group + 1):
            for base in range(0, NR - 16, 16):
                pieces.append(combine(basis_ref, (at, slice(base, base + 16))))
            pieces.append(
                jnp.where(
                    reached,
                    combine(outer_ref, (at,)),
                    combine(basis_ref, (at, slice(NR - 16, NR))),
                )
            )
        cells = jnp.concatenate(pieces, axis=0).T
        for slot in range(nodes // 8):
            tile = 4 * slot + group
            for x in range(rows):
                start = (slot * rows + x) * ys
                conc_ref[x, :, tile * LANES : (tile + 1) * LANES] = cells[start : start + ys]
            view = (slice(None), slice(None), slice(tile * LANES, (tile + 1) * LANES))
            copy = pltpu.make_async_copy(conc_ref.at[view], conc_out.at[view], sems.at[1 + tile])
            copy.start()
            copies.append(copy)
    for copy in copies:
        copy.wait()


def tree_sum(values):
    while len(values) > 1:
        values = [
            values[i] + values[i + 1] if i + 1 < len(values) else values[i]
            for i in range(0, len(values), 2)
        ]
    return values[0]


def least_squares(columns, start_norm):
    count = len(columns)
    target = [start_norm] + [jnp.zeros_like(start_norm) for step in range(count)]
    cosines = []
    sines = []
    upper_rows = []
    inverses = []
    for step in range(count):
        entries = list(columns[step])
        for row in range(step):
            first = cosines[row] * entries[row] + sines[row] * entries[row + 1]
            second = cosines[row] * entries[row + 1] - sines[row] * entries[row]
            entries[row] = first
            entries[row + 1] = second
        inverse = lax.rsqrt(entries[step] * entries[step] + entries[step + 1] * entries[step + 1])
        cosine = entries[step] * inverse
        sine = entries[step + 1] * inverse
        inverses.append(inverse)
        cosines.append(cosine)
        sines.append(sine)
        lead = target[step]
        target[step] = cosine * lead
        target[step + 1] = -sine * lead
        upper_rows.append(entries[:step])
    weights = [None] * count
    for row in range(count - 1, -1, -1):
        total = target[row]
        for later in range(count - 1, row, -1):
            total = total - upper_rows[later][row] * weights[later]
        weights[row] = total * inverses[row]
    return weights


def shifted(cells, axis, dim):
    count = lax.axis_size(axis)
    size = cells.shape[dim]
    head = lax.slice_in_dim(cells, 0, 1, axis=dim)
    tail = lax.slice_in_dim(cells, size - 1, size, axis=dim)
    before = lax.ppermute(tail, axis, [(i, i + 1) for i in range(count - 1)])
    after = lax.ppermute(head, axis, [(i + 1, i) for i in range(count - 1)])
    padded = jnp.concatenate([before, cells, after], axis=dim)
    return lax.slice_in_dim(padded, 0, size, axis=dim), lax.slice_in_dim(padded, 2, size + 2, axis=dim)


def mirror_laplace(values):
    inner = jnp.concatenate([values[..., :1], values[..., :-1]], axis=-1)
    outer = jnp.concatenate([values[..., 1:], values[..., -1:]], axis=-1)
    return 2.0 * values - inner - outer


def local_operator(conc, pots, diffusion, exchange, slope):
    nodes = exchange.shape[2]
    shells = conc.reshape(conc.shape[0], conc.shape[1], nodes, NR)
    xm, xp = shifted(pots, "gx", 0)
    ym, yp = shifted(pots, "gy", 1)
    lateral = 4.0 * pots - xm - xp - ym - yp
    node_pot = pots[..., :nodes]
    current = exchange * (node_pot - pots[..., nodes:])
    flag = (lax.broadcasted_iota(jnp.int32, (NR,), 0) == NR - 1).astype(jnp.float32)
    new_shells = shells + diffusion[..., None] * mirror_laplace(shells) + current[..., None] * flag
    new_nodes = (
        node_cond * mirror_laplace(node_pot)
        + current
        - slope * shells[..., NR - 1]
        + plane_cond * lateral[..., :nodes]
    )
    new_collector = collector_cond * lateral[..., nodes:] - jnp.mean(current, axis=-1, keepdims=True)
    return new_shells.reshape(conc.shape), jnp.concatenate([new_nodes, new_collector], axis=-1)


def weights_kernel(hess_ref, out_ref):
    def entry(i, j):
        return hess_ref[j, i : i + 1, 0:1]

    columns = [[entry(i, j) for i in range(j + 2)] for j in range(ITERS)]
    start = hess_ref[ITERS, 0:1, 0:1]
    for k, weight in enumerate(least_squares(columns, start)):
        out_ref[k : k + 1, :] = jnp.broadcast_to(weight, (1, LANES))


def plain_cycle(rhs_conc, rhs_pots, diffusion, exchange, slope):
    axes = ("gx", "gy")
    square = jnp.sum(rhs_conc * rhs_conc) + jnp.sum(rhs_pots * rhs_pots)
    start = jnp.sqrt(lax.psum(square, axes) + epsilon)
    basis_c = jnp.zeros((KV,) + rhs_conc.shape, jnp.float32).at[0].set(rhs_conc / start)
    basis_p = jnp.zeros((KV,) + rhs_pots.shape, jnp.float32).at[0].set(rhs_pots / start)
    hess = jnp.zeros((KV, 16), jnp.float32).at[ITERS, 0].set(start)
    spot = jnp.arange(16)

    def body(step, carry):
        basis_c, basis_p, hess = carry
        conc = lax.dynamic_index_in_dim(basis_c, step, 0, False)
        pots = lax.dynamic_index_in_dim(basis_p, step, 0, False)
        image_c, image_p = local_operator(conc, pots, diffusion, exchange, slope)
        dots = jnp.sum(basis_c * image_c, axis=(1, 2, 3)) + jnp.sum(basis_p * image_p, axis=(1, 2, 3))
        dots = lax.psum(dots, axes)
        rest_c = image_c - jnp.sum(dots[:, None, None, None] * basis_c, axis=0)
        rest_p = image_p - jnp.sum(dots[:, None, None, None] * basis_p, axis=0)
        square = lax.psum(jnp.sum(rest_c * rest_c) + jnp.sum(rest_p * rest_p), axes)
        height = jnp.sqrt(square + epsilon)
        basis_c = lax.dynamic_update_index_in_dim(basis_c, rest_c / height, step + 1, 0)
        basis_p = lax.dynamic_update_index_in_dim(basis_p, rest_p / height, step + 1, 0)
        line = jnp.concatenate([dots, jnp.zeros((16 - KV,), jnp.float32)])
        line = jnp.where(spot == step + 1, height, line)
        hess = lax.dynamic_update_index_in_dim(hess, line, step, 0)
        return basis_c, basis_p, hess

    basis_c, basis_p, hess = lax.fori_loop(0, ITERS, body, (basis_c, basis_p, hess))
    wide = jnp.broadcast_to(hess[:, :, None], hess.shape + (LANES,))
    weights = pl.pallas_call(
        weights_kernel, out_shape=jax.ShapeDtypeStruct((16, LANES), jnp.float32)
    )(wide)[:KV, 0]
    weights = jnp.where(jnp.arange(KV) < ITERS, weights, 0.0)[:, None, None, None]
    return jnp.sum(weights * basis_c, axis=0), jnp.sum(weights * basis_p, axis=0)


def shards(rhs_conc, rhs_pots, diffusion, exchange, slope):
    rows, ys, nodes = exchange.shape
    gx, gy = lax.axis_size("gx"), lax.axis_size("gy")
    half = rows * nodes
    pairs = FIELDS // 2
    assert half * 2 == LANES and nodes * NR == rhs_conc.shape[2]
    assert ys == 16 and ITERS <= ys and gx % 2 == 0
    assert half * 2 == rows * nodes // 8 * ys and LANES == 2 * NR
    window = 8 * ((ys + 2 * ITERS + 1 + 7) // 8)
    f32 = jnp.float32
    vmem = pl.BlockSpec(memory_space=pltpu.VMEM)
    smem = pl.BlockSpec(memory_space=pltpu.SMEM)
    hbm = pl.BlockSpec(memory_space=pltpu.HBM)
    params = pltpu.CompilerParams(vmem_limit_bytes=24 << 20)

    send, up, down, conc_copy, diff_copy = pl.pallas_call(
        pack_kernel,
        out_shape=(
            jax.ShapeDtypeStruct((pairs * ys, LANES), f32),
            jax.ShapeDtypeStruct((EDGE, LANES), f32),
            jax.ShapeDtypeStruct((EDGE, LANES), f32),
            jax.ShapeDtypeStruct(rhs_conc.shape, f32),
            jax.ShapeDtypeStruct(diffusion.shape, f32),
        ),
        compiler_params=params,
    )(rhs_conc, rhs_pots, diffusion, exchange, slope)
    even = lax.axis_index("gy") % 2 == 0
    swaps = [
        [pair for i in range(first, gy - 1, 2) for pair in ((i, i + 1), (i + 1, i))]
        for first in (0, 1)
    ]
    one = lax.ppermute(jnp.where(even, up, down), "gy", swaps[0])
    two = lax.ppermute(jnp.where(even, down, up), "gy", swaps[1])
    basis, coefs, deep, inner_gram = pl.pallas_call(
        free_kernel,
        out_shape=(
            jax.ShapeDtypeStruct((ITERS, 8, NR, LANES), f32),
            jax.ShapeDtypeStruct((2, 8, LANES), f32),
            jax.ShapeDtypeStruct((ys, LANES), f32),
            jax.ShapeDtypeStruct((8, LANES), f32),
        ),
        scratch_shapes=[
            pltpu.VMEM((8, NR, LANES), f32),
            pltpu.VMEM((LANES, 8, LANES), f32),
        ],
        compiler_params=params,
        cost_estimate=pl.CostEstimate(flops=20000000, transcendentals=0, bytes_accessed=3000000),
    )(conc_copy, diff_copy)
    one, two, inner_gram = lax.optimization_barrier((one, two, inner_gram))
    left, right = jnp.where(even, two, one), jnp.where(even, one, two)
    block = jnp.concatenate([send, left, right], axis=0)
    everything = lax.all_gather(block, "gx", axis=0, tiled=False)
    spot = lax.axis_index("gx").astype(jnp.int32).reshape(1)

    quads = gx // 2
    outer, gram = pl.pallas_call(
        functools.partial(powers_kernel, rows=rows, nodes=nodes),
        in_specs=[smem] + [vmem] * 5,
        out_specs=(vmem, vmem),
        out_shape=(
            jax.ShapeDtypeStruct((ITERS, 9, 16, LANES), f32),
            jax.ShapeDtypeStruct((gx * gy, LANES), f32),
        ),
        scratch_shapes=[
            pltpu.VMEM((2, quads, window, LANES), f32),
            pltpu.VMEM((2, quads, window, LANES), f32),
            pltpu.VMEM((2, SHELLS + 1, quads, window, LANES), f32),
            pltpu.VMEM((3, quads, window, LANES), f32),
            pltpu.VMEM((quads, window, LANES), f32),
            pltpu.VMEM((quads, window, LANES), f32),
            pltpu.VMEM((LANES * pl.cdiv(ITERS * ys, LANES), LANES), f32),
            pltpu.VMEM((9, 16, LANES), f32),
            pltpu.VMEM((LANES, 8, LANES), f32),
        ],
        compiler_params=params,
    )(spot, everything, basis, coefs, deep, inner_gram)

    sums = lax.all_to_all(gram, ("gy", "gx"), 0, 0, tiled=True)

    conc, pots, flag = pl.pallas_call(
        solve_kernel,
        out_shape=(
            jax.ShapeDtypeStruct(rhs_conc.shape, f32),
            jax.ShapeDtypeStruct(rhs_pots.shape, f32),
            jax.ShapeDtypeStruct((1,), jnp.int32),
        ),
        out_specs=(hbm, hbm, smem),
        scratch_shapes=[
            pltpu.VMEM(rhs_conc.shape, f32),
            pltpu.VMEM(rhs_pots.shape, f32),
            pltpu.SemaphoreType.DMA((1 + nodes * NR // LANES,)),
        ],
        compiler_params=params,
    )(sums, basis, outer)
    return lax.while_loop(
        lambda carry: carry[0] > 0,
        lambda carry: (0, *plain_cycle(rhs_conc, rhs_pots, diffusion, exchange, slope)),
        (flag[0], conc, pots),
    )[1:]


def solution(mesh):
    spec = P("gx", "gy", None)
    return jax.shard_map(
        shards, mesh=mesh, in_specs=(spec,) * 5, out_specs=(spec, spec), check_vma=False
    )
```
